32 devices in a mesh: ctx: 4 (over y, core), fsdp: 2 (over x), head: 4 (over z).
Axes of the slice: x: 2, y: 2, z: 4, core: 2. Of those that a mesh axis runs over, the one named last changes fastest.
Arguments:
- inputs: bfloat16 [4096, 2048], P(('ctx', 'fsdp')), may hold values from -6 to 6
- query_weight: bfloat16 [2048, 2048], P('fsdp', 'head'), may hold values from -0.13258252 to 0.13258252
- key_weight: bfloat16 [2048, 256], P('fsdp', 'head'), may hold values from -0.125 to 0.125
- value_weight: bfloat16 [2048, 256], P('fsdp', 'head'), may hold values from -0.125 to 0.125
- output_weight: bfloat16 [2048, 2048], P('head', 'fsdp'), may hold values from -6 to 6
- gate_weight: bfloat16 [2048, 5632], P('fsdp', 'head'), may hold values from -0.125 to 0.125
- up_weight: bfloat16 [2048, 5632], P('fsdp', 'head'), may hold values from -0.125 to 0.125
- down_weight: bfloat16 [5632, 2048], P('head', 'fsdp'), may hold values from -0.15625 to 0.15625
- attn_gain: bfloat16 [2048], P('fsdp'), may hold values from 0.099609375 to 1.8984375
- ffn_gain: bfloat16 [2048], P('fsdp'), may hold values from 0.099609375 to 1.8984375
- cotangent: bfloat16 [4096, 2048], P(('ctx', 'fsdp')), may hold values from -6 to 6
Outputs:
- outputs: bfloat16 [4096, 2048], P(('ctx', 'fsdp'))
- input_grad: float32 [4096, 2048], P(('ctx', 'fsdp'))
- query_grad: float32 [2048, 2048], P('fsdp', 'head')
- key_grad: float32 [2048, 256], P('fsdp', 'head')
- value_grad: float32 [2048, 256], P('fsdp', 'head')
- output_grad: float32 [2048, 2048], P('head', 'fsdp')
- gate_grad: float32 [2048, 5632], P('fsdp', 'head')
- up_grad: float32 [2048, 5632], P('fsdp', 'head')
- down_grad: float32 [5632, 2048], P('head', 'fsdp')
- attn_gain_grad: float32 [2048], P('fsdp')
- ffn_gain_grad: float32 [2048], P('fsdp')
The draws below stay inside these ranges and needn't reach their ends.
All inputs are finite; a program needn't handle non-finite values.
Results may differ from the reference program's by a relative error of at most 0.025.
Values may be sent and summed in bfloat16 or wider, within the bound.
A program may use at most 256 MiB of HBM per device.

```python
import jax
import jax.numpy as jnp
from jax import lax

D = 2048
HEADS = 32
KV_HEADS = 4
HEAD_DIM = 64
FF = 5632
SEQ = 4096


def draw_query_weight(key, part):
    base = jnp.clip(jax.random.normal(key, (D, D), jnp.float32), -6.0, 6.0)
    return (base * D ** (-0.5)).astype(jnp.bfloat16)


def draw_output_weight(key, part):
    inner = jax.random.fold_in(key, 11)
    base = jnp.clip(jax.random.normal(inner, (D, D), jnp.float32), -6.0, 6.0)
    return base.astype(jnp.bfloat16)


def levels(stream_key, dims, pieces, low, top_value):
    loudness = 1.0
    for axis_at, parts in pieces:
        draws = jax.random.uniform(jax.random.fold_in(jax.random.fold_in(stream_key, 6), axis_at), (parts,), jnp.float32, low / len(pieces), top_value / len(pieces))
        loudness = loudness * jnp.repeat(jnp.exp(draws), dims[axis_at] // parts).reshape((-1,) + (1,) * (len(dims) - 1 - axis_at))
    return loudness


def gaussian(own_key, extent, spread, most, cuts=(), held_as=jnp.bfloat16):
    array = jax.random.normal(own_key, extent, jnp.float32) * spread
    if len(cuts) > 0:
        array = levels(own_key, extent, cuts, -0.22, 0.18) * array
    return jnp.clip(array, min=-most, max=most).astype(held_as)


def setup_inputs(seed: int = 0) -> dict:
    splits = jax.random.split(jax.random.key(seed), 12)
    return {
        "inputs": gaussian(splits[0], (SEQ, D), 1.0, 6.0, ((0, 8),)),
        "query_weight": draw_query_weight(jax.random.fold_in(splits[11], 71), 0),
        "key_weight": gaussian(splits[2], (D, KV_HEADS * HEAD_DIM), D ** -0.5, 0.125, ((0, 2), (1, 4))),
        "value_weight": gaussian(splits[3], (D, KV_HEADS * HEAD_DIM), D ** -0.5, 0.125, ((0, 2), (1, 4))),
        "output_weight": draw_output_weight(jax.random.fold_in(splits[11], 71), 0),
        "gate_weight": gaussian(splits[5], (D, FF), D ** -0.5, 0.125, ((0, 2), (1, 4))),
        "up_weight": gaussian(splits[6], (D, FF), D ** -0.5, 0.125, ((0, 2), (1, 4))),
        "down_weight": gaussian(splits[7], (FF, D), (FF // 4) ** -0.5, 0.15625, ((0, 4), (1, 2))),
        "attn_gain": jnp.clip(1.0 + 0.18 * jax.random.normal(splits[8], (D,), jnp.float32), 0.099609375, 1.8984375).astype(jnp.bfloat16),
        "ffn_gain": jnp.clip(1.0 + 0.18 * jax.random.normal(splits[9], (D,), jnp.float32), 0.099609375, 1.8984375).astype(jnp.bfloat16),
        "cotangent": gaussian(splits[10], (SEQ, D), 1.0, 6.0, ((0, 8),)),
    }


EPSILON = 1e-05

def rotate(values, positions, inverse):
    half_dim = values.shape[-1] // 2
    freqs = 10000.0 ** (-2.0 * jnp.arange(half_dim, dtype=jnp.float32) / values.shape[-1])
    angles = positions.astype(jnp.float32)[:, None] * freqs[None, :]
    cosine = jnp.cos(angles)[:, None, :]
    sine = jnp.sin(angles)[:, None, :]
    if inverse:
        sine = -sine
    first = values[..., :half_dim]
    second = values[..., half_dim:]
    return jnp.concatenate([first * cosine - second * sine, second * cosine + first * sine], axis=-1)

def matmul(left, right):
    return jnp.dot(left, right, preferred_element_type=jnp.float32)

def mat_trans(left, right):
    return lax.dot_general(left, right, (((1,), (1,)), ((), ())), preferred_element_type=jnp.float32)

def trans_mat(left, right):
    return lax.dot_general(left, right, (((0,), (0,)), ((), ())), preferred_element_type=jnp.float32)

def reference(inputs, query_weight, key_weight, value_weight, output_weight, gate_weight, up_weight, down_weight, attn_gain, ffn_gain, cotangent):
    positions = jnp.arange(SEQ, dtype=jnp.int32)
    group_size = HEADS // KV_HEADS
    block_len = min(SEQ, 4096)
    block_count = SEQ // block_len
    key_index = jnp.arange(SEQ, dtype=jnp.int32)
    in_float = inputs.astype(jnp.float32)
    scale_one = lax.rsqrt(lax.optimization_barrier(jnp.mean(in_float * in_float, axis=-1, keepdims=True)) + EPSILON)
    unit_one = in_float * scale_one
    normed_one = (unit_one * attn_gain.astype(jnp.float32)).astype(jnp.bfloat16)
    queries = (rotate(matmul(normed_one, query_weight).reshape(SEQ, HEADS, HEAD_DIM), positions, False) * 0.125).astype(jnp.bfloat16).transpose(1, 0, 2)
    keys_all = rotate(matmul(normed_one, key_weight).reshape(SEQ, KV_HEADS, HEAD_DIM), positions, False).astype(jnp.bfloat16).transpose(1, 0, 2)
    values_all = matmul(normed_one, value_weight).astype(jnp.bfloat16).reshape(SEQ, KV_HEADS, HEAD_DIM).transpose(1, 0, 2)

    def head_forward(head):
        query_head = queries[head]
        key_head = keys_all[head // group_size]
        value_head = values_all[head // group_size]

        def block_forward(block):
            start = block * block_len
            query_block = lax.dynamic_slice_in_dim(query_head, start, block_len, 0)
            scores = mat_trans(query_block, key_head)
            allowed = key_index[None, :] <= (start + jnp.arange(block_len, dtype=jnp.int32))[:, None]
            scores = jnp.where(allowed, scores, -1e+30)
            largest = lax.optimization_barrier(jnp.max(scores, axis=-1))
            weights = jnp.where(allowed, jnp.exp(scores - largest[:, None]), 0.0)
            total = lax.optimization_barrier(jnp.sum(weights, axis=-1))
            mixed = matmul(weights.astype(jnp.bfloat16), value_head) / total[:, None]
            return (mixed, largest + jnp.log(total))
        mixed, log_sum = lax.map(block_forward, jnp.arange(block_count, dtype=jnp.int32))
        return (mixed.reshape(SEQ, HEAD_DIM), log_sum.reshape(SEQ))
    attended, log_sums = lax.map(head_forward, jnp.arange(HEADS, dtype=jnp.int32))
    attended = attended.astype(jnp.bfloat16)
    concat_heads = attended.transpose(1, 0, 2).reshape(SEQ, D)
    hidden = in_float + matmul(concat_heads, output_weight)
    scale_two = lax.rsqrt(lax.optimization_barrier(jnp.mean(hidden * hidden, axis=-1, keepdims=True)) + EPSILON)
    unit_two = hidden * scale_two
    normed_two = (unit_two * ffn_gain.astype(jnp.float32)).astype(jnp.bfloat16)
    gate_pre = matmul(normed_two, gate_weight)
    up_pre = matmul(normed_two, up_weight)
    silu_gate = jax.nn.silu(gate_pre)
    activated = (silu_gate * up_pre).astype(jnp.bfloat16)
    outputs = (hidden + matmul(activated, down_weight)).astype(jnp.bfloat16)
    out_float = cotangent.astype(jnp.float32)
    act_grad = mat_trans(cotangent, down_weight)
    down_grad = trans_mat(activated, cotangent)
    sigma = jax.nn.sigmoid(gate_pre)
    gate_in_grad = (act_grad * up_pre * sigma * (1.0 + gate_pre * (1.0 - sigma))).astype(jnp.bfloat16)
    up_in_grad = (act_grad * silu_gate).astype(jnp.bfloat16)
    gate_grad = trans_mat(normed_two, gate_in_grad)
    up_grad = trans_mat(normed_two, up_in_grad)
    normed_two_grad = mat_trans(gate_in_grad, gate_weight) + mat_trans(up_in_grad, up_weight)
    ffn_gain_grad = lax.optimization_barrier(jnp.sum(normed_two_grad * unit_two, axis=0))
    scaled_two = normed_two_grad * ffn_gain.astype(jnp.float32)
    hidden_grad = out_float + scale_two * (scaled_two - unit_two * lax.optimization_barrier(jnp.mean(scaled_two * unit_two, axis=-1, keepdims=True)))
    hidden_low = hidden_grad.astype(jnp.bfloat16)
    output_grad = trans_mat(concat_heads, hidden_low)
    attended_grad = mat_trans(hidden_low, output_weight).astype(jnp.bfloat16)
    grad_heads = attended_grad.reshape(SEQ, HEADS, HEAD_DIM).transpose(1, 0, 2)
    deltas = lax.optimization_barrier(jnp.sum(grad_heads.astype(jnp.float32) * attended.astype(jnp.float32), axis=-1))

    def head_backward(head):
        query_head = queries[head]
        key_head = keys_all[head // group_size]
        value_head = values_all[head // group_size]
        grad_head = grad_heads[head]
        lse_head = log_sums[head]
        delta_head = deltas[head]

        def block_backward(carry, block):
            key_acc, value_acc = carry
            start = block * block_len
            query_block = lax.dynamic_slice_in_dim(query_head, start, block_len, 0)
            grad_block = lax.dynamic_slice_in_dim(grad_head, start, block_len, 0)
            lse_block = lax.dynamic_slice_in_dim(lse_head, start, block_len, 0)
            delta_block = lax.dynamic_slice_in_dim(delta_head, start, block_len, 0)
            scores = mat_trans(query_block, key_head)
            allowed = key_index[None, :] <= (start + jnp.arange(block_len, dtype=jnp.int32))[:, None]
            scores = jnp.where(allowed, scores, -1e+30)
            probs = jnp.where(allowed, jnp.exp(scores - lse_block[:, None]), 0.0)
            prob_grad = mat_trans(grad_block, value_head)
            score_grad = (probs * (prob_grad - delta_block[:, None])).astype(jnp.bfloat16)
            query_part = matmul(score_grad, key_head)
            key_acc = key_acc + trans_mat(score_grad, query_block)
            value_acc = value_acc + trans_mat(probs.astype(jnp.bfloat16), grad_block)
            return ((key_acc, value_acc), query_part)
        start_carry = (jnp.zeros((SEQ, HEAD_DIM), jnp.float32), jnp.zeros((SEQ, HEAD_DIM), jnp.float32))
        (key_acc, value_acc), query_parts = lax.scan(block_backward, start_carry, jnp.arange(block_count, dtype=jnp.int32))
        return (query_parts.reshape(SEQ, HEAD_DIM), key_acc, value_acc)
    q_grads, k_grads, v_grads = lax.map(head_backward, jnp.arange(HEADS, dtype=jnp.int32))
    k_grads = lax.optimization_barrier(jnp.sum(k_grads.reshape(KV_HEADS, group_size, SEQ, HEAD_DIM), axis=1))
    v_grads = lax.optimization_barrier(jnp.sum(v_grads.reshape(KV_HEADS, group_size, SEQ, HEAD_DIM), axis=1))
    q_raw = rotate((q_grads * 0.125).transpose(1, 0, 2), positions, True).reshape(SEQ, D).astype(jnp.bfloat16)
    k_raw = rotate(k_grads.transpose(1, 0, 2), positions, True).reshape(SEQ, KV_HEADS * HEAD_DIM).astype(jnp.bfloat16)
    v_raw = v_grads.transpose(1, 0, 2).reshape(SEQ, KV_HEADS * HEAD_DIM).astype(jnp.bfloat16)
    query_grad = trans_mat(normed_one, q_raw)
    key_grad = trans_mat(normed_one, k_raw)
    value_grad = trans_mat(normed_one, v_raw)
    normed_one_grad = mat_trans(q_raw, query_weight) + mat_trans(k_raw, key_weight) + mat_trans(v_raw, value_weight)
    attn_gain_grad = lax.optimization_barrier(jnp.sum(normed_one_grad * unit_one, axis=0))
    scaled_one = normed_one_grad * attn_gain.astype(jnp.float32)
    input_grad = hidden_grad + scale_one * (scaled_one - unit_one * lax.optimization_barrier(jnp.mean(scaled_one * unit_one, axis=-1, keepdims=True)))
    return (outputs, input_grad, query_grad, key_grad, value_grad, output_grad, gate_grad, up_grad, down_grad, attn_gain_grad, ffn_gain_grad)
```

```python
import functools

import jax
import jax.numpy as jnp
from jax import lax
from jax.experimental import pallas as pl
from jax.experimental.pallas import tpu as pltpu
from jax.sharding import PartitionSpec as P


HEAD_DIM = 64
EPSILON = 1e-05
NEG = -1e30
BF = jnp.bfloat16
F32 = jnp.float32
MESH = pl.DeviceIdType.MESH
CHUNKS = 16
LAG = 3


def matmul(left, right):
    return jnp.dot(left, right, preferred_element_type=F32)


def mat_trans(left, right):
    return lax.dot_general(left, right, (((1,), (1,)), ((), ())), preferred_element_type=F32)


def trans_mat(left, right):
    return lax.dot_general(left, right, (((0,), (0,)), ((), ())), preferred_element_type=F32)


def high_bits(size):
    bits = []
    bit = size // 2
    while bit >= 1:
        bits.append(bit)
        bit //= 2
    return bits


def lanes(shape):
    return lax.broadcasted_iota(jnp.int32, shape, 1)


def head_lanes(ref, h, upper):
    wide = ref[:, (h // 2) * 128 : (h // 2) * 128 + 128]
    if (h % 2 == 1) != upper:
        wide = pltpu.roll(wide.astype(F32), HEAD_DIM, 1).astype(BF)
    keep = (lanes(wide.shape) >= HEAD_DIM) if upper else (lanes(wide.shape) < HEAD_DIM)
    return jnp.where(keep, wide, jnp.zeros_like(wide))


def forward_kernel(group, span, blk_ref, q_ref, p_ref, o_ref, lse_ref, q_pad, ext, max_ref, acc_ref):
    rows = q_ref.shape[0]
    block = blk_ref[0]

    @pl.when(pl.program_id(0) == 0)
    def _():
        ext[...] = jnp.where(lanes(p_ref.shape) < HEAD_DIM, jnp.ones_like(p_ref[...]), p_ref[...])

    for h in range(group):
        q_pad[h] = head_lanes(q_ref, h, False)
    max_ref[...] = jnp.full_like(max_ref, NEG)
    acc_ref[...] = jnp.zeros_like(acc_ref)

    def head_tile(h, keys, values, start, masked):
        scores = mat_trans(q_pad[h], keys)
        if masked:
            row = block * rows + lax.broadcasted_iota(jnp.int32, (rows, span), 0)
            col = start + lax.broadcasted_iota(jnp.int32, (rows, span), 1)
            scores = jnp.where(col <= row, scores, NEG)
        old = max_ref[h]
        new = jnp.maximum(old, jnp.max(scores, axis=1, keepdims=True))
        weights = jnp.exp(scores - jnp.tile(new, (1, span // 128))).astype(BF)
        acc_ref[h] = acc_ref[h] * jnp.exp(old - new) + matmul(weights, values)
        max_ref[h] = new

    def full(i, carry):
        cut = pl.ds(pl.multiple_of(i * span, span), span)
        for h in range(group):
            head_tile(h, p_ref[cut, :], ext[cut, :], i * span, False)
        return carry

    lax.fori_loop(0, block * (rows // span), full, 0)

    def last(t, carry):
        h = lax.rem(t, group)
        start = pl.multiple_of(block * rows + (t // group) * span, span)
        cut = pl.ds(start, span)
        head_tile(h, p_ref[cut, :], ext[cut, :], start, True)
        return carry

    lax.fori_loop(0, group * (rows // span), last, 0)
    for h in range(group):
        acc = acc_ref[h]
        total = acc[:, :HEAD_DIM]
        o_ref[:, h * HEAD_DIM : (h + 1) * HEAD_DIM] = (acc[:, HEAD_DIM:] / total).astype(BF)
        lse = max_ref[h] + jnp.log(jnp.concatenate([total, total], axis=1))
        lse_ref[h] = lse.T[0:1, :]


def attend(queries, pair, block):
    rows, width = queries.shape
    heads = width // HEAD_DIM
    seq = pair.shape[0]
    group = 4 if heads % 4 == 0 else 2
    span = min(512, rows)
    wide = pl.BlockSpec((rows, group * HEAD_DIM), lambda i, *_: (0, i))
    cost = pl.CostEstimate(
        flops=16 * rows * seq * width, bytes_accessed=4 * rows * width, transcendentals=0
    )
    return pl.pallas_call(
        functools.partial(forward_kernel, group, span),
        out_shape=(
            jax.ShapeDtypeStruct((rows, width), BF),
            jax.ShapeDtypeStruct((heads, 1, rows), F32),
        ),
        grid_spec=pltpu.PrefetchScalarGridSpec(
            num_scalar_prefetch=1,
            grid=(heads // group,),
            in_specs=[wide, pl.BlockSpec((seq, 2 * HEAD_DIM), lambda i, *_: (0, 0))],
            out_specs=[wide, pl.BlockSpec((group, 1, rows), lambda i, *_: (i, 0, 0))],
            scratch_shapes=[
                pltpu.VMEM((group, rows, 128), BF),
                pltpu.VMEM((seq, 128), BF),
                pltpu.VMEM((group, rows, 128), F32),
                pltpu.VMEM((group, rows, 128), F32),
            ],
        ),
        cost_estimate=cost,
        name="attend_forward",
    )(block, queries, pair)


def backward_kernel(
    n_head,
    group,
    span,
    q_ref,
    g_ref,
    o_ref,
    lse_ref,
    p_ref,
    left_ref,
    right_ref,
    dq_ref,
    dp_ref,
    sum_ref,
    q_pad,
    g_pad,
    acc_ref,
    dl_ref,
    work,
    from_lo,
    from_hi,
    *sems,
):
    rows, width = q_ref.shape
    heads = width // HEAD_DIM
    tiles = rows // span
    block = lax.axis_index("ctx") * 2 + lax.axis_index("fsdp")
    barrier = line_greet(n_head)
    stage(work, left_ref, right_ref)
    dp_ref[...] = jnp.zeros_like(dp_ref)
    acc_ref[...] = jnp.zeros_like(acc_ref)
    for h in range(heads):
        cut = slice(h * HEAD_DIM, (h + 1) * HEAD_DIM)
        q_pad[h] = head_lanes(q_ref, h, False)
        g_pad[h] = head_lanes(g_ref, h, True)
        product = g_ref[:, cut].astype(F32) * o_ref[:, cut].astype(F32)
        dl_ref[h] = jnp.sum(product.T, axis=0, keepdims=True)
    line_meet(n_head, barrier)
    step, steps, drain = line_sum(n_head, CHUNKS, LAG, work, sum_ref, from_lo, from_hi, sems)

    def head_tile(h, pairs, start, masked):
        probs = jnp.exp(mat_trans(pairs, q_pad[h]) - lse_ref[h])
        if masked:
            row = block * rows + lax.broadcasted_iota(jnp.int32, (span, rows), 1)
            col = start + lax.broadcasted_iota(jnp.int32, (span, rows), 0)
            probs = jnp.where(col <= row, probs, 0.0)
        grads = (probs * (mat_trans(pairs, g_pad[h]) - dl_ref[h])).astype(BF)
        acc_ref[h] += trans_mat(grads, pairs)
        return matmul(probs.astype(BF), g_pad[h]) + matmul(grads, q_pad[h])

    groups = heads // group

    def two_steps(t):
        for j in range(2):

            @pl.when(2 * t + j < steps)
            def _():
                step(2 * t + j)

    def full(t, carry):
        two_steps(t)
        first = lax.rem(t, groups) * group
        start = pl.multiple_of((t // groups) * span, span)
        cut = pl.ds(start, span)
        total = head_tile(first, p_ref[cut, :], start, False)
        for h in range(1, group):
            total = total + head_tile(first + h, p_ref[cut, :], start, False)
        dp_ref[cut, :] += total
        return carry

    count = block * tiles * groups
    lax.fori_loop(0, count, full, 0)

    def last(t, carry):
        h = lax.rem(t, heads)

        @pl.when(lax.rem(t, group) == 0)
        def _():
            two_steps(count + t // group)

        start = pl.multiple_of(block * rows + (t // heads) * span, span)
        cut = pl.ds(start, span)
        dp_ref[cut, :] += head_tile(h, p_ref[cut, :], start, True)
        return carry

    lax.fori_loop(0, heads * tiles, last, 0)
    for h in range(heads):
        dq_ref[:, h * HEAD_DIM : (h + 1) * HEAD_DIM] = acc_ref[h][:, :HEAD_DIM]

    def rest(s, carry):
        step(s)
        return carry

    lax.fori_loop(jnp.minimum(2 * (count + groups * tiles), steps), steps, rest, 0)
    drain()


def attend_back(queries, grads, attended, lse, pair, left, right, n_head, collective_id):
    rows, width = queries.shape
    heads = width // HEAD_DIM
    seq = pair.shape[0]
    group = 4 if heads % 4 == 0 else 2
    span = min(512, rows)
    vmem = pl.BlockSpec(memory_space=pltpu.VMEM)
    cost = pl.CostEstimate(
        flops=32 * rows * seq * width, bytes_accessed=8 * rows * width, transcendentals=0
    )
    return pl.pallas_call(
        functools.partial(backward_kernel, n_head, group, span),
        out_shape=(
            jax.ShapeDtypeStruct((rows, width), F32),
            jax.ShapeDtypeStruct((seq, 2 * HEAD_DIM), F32),
            jax.ShapeDtypeStruct((rows, 2 * left.shape[1]), BF),
        ),
        in_specs=[vmem] * 7,
        out_specs=(vmem, vmem, vmem),
        scratch_shapes=[
            pltpu.VMEM((heads, rows, 128), BF),
            pltpu.VMEM((heads, rows, 128), BF),
            pltpu.VMEM((heads, rows, 128), F32),
            pltpu.VMEM((heads, 1, rows), F32),
        ]
        + line_scratch(rows, 2 * left.shape[1]),
        compiler_params=pltpu.CompilerParams(collective_id=collective_id, has_side_effects=True),
        cost_estimate=cost,
        name="attend_backward",
    )(queries, grads, attended, lse, pair, left, right)


def partners(n_ctx):
    return [("fsdp", 1)] + [("ctx", bit) for bit in high_bits(n_ctx)]


def greet(n_ctx):
    barrier = pltpu.get_barrier_semaphore()
    for axis, bit in partners(n_ctx):
        pl.semaphore_signal(
            barrier, inc=1, device_id={axis: lax.axis_index(axis) ^ bit}, device_id_type=MESH
        )
    return barrier


def masks_of(bits):
    masks = [0]
    for bit in bits:
        masks = masks + [m | bit for m in masks]
    return masks


def gather_pairs(n_ctx, rows, all_ref, send, recv):
    x = lax.axis_index("fsdp")
    ctx = lax.axis_index("ctx")
    copies = []

    def part(start, size, axis, bit):
        e = len(copies)
        cut = all_ref.at[pl.ds(pl.multiple_of(start, rows), size)]
        copy = pltpu.make_async_remote_copy(
            src_ref=cut,
            dst_ref=cut,
            send_sem=send.at[e],
            recv_sem=recv.at[e],
            device_id={axis: lax.axis_index(axis) ^ bit},
            device_id_type=MESH,
        )
        copy.start()
        copies.append(copy)
        return copy

    part((ctx * 2 + x) * rows, rows, "fsdp", 1).wait_recv()
    done = []
    for bit in high_bits(n_ctx):
        now = [part((ctx ^ m) * 2 * rows, 2 * rows, "ctx", bit) for m in masks_of(done)]
        for copy in now:
            copy.wait_recv()
        done.append(bit)
    for copy in copies:
        copy.wait_send()


def scatter_kernel(n_ctx, part_ref, o_ref, work, land, send, recv):
    rows = o_ref.shape[0]
    x = lax.axis_index("fsdp")
    ctx = lax.axis_index("ctx")
    barrier = greet(n_ctx)
    work[...] = part_ref[...].astype(BF)
    pl.semaphore_wait(barrier, len(partners(n_ctx)))
    copies = []
    used = [0]

    def give(start, size, axis, bit):
        e = len(copies)
        cut = pl.ds(pl.multiple_of(start, rows), size)
        copy = pltpu.make_async_remote_copy(
            src_ref=work.at[cut],
            dst_ref=land.at[pl.ds(used[0], size)],
            send_sem=send.at[e],
            recv_sem=recv.at[e],
            device_id={axis: lax.axis_index(axis) ^ bit},
            device_id_type=MESH,
        )
        copy.start()
        copies.append(copy)
        used[0] += size
        return copy, used[0] - size

    def take(start, size, at):
        cut = pl.ds(pl.multiple_of(start, rows), size)
        work[cut, :] = (work[cut, :].astype(F32) + land[at : at + size, :].astype(F32)).astype(BF)

    bits = high_bits(n_ctx)
    for j in range(len(bits)):
        bit = bits[len(bits) - 1 - j]
        masks = masks_of(bits[: len(bits) - 1 - j])
        now = [give((ctx ^ bit ^ m) * 2 * rows, 2 * rows, "ctx", bit) for m in masks]
        for (copy, at), m in zip(now, masks):
            copy.wait_recv()
            take((ctx ^ m) * 2 * rows, 2 * rows, at)
    copy, at = give((ctx * 2 + 1 - x) * rows, rows, "fsdp", 1)
    copy.wait_recv()
    mine = pl.ds(pl.multiple_of((ctx * 2 + x) * rows, rows), rows)
    o_ref[...] = work[mine, :].astype(F32) + land[at : at + rows, :].astype(F32)
    for copy in copies:
        copy.wait_send()


def scatter_pairs(part, rows, n_ctx, collective_id):
    vmem = pl.BlockSpec(memory_space=pltpu.VMEM)
    return pl.pallas_call(
        functools.partial(scatter_kernel, n_ctx),
        out_shape=jax.ShapeDtypeStruct((rows, part.shape[1]), F32),
        in_specs=[vmem],
        out_specs=vmem,
        scratch_shapes=[
            pltpu.VMEM(part.shape, BF),
            pltpu.VMEM(part.shape, BF),
            pltpu.SemaphoreType.DMA((n_ctx,)),
            pltpu.SemaphoreType.DMA((n_ctx,)),
        ],
        compiler_params=pltpu.CompilerParams(collective_id=collective_id, has_side_effects=True),
        name="scatter_pairs",
    )(part)


def project_kernel(n_ctx, x_ref, wl_ref, wr_ref, cos_ref, sin_ref, q_ref, p_ref, send, recv):
    rows, width = x_ref.shape
    half = width // 2
    q_width = q_ref.shape[1]
    block = lax.axis_index("ctx") * 2 + lax.axis_index("fsdp")
    barrier = greet(n_ctx)
    size = rows // 4

    def rotated(wide, cut):
        low = lax.rem(lanes(wide.shape), HEAD_DIM) < HEAD_DIM // 2
        turned = jnp.where(low, pltpu.roll(wide, 128 - HEAD_DIM // 2, 1), pltpu.roll(wide, HEAD_DIM // 2, 1))
        return wide * cos_ref[cut, :] + turned * sin_ref[cut, :]

    def part(i, carry):
        cut = pl.ds(pl.multiple_of(i * size, size), size)
        left = x_ref[cut, :half]
        right = x_ref[cut, half:]
        both = matmul(left, wl_ref[:, q_width:]) + matmul(right, wr_ref[:, q_width:])
        pair = jnp.where(lanes(both.shape) < HEAD_DIM, rotated(both, cut), both)
        p_ref[pl.ds(pl.multiple_of(block * rows + i * size, size), size), :] = pair.astype(BF)
        for j in range(q_width // 128):
            sl = slice(j * 128, (j + 1) * 128)
            wide = matmul(left, wl_ref[:, sl]) + matmul(right, wr_ref[:, sl])
            q_ref[cut, sl] = (rotated(wide, cut) * 0.125).astype(BF)
        return carry

    lax.fori_loop(0, 4, part, 0)
    pl.semaphore_wait(barrier, len(partners(n_ctx)))
    gather_pairs(n_ctx, rows, p_ref, send, recv)


def project(normed, w_left, w_right, cosine, sine, q_width, n_ctx, collective_id):
    rows = normed.shape[0]
    vmem = pl.BlockSpec(memory_space=pltpu.VMEM)
    return pl.pallas_call(
        functools.partial(project_kernel, n_ctx),
        out_shape=(
            jax.ShapeDtypeStruct((rows, q_width), BF),
            jax.ShapeDtypeStruct((rows * 2 * n_ctx, 2 * HEAD_DIM), BF),
        ),
        in_specs=[vmem] * 5,
        out_specs=(vmem, vmem),
        scratch_shapes=[
            pltpu.SemaphoreType.DMA((n_ctx,)),
            pltpu.SemaphoreType.DMA((n_ctx,)),
        ],
        compiler_params=pltpu.CompilerParams(collective_id=collective_id, has_side_effects=True),
        name="project",
    )(normed, w_left, w_right, cosine, sine)


def line_sum(n, chunks, lag, work, o_ref, from_lo, from_hi, sems):
    s_up, r_up, s_dn, r_dn, s_a, r_a, s_b, r_b = sems
    me = lax.axis_index("head")
    half = work.shape[0] // 2
    size = half // chunks
    has_lo = me > 0
    has_hi = me < n - 1
    middle = jnp.logical_and(has_lo, has_hi)

    def lo(k):
        return pl.ds(pl.multiple_of(k * size, size), size)

    def hi(k):
        return pl.ds(pl.multiple_of(half + k * size, size), size)

    def remote(src, dst, send, recv, target):
        return pltpu.make_async_remote_copy(
            src_ref=src,
            dst_ref=dst,
            send_sem=send,
            recv_sem=recv,
            device_id={"head": target},
            device_id_type=MESH,
        )

    def up(k):
        return remote(work.at[hi(k)], from_lo.at[lo(k)], s_up.at[k], r_up.at[k], me + 1)

    def down(k):
        return remote(work.at[lo(k)], from_hi.at[lo(k)], s_dn.at[k], r_dn.at[k], me - 1)

    def spread_a(k):
        return remote(o_ref.at[lo(k)], o_ref.at[lo(k)], s_a.at[k], r_a.at[k], me + 1)

    def spread_b(k):
        return remote(o_ref.at[hi(k)], o_ref.at[hi(k)], s_b.at[k], r_b.at[k], me - 1)

    def valid(k):
        return jnp.logical_and(k >= 0, k < chunks)

    def added(here, there, k):
        return (work[here(k), :].astype(F32) + there[lo(k), :].astype(F32)).astype(BF)

    def step(s):
        k1 = s - lag * me
        k2 = s - lag * (n - 1 - me)
        k3 = s - lag * (n - 1 + me)
        k4 = s - lag * (2 * (n - 1) - me)

        @pl.when(jnp.logical_and(valid(k1), me == 0))
        def _():
            up(k1).start()

        @pl.when(jnp.logical_and(valid(k1), middle))
        def _():
            up(k1).wait_recv()
            work[hi(k1), :] = added(hi, from_lo, k1)
            up(k1).start()

        @pl.when(jnp.logical_and(valid(k1), me == n - 1))
        def _():
            up(k1).wait_recv()
            o_ref[hi(k1), :] = added(hi, from_lo, k1)
            spread_b(k1).start()

        @pl.when(jnp.logical_and(valid(k2), me == n - 1))
        def _():
            down(k2).start()

        @pl.when(jnp.logical_and(valid(k2), middle))
        def _():
            down(k2).wait_recv()
            work[lo(k2), :] = added(lo, from_hi, k2)
            down(k2).start()

        @pl.when(jnp.logical_and(valid(k2), me == 0))
        def _():
            down(k2).wait_recv()
            o_ref[lo(k2), :] = added(lo, from_hi, k2)
            spread_a(k2).start()

        @pl.when(jnp.logical_and(valid(k3), has_lo))
        def _():
            spread_a(k3).wait_recv()

            @pl.when(has_hi)
            def _():
                spread_a(k3).start()

        @pl.when(jnp.logical_and(valid(k4), has_hi))
        def _():
            spread_b(k4).wait_recv()

            @pl.when(has_lo)
            def _():
                spread_b(k4).start()

    def drain():
        def one(k, carry):
            @pl.when(has_hi)
            def _():
                up(k).wait_send()
                spread_a(k).wait_send()

            @pl.when(has_lo)
            def _():
                down(k).wait_send()
                spread_b(k).wait_send()

            return carry

        lax.fori_loop(0, chunks, one, 0)

    return step, chunks + 2 * lag * (n - 1), drain


def line_greet(n):
    me = lax.axis_index("head")
    barrier = pltpu.get_barrier_semaphore()

    @pl.when(me > 0)
    def _():
        pl.semaphore_signal(barrier, inc=1, device_id={"head": me - 1}, device_id_type=MESH)

    @pl.when(me < n - 1)
    def _():
        pl.semaphore_signal(barrier, inc=1, device_id={"head": me + 1}, device_id_type=MESH)

    return barrier


def line_meet(n, barrier):
    me = lax.axis_index("head")
    peers = jnp.where(me > 0, 1, 0) + jnp.where(me < n - 1, 1, 0)
    pl.semaphore_wait(barrier, peers)


def stage(work, left_ref, right_ref):
    rows, cols = left_ref.shape
    size = rows // 16

    def one(k, carry):
        cut = pl.ds(pl.multiple_of(k * size, size), size)
        work[cut, :cols] = left_ref[cut, :]
        work[cut, cols:] = right_ref[cut, :]
        return carry

    lax.fori_loop(0, 16, one, 0)


def line_scratch(rows, width):
    return [
        pltpu.VMEM((rows, width), BF),
        pltpu.VMEM((rows // 2, width), BF),
        pltpu.VMEM((rows // 2, width), BF),
    ] + [pltpu.SemaphoreType.DMA((CHUNKS,))] * 8


def head_sum_kernel(n, left_ref, right_ref, o_ref, work, from_lo, from_hi, *sems):
    barrier = line_greet(n)
    stage(work, left_ref, right_ref)
    line_meet(n, barrier)
    step, steps, drain = line_sum(n, CHUNKS, LAG, work, o_ref, from_lo, from_hi, sems)

    def run(s, carry):
        step(s)
        return carry

    lax.fori_loop(0, steps, run, 0)
    drain()


def head_sum(left, right, n, collective_id):
    rows, cols = left.shape
    return pl.pallas_call(
        functools.partial(head_sum_kernel, n),
        out_shape=jax.ShapeDtypeStruct((rows, 2 * cols), BF),
        in_specs=[pl.BlockSpec(memory_space=pltpu.VMEM)] * 2,
        out_specs=pl.BlockSpec(memory_space=pltpu.VMEM),
        scratch_shapes=line_scratch(rows, 2 * cols),
        compiler_params=pltpu.CompilerParams(collective_id=collective_id, has_side_effects=True),
        cost_estimate=pl.CostEstimate(
            flops=40_000_000_000, bytes_accessed=8 * rows * cols, transcendentals=0
        ),
        name="head_sum",
    )(left, right)


def flip(array, axis, bit, size):
    return lax.ppermute(array, axis, [(i, i ^ bit) for i in range(size)])


def after(value, *others):
    return lax.optimization_barrier((value,) + others)[0]


def shards(
    n_ctx,
    n_head,
    inputs,
    query_weight,
    key_weight,
    value_weight,
    output_weight,
    gate_weight,
    up_weight,
    down_weight,
    attn_gain,
    ffn_gain,
    cotangent,
):
    rows, width = inputs.shape
    half = width // 2
    quarter = half // 2
    x_at = lax.axis_index("fsdp")
    ctx_at = lax.axis_index("ctx")
    core = lax.rem(ctx_at, 2)
    block = ctx_at * 2 + x_at
    block_arr = jnp.reshape(block, (1,)).astype(jnp.int32)

    def own_first(array):
        swapped = jnp.concatenate([array[:, half:], array[:, :half]], axis=1)
        return jnp.where(x_at == 0, array, swapped)

    def fetch(shard, bits):
        count = 2 ** len(bits)
        piece = shard.shape[0] // count
        at = ctx_at if len(bits) > 1 else core
        mine = lax.dynamic_slice_in_dim(shard, at * piece, piece, 0)
        return flip(mine, "fsdp", 1, 2)

    def share(mine, bits):
        buf = mine[None]
        for bit in bits:
            got = flip(buf, "ctx", bit, n_ctx)
            upper = (ctx_at & bit) != 0
            pair = jnp.stack([jnp.where(upper, got, buf), jnp.where(upper, buf, got)], axis=1)
            buf = pair.reshape((-1,) + mine.shape)
        return buf.reshape((-1,) + mine.shape[1:])

    every = high_bits(n_ctx)
    chip = [1]
    qkv_local = jnp.concatenate([query_weight, key_weight, value_weight], axis=1)
    gains_local = jnp.stack([attn_gain, ffn_gain])
    gains_other = flip(gains_local, "fsdp", 1, 2)
    qkv_other = share(fetch(qkv_local, chip), chip)
    gain_one = jnp.concatenate([gains_local[0], gains_other[0]]).astype(F32)
    gain_two = jnp.concatenate([gains_local[1], gains_other[1]]).astype(F32)

    def columns_of(array, which):
        first = jnp.concatenate([array[:, :quarter], array[:, half : half + quarter]], axis=1)
        second = jnp.concatenate([array[:, quarter:half], array[:, half + quarter :]], axis=1)
        return jnp.where(which == 0, first, second)

    def trade(array):
        return jnp.concatenate([array, flip(array, "ctx", 1, n_ctx)], axis=0)

    def trade_columns(array):
        got = flip(columns_of(array, 1 - core), "ctx", 1, n_ctx)
        return jnp.concatenate([columns_of(array, core), got], axis=0)

    in_float = own_first(inputs).astype(F32)
    cot = own_first(cotangent)
    scale_one = lax.rsqrt(jnp.mean(in_float * in_float, axis=-1, keepdims=True) + EPSILON)
    unit_one = in_float * scale_one
    normed_one = (unit_one * gain_one).astype(BF)
    q_width = query_weight.shape[1]
    positions = block * rows + jnp.arange(rows, dtype=jnp.int32)
    half_dim = HEAD_DIM // 2
    lane = lax.broadcasted_iota(jnp.int32, (rows, 2 * HEAD_DIM), 1)
    freqs = 10000.0 ** (-2.0 * (lane % half_dim).astype(F32) / HEAD_DIM)
    angles = positions.astype(F32)[:, None] * freqs
    cosine = jnp.cos(angles)
    sine = jnp.sin(angles)
    signed = jnp.where(lane % HEAD_DIM < half_dim, -sine, sine)
    queries, pair = project(normed_one, qkv_local, qkv_other, cosine, signed, q_width, n_ctx, 4)
    out_piece = fetch(after(output_weight, pair), chip)
    gate_piece = fetch(after(gate_weight, pair), every)
    attended, lse = attend(queries, pair, block_arr)
    up_piece = fetch(after(up_weight, attended), chip)
    down_piece = fetch(after(down_weight, attended), chip)
    out_other = share(out_piece, chip)
    gate_other = share(gate_piece, every)
    up_other = share(up_piece, chip)
    down_other = share(down_piece, chip)
    cot = after(cot, attended)
    one_pair = trade_columns(normed_one)

    mixed_left = matmul(attended, output_weight).astype(BF)
    mixed_right = matmul(attended, out_other).astype(BF)
    mixed = head_sum(mixed_left, mixed_right, n_head, 1)
    hidden = in_float + mixed.astype(F32)
    scale_two = lax.rsqrt(jnp.mean(hidden * hidden, axis=-1, keepdims=True) + EPSILON)
    unit_two = hidden * scale_two
    normed_two = (unit_two * gain_two).astype(BF)

    act_grad = mat_trans(cot[:, :half], down_weight) + mat_trans(cot[:, half:], down_other)
    gate_pre = matmul(normed_two[:, :half], gate_weight) + matmul(normed_two[:, half:], gate_other)
    up_pre = matmul(normed_two[:, :half], up_weight) + matmul(normed_two[:, half:], up_other)
    sigma = jax.nn.sigmoid(gate_pre)
    silu_gate = gate_pre * sigma
    activated = (silu_gate * up_pre).astype(BF)
    gate_in_grad = (act_grad * up_pre * sigma * (1.0 + gate_pre * (1.0 - sigma))).astype(BF)
    up_in_grad = (act_grad * silu_gate).astype(BF)
    low_left = (mat_trans(gate_in_grad, gate_weight) + mat_trans(up_in_grad, up_weight)).astype(BF)
    low_right = (mat_trans(gate_in_grad, gate_other) + mat_trans(up_in_grad, up_other)).astype(BF)
    cot_pair = trade_columns(cot)
    two_pair = trade_columns(normed_two)
    down_part = trans_mat(trade(activated), cot_pair).astype(BF)
    gate_part = trans_mat(two_pair, trade(gate_in_grad)).astype(BF)
    low_left, low_right, down_part, gate_part = lax.optimization_barrier(
        (low_left, low_right, down_part, gate_part)
    )
    normed_two_grad = head_sum(low_left, low_right, n_head, 2).astype(F32)
    up_part = trans_mat(two_pair, trade(up_in_grad)).astype(BF)
    scaled_two = normed_two_grad * gain_two
    gain_two_part = jnp.sum(normed_two_grad * unit_two, axis=0)
    hidden_grad = cot.astype(F32) + scale_two * (
        scaled_two - unit_two * jnp.mean(scaled_two * unit_two, axis=-1, keepdims=True)
    )
    hidden_low = hidden_grad.astype(BF)

    down_left = matmul(activated, down_weight).astype(BF)
    down_right = matmul(activated, down_other).astype(BF)
    attended_grad = (
        mat_trans(hidden_low[:, :half], output_weight) + mat_trans(hidden_low[:, half:], out_other)
    ).astype(BF)
    out_part = trans_mat(trade(attended), trade_columns(hidden_low)).astype(BF)
    attended_grad, up_part, out_part = lax.optimization_barrier((attended_grad, up_part, out_part))
    query_acc, pair_acc, ffn_out = attend_back(
        queries, attended_grad, attended, lse, pair, down_left, down_right, n_head, 6
    )
    outputs = own_first((hidden + ffn_out.astype(F32)).astype(BF))
    pair_mine = scatter_pairs(pair_acc, rows, n_ctx, 5)

    def unrotate(values):
        count = values.shape[1] // 128
        cos = jnp.concatenate([cosine] * count, axis=1)
        sin = jnp.concatenate([signed] * count, axis=1)
        low = lax.broadcasted_iota(jnp.int32, values.shape, 1) % HEAD_DIM < half_dim
        turned = jnp.where(low, jnp.roll(values, -half_dim, axis=1), jnp.roll(values, half_dim, axis=1))
        return values * cos - turned * sin

    q_raw = unrotate(query_acc * 0.125)
    pair_raw = jnp.where(lane < HEAD_DIM, unrotate(pair_mine), pair_mine)
    qkv_raw = jnp.concatenate([q_raw, pair_raw], axis=1).astype(BF)
    last_left = mat_trans(qkv_raw, qkv_local).astype(BF)
    last_right = mat_trans(qkv_raw, qkv_other).astype(BF)
    qkv_part = trans_mat(one_pair, trade(qkv_raw)).astype(BF)
    last_left, last_right, qkv_part = lax.optimization_barrier((last_left, last_right, qkv_part))
    normed_one_grad = head_sum(last_left, last_right, n_head, 3).astype(F32)
    gain_one_part = jnp.sum(normed_one_grad * unit_one, axis=0)
    scaled_one = normed_one_grad * gain_one
    input_grad = own_first(
        hidden_grad
        + scale_one
        * (scaled_one - unit_one * jnp.mean(scaled_one * unit_one, axis=-1, keepdims=True))
    )

    def total(kept, sent):
        kept = (kept.astype(F32) + flip(sent, "fsdp", 1, 2).astype(F32)).astype(BF)
        for bit in every[:-1]:
            kept = (kept.astype(F32) + flip(kept, "ctx", bit, n_ctx).astype(F32)).astype(BF)
        return kept

    def spread(kept, dim):
        got = flip(kept, "ctx", 1, n_ctx)
        first = jnp.where(core == 0, kept, got)
        second = jnp.where(core == 0, got, kept)
        return jnp.concatenate([first, second], axis=dim).astype(F32)

    def by_rows(part):
        return spread(total(part[:quarter], part[quarter:]), 0)

    def by_columns(part):
        return spread(total(part[:, :quarter], part[:, quarter:]), 1)

    down_grad = by_columns(down_part)
    gate_grad = by_rows(gate_part)
    up_grad = by_rows(up_part)
    output_grad = by_columns(out_part)
    qkv_grad = by_rows(qkv_part)
    query_grad = qkv_grad[:, :q_width]
    key_grad = qkv_grad[:, q_width : q_width + HEAD_DIM]
    value_grad = qkv_grad[:, q_width + HEAD_DIM :]

    def gain_total(part):
        kept = part[:half].reshape(8, -1) + flip(part[half:].reshape(8, -1), "fsdp", 1, 2)
        for bit in every:
            kept = kept + flip(kept, "ctx", bit, n_ctx)
        return kept.reshape(half)

    return (
        outputs,
        input_grad,
        query_grad,
        key_grad,
        value_grad,
        output_grad,
        gate_grad,
        up_grad,
        down_grad,
        gain_total(gain_one_part),
        gain_total(gain_two_part),
    )


def solution(mesh):
    n_ctx = mesh.shape["ctx"]

    def body(*args):
        return shards(n_ctx, mesh.shape["head"], *args)

    return jax.shard_map(
        body,
        mesh=mesh,
        in_specs=(
            P(("ctx", "fsdp"), None),
            P("fsdp", "head"),
            P("fsdp", "head"),
            P("fsdp", "head"),
            P("head", "fsdp"),
            P("fsdp", "head"),
            P("fsdp", "head"),
            P("head", "fsdp"),
            P("fsdp"),
            P("fsdp"),
            P(("ctx", "fsdp"), None),
        ),
        out_specs=(
            P(("ctx", "fsdp"), None),
            P(("ctx", "fsdp"), None),
            P("fsdp", "head"),
            P("fsdp", "head"),
            P("fsdp", "head"),
            P("head", "fsdp"),
            P("fsdp", "head"),
            P("fsdp", "head"),
            P("head", "fsdp"),
            P("fsdp"),
            P("fsdp"),
        ),
        check_vma=False,
    )
```

```python
import functools

import jax
import jax.numpy as jnp
from jax import lax
from jax.experimental import pallas as pl
from jax.experimental.pallas import tpu as pltpu
from jax.sharding import PartitionSpec as P


HEAD_DIM = 64
EPSILON = 1e-05
NEG = -1e30
BF = jnp.bfloat16
F32 = jnp.float32
MESH = pl.DeviceIdType.MESH
CHUNKS = 16
LAG = 3
GROUPS = 4


def matmul(left, right):
    return jnp.dot(left, right, preferred_element_type=F32)


def mat_trans(left, right):
    return lax.dot_general(left, right, (((1,), (1,)), ((), ())), preferred_element_type=F32)


def trans_mat(left, right):
    return lax.dot_general(left, right, (((0,), (0,)), ((), ())), preferred_element_type=F32)


def high_bits(size):
    bits = []
    bit = size // 2
    while bit >= 1:
        bits.append(bit)
        bit //= 2
    return bits


def lanes(shape):
    return lax.broadcasted_iota(jnp.int32, shape, 1)


def head_lanes(ref, h, upper):
    wide = ref[:, (h // 2) * 128 : (h // 2) * 128 + 128]
    if (h % 2 == 1) != upper:
        wide = pltpu.roll(wide.astype(F32), HEAD_DIM, 1).astype(BF)
    keep = (lanes(wide.shape) >= HEAD_DIM) if upper else (lanes(wide.shape) < HEAD_DIM)
    return jnp.where(keep, wide, jnp.zeros_like(wide))


class Relay:
    def __init__(self, n_ctx, src, dst, send, recv):
        self.src, self.dst, self.send, self.recv = src, dst, send, recv
        self.piece = src.shape[0] // n_ctx
        self.ctx = lax.axis_index("ctx")
        self.bits = high_bits(n_ctx)
        self.count = 0
        self.all = []
        self.last = []

    def _copy(self, src, dst, axis, bit):
        e = self.count
        self.count += 1
        copy = pltpu.make_async_remote_copy(
            src_ref=src,
            dst_ref=dst,
            send_sem=self.send.at[e],
            recv_sem=self.recv.at[e],
            device_id={axis: lax.axis_index(axis) ^ bit},
            device_id_type=MESH,
        )
        copy.start()
        self.all.append(copy)
        return copy

    def _cut(self, which):
        return pl.ds(pl.multiple_of(which * self.piece, self.piece), self.piece)

    def start(self):
        mine = self._cut(self.ctx)
        self.last = [self._copy(self.src.at[mine], self.dst.at[mine], "fsdp", 1)]

    def hop(self, j):
        self.landed()
        bit = self.bits[j]
        parts = [self.dst.at[self._cut(self.ctx ^ m)] for m in masks_of(self.bits[:j])]
        self.last = [self._copy(part, part, "ctx", bit) for part in parts]

    def landed(self):
        for copy in self.last:
            copy.wait_recv()
        self.last = []

    def drain(self):
        for copy in self.all:
            copy.wait_send()


def forward_kernel(
    n_ctx,
    n_head,
    span,
    q_ref,
    p_ref,
    wl_ref,
    wr_ref,
    gate_ref,
    up_ref,
    down_ref,
    o_ref,
    lse_ref,
    sum_ref,
    gate_other,
    up_other,
    down_other,
    q_pad,
    ext,
    max_ref,
    acc_ref,
    relay_send,
    relay_recv,
    left,
    right,
    from_lo,
    from_hi,
    *sems,
):
    rows, width = q_ref.shape
    heads = width // HEAD_DIM
    block = lax.axis_index("ctx") * 2 + lax.axis_index("fsdp")
    barrier = line_greet(n_head)
    greet(n_ctx)
    ext[...] = jnp.where(lanes(p_ref.shape) < HEAD_DIM, jnp.ones_like(p_ref[...]), p_ref[...])
    pl.semaphore_wait(barrier, line_peers(n_head) + len(partners(n_ctx)))
    gate = Relay(n_ctx, gate_ref, gate_other, relay_send.at[0], relay_recv.at[0])
    up = Relay(n_ctx, up_ref, up_other, relay_send.at[1], relay_recv.at[1])
    down = Relay(n_ctx, down_ref, down_other, relay_send.at[2], relay_recv.at[2])
    gate.start()
    up.start()
    down.hop(0)
    step, steps, drain = line_sum(n_head, left, right, left, right, sum_ref, from_lo, from_hi, sems)
    size = rows // GROUPS
    stack = heads * size
    sub = min(512, stack)
    per_group = CHUNKS // GROUPS

    def tile(start, first_row, masked):
        cut = pl.ds(start, span)
        for j in range(stack // sub):
            part = pl.ds(j * sub, sub)
            scores = mat_trans(q_pad[part, :], p_ref[cut, :])
            if masked:
                row = first_row + lax.rem(lax.broadcasted_iota(jnp.int32, (sub, span), 0), size)
                col = start + lax.broadcasted_iota(jnp.int32, (sub, span), 1)
                scores = jnp.where(col <= row, scores, NEG)
            old = max_ref[part, :]
            new = jnp.maximum(old, jnp.max(scores, axis=1, keepdims=True))
            weights = jnp.exp(scores - jnp.tile(new, (1, span // 128))).astype(BF)
            acc_ref[part, :] = acc_ref[part, :] * jnp.exp(old - new) + matmul(weights, ext[cut, :])
            max_ref[part, :] = new

    def run(s, carry):
        step(s)
        return carry

    def one_group(g, carry):
        mine = pl.ds(pl.multiple_of(g * size, size), size)
        first_row = block * rows + g * size
        for h in range(heads):
            q_pad[h * size : (h + 1) * size, :] = head_lanes(q_ref.at[mine], h, False)
        max_ref[...] = jnp.full_like(max_ref, NEG)
        acc_ref[...] = jnp.zeros_like(acc_ref)

        tiles = (block + 1) * (rows // span)
        base = (g - 1) * per_group

        def sums(i):
            lax.fori_loop((i * per_group) // tiles, ((i + 1) * per_group) // tiles, lambda j, c: run(base + j, c), 0)

        def full(i, c):
            sums(i)
            tile(pl.multiple_of(i * span, span), first_row, False)
            return c

        lax.fori_loop(0, block * (rows // span), full, 0)
        for j in range(rows // span):
            sums(block * (rows // span) + j)
            tile(pl.multiple_of(block * rows + j * span, span), first_row, True)
        for h in range(heads):
            acc = acc_ref[h * size : (h + 1) * size, :]
            total = acc[:, :HEAD_DIM]
            o_ref[mine, h * HEAD_DIM : (h + 1) * HEAD_DIM] = (acc[:, HEAD_DIM:] / total).astype(BF)
            lse = max_ref[h * size : (h + 1) * size, :] + jnp.log(jnp.concatenate([total, total], axis=1))
            lse_ref[h, :, mine] = lse.T[0:1, :]
        att = o_ref[mine, :]
        left[mine, :] = matmul(att, wl_ref[...]).astype(BF)
        right[mine, :] = matmul(att, wr_ref[...]).astype(BF)
        return carry

    lax.fori_loop(0, GROUPS - 1, one_group, 0)
    gate.hop(0)
    down.hop(1)
    lax.fori_loop(GROUPS - 1, GROUPS, one_group, 0)
    hops = len(high_bits(n_ctx))
    later = [(down, j) for j in range(2, hops)] + [(gate, 1), (up, 0)]
    for j in range(1, hops):
        later += [(up, j)] + ([(gate, j + 1)] if j + 1 < hops else [])
    at = CHUNKS - per_group
    rest = steps - at
    for i, (relay, j) in enumerate(later):
        to = CHUNKS - per_group + (rest * (2 * i + 1)) // (2 * len(later))
        lax.fori_loop(at, to, run, 0)
        at = to
        relay.hop(j)
    lax.fori_loop(at, steps, run, 0)
    for relay in (gate, up, down):
        relay.landed()
        relay.drain()
    drain()


def attend_sum(queries, pair, out_left, out_right, gate, up, down, n_ctx, n_head, collective_id):
    rows, width = queries.shape
    heads = width // HEAD_DIM
    seq = pair.shape[0]
    span = min(512, rows)
    wide = 2 * out_left.shape[1]
    vmem = pl.BlockSpec(memory_space=pltpu.VMEM)
    anywhere = pl.BlockSpec(memory_space=pl.ANY)
    stack = heads * rows // GROUPS
    cost = pl.CostEstimate(flops=50_000_000_000, bytes_accessed=8 * rows * wide, transcendentals=0)
    return pl.pallas_call(
        functools.partial(forward_kernel, n_ctx, n_head, span),
        out_shape=(
            jax.ShapeDtypeStruct((rows, width), BF),
            jax.ShapeDtypeStruct((heads, 1, rows), F32),
            jax.ShapeDtypeStruct((rows, wide), BF),
            jax.ShapeDtypeStruct(gate.shape, BF),
            jax.ShapeDtypeStruct(up.shape, BF),
            jax.ShapeDtypeStruct(down.shape, BF),
        ),
        input_output_aliases={6: 5},
        in_specs=[vmem] * 4 + [anywhere] * 3,
        out_specs=(vmem, vmem, vmem, anywhere, anywhere, anywhere),
        scratch_shapes=[
            pltpu.VMEM((stack, 128), BF),
            pltpu.VMEM((seq, 128), BF),
            pltpu.VMEM((stack, 128), F32),
            pltpu.VMEM((stack, 128), F32),
            pltpu.SemaphoreType.DMA((3, n_ctx)),
            pltpu.SemaphoreType.DMA((3, n_ctx)),
        ]
        + line_scratch(rows, wide),
        compiler_params=pltpu.CompilerParams(collective_id=collective_id, has_side_effects=True),
        cost_estimate=cost,
        name="attend_sum",
    )(queries, pair, out_left, out_right, gate, up, down)


def backward_kernel(
    n_head,
    group,
    span,
    q_ref,
    g_ref,
    o_ref,
    lse_ref,
    p_ref,
    left_ref,
    right_ref,
    dq_ref,
    dp_ref,
    sum_ref,
    q_pad,
    g_pad,
    acc_ref,
    dl_ref,
    work_l,
    work_r,
    from_lo,
    from_hi,
    *sems,
):
    rows, width = q_ref.shape
    heads = width // HEAD_DIM
    tiles = rows // span
    block = lax.axis_index("ctx") * 2 + lax.axis_index("fsdp")
    barrier = line_greet(n_head)
    dp_ref[...] = jnp.zeros_like(dp_ref)
    acc_ref[...] = jnp.zeros_like(acc_ref)
    for h in range(heads):
        cut = slice(h * HEAD_DIM, (h + 1) * HEAD_DIM)
        q_pad[h] = head_lanes(q_ref, h, False)
        g_pad[h] = head_lanes(g_ref, h, True)
        product = g_ref[:, cut].astype(F32) * o_ref[:, cut].astype(F32)
        dl_ref[h] = jnp.sum(product.T, axis=0, keepdims=True)
    pl.semaphore_wait(barrier, line_peers(n_head))
    step, steps, drain = line_sum(
        n_head, left_ref, right_ref, work_l, work_r, sum_ref, from_lo, from_hi, sems
    )

    def head_tile(h, pairs, start, masked):
        probs = jnp.exp(mat_trans(pairs, q_pad[h]) - lse_ref[h])
        if masked:
            row = block * rows + lax.broadcasted_iota(jnp.int32, (span, rows), 1)
            col = start + lax.broadcasted_iota(jnp.int32, (span, rows), 0)
            probs = jnp.where(col <= row, probs, 0.0)
        grads = (probs * (mat_trans(pairs, g_pad[h]) - dl_ref[h])).astype(BF)
        acc_ref[h] += trans_mat(grads, pairs)
        return matmul(probs.astype(BF), g_pad[h]) + matmul(grads, q_pad[h])

    groups = heads // group

    def two_steps(t):
        for j in range(2):

            @pl.when(2 * t + j < steps)
            def _():
                step(2 * t + j)

    def full(t, carry):
        two_steps(t)
        first = lax.rem(t, groups) * group
        start = pl.multiple_of((t // groups) * span, span)
        cut = pl.ds(start, span)
        total = head_tile(first, p_ref[cut, :], start, False)
        for h in range(1, group):
            total = total + head_tile(first + h, p_ref[cut, :], start, False)
        dp_ref[cut, :] += total
        return carry

    count = block * tiles * groups
    lax.fori_loop(0, count, full, 0)

    def last(t, carry):
        h = lax.rem(t, heads)

        @pl.when(lax.rem(t, group) == 0)
        def _():
            two_steps(count + t // group)

        start = pl.multiple_of(block * rows + (t // heads) * span, span)
        cut = pl.ds(start, span)
        dp_ref[cut, :] += head_tile(h, p_ref[cut, :], start, True)
        return carry

    lax.fori_loop(0, heads * tiles, last, 0)
    for h in range(heads):
        dq_ref[:, h * HEAD_DIM : (h + 1) * HEAD_DIM] = acc_ref[h][:, :HEAD_DIM]

    def rest(s, carry):
        step(s)
        return carry

    lax.fori_loop(jnp.minimum(2 * (count + groups * tiles), steps), steps, rest, 0)
    drain()


def attend_back(queries, grads, attended, lse, pair, left, right, n_head, collective_id):
    rows, width = queries.shape
    heads = width // HEAD_DIM
    seq = pair.shape[0]
    group = 4 if heads % 4 == 0 else 2
    span = min(512, rows)
    vmem = pl.BlockSpec(memory_space=pltpu.VMEM)
    cost = pl.CostEstimate(
        flops=32 * rows * seq * width, bytes_accessed=8 * rows * width, transcendentals=0
    )
    return pl.pallas_call(
        functools.partial(backward_kernel, n_head, group, span),
        out_shape=(
            jax.ShapeDtypeStruct((rows, width), F32),
            jax.ShapeDtypeStruct((seq, 2 * HEAD_DIM), F32),
            jax.ShapeDtypeStruct((rows, 2 * left.shape[1]), BF),
        ),
        in_specs=[vmem] * 7,
        out_specs=(vmem, vmem, vmem),
        scratch_shapes=[
            pltpu.VMEM((heads, rows, 128), BF),
            pltpu.VMEM((heads, rows, 128), BF),
            pltpu.VMEM((heads, rows, 128), F32),
            pltpu.VMEM((heads, 1, rows), F32),
        ]
        + line_scratch(rows, 2 * left.shape[1]),
        compiler_params=pltpu.CompilerParams(collective_id=collective_id, has_side_effects=True),
        cost_estimate=cost,
        name="attend_backward",
    )(queries, grads, attended, lse, pair, left, right)


def partners(n_ctx):
    return [("fsdp", 1)] + [("ctx", bit) for bit in high_bits(n_ctx)]


def greet(n_ctx):
    barrier = pltpu.get_barrier_semaphore()
    for axis, bit in partners(n_ctx):
        pl.semaphore_signal(
            barrier, inc=1, device_id={axis: lax.axis_index(axis) ^ bit}, device_id_type=MESH
        )
    return barrier


def masks_of(bits):
    masks = [0]
    for bit in bits:
        masks = masks + [m | bit for m in masks]
    return masks


def gather_pairs(n_ctx, rows, all_ref, send, recv):
    x = lax.axis_index("fsdp")
    ctx = lax.axis_index("ctx")
    copies = []

    def part(start, size, axis, bit):
        e = len(copies)
        cut = all_ref.at[pl.ds(pl.multiple_of(start, rows), size)]
        copy = pltpu.make_async_remote_copy(
            src_ref=cut,
            dst_ref=cut,
            send_sem=send.at[e],
            recv_sem=recv.at[e],
            device_id={axis: lax.axis_index(axis) ^ bit},
            device_id_type=MESH,
        )
        copy.start()
        copies.append(copy)
        return copy

    opening = part((ctx * 2 + x) * rows, rows, "fsdp", 1)

    def finish():
        opening.wait_recv()
        done = []
        for bit in high_bits(n_ctx):
            now = [part((ctx ^ m) * 2 * rows, 2 * rows, "ctx", bit) for m in masks_of(done)]
            for copy in now:
                copy.wait_recv()
            done.append(bit)
        for copy in copies:
            copy.wait_send()

    return finish


def scatter_kernel(n_ctx, part_ref, o_ref, work, land, send, recv):
    rows = o_ref.shape[0]
    x = lax.axis_index("fsdp")
    ctx = lax.axis_index("ctx")
    barrier = greet(n_ctx)
    work[...] = part_ref[...].astype(BF)
    pl.semaphore_wait(barrier, len(partners(n_ctx)))
    copies = []
    used = [0]

    def give(start, size, axis, bit):
        e = len(copies)
        cut = pl.ds(pl.multiple_of(start, rows), size)
        copy = pltpu.make_async_remote_copy(
            src_ref=work.at[cut],
            dst_ref=land.at[pl.ds(used[0], size)],
            send_sem=send.at[e],
            recv_sem=recv.at[e],
            device_id={axis: lax.axis_index(axis) ^ bit},
            device_id_type=MESH,
        )
        copy.start()
        copies.append(copy)
        used[0] += size
        return copy, used[0] - size

    def take(start, size, at):
        cut = pl.ds(pl.multiple_of(start, rows), size)
        work[cut, :] = (work[cut, :].astype(F32) + land[at : at + size, :].astype(F32)).astype(BF)

    bits = high_bits(n_ctx)
    for j in range(len(bits)):
        bit = bits[len(bits) - 1 - j]
        masks = masks_of(bits[: len(bits) - 1 - j])
        now = [give((ctx ^ bit ^ m) * 2 * rows, 2 * rows, "ctx", bit) for m in masks]
        for (copy, at), m in zip(now, masks):
            copy.wait_recv()
            take((ctx ^ m) * 2 * rows, 2 * rows, at)
    copy, at = give((ctx * 2 + 1 - x) * rows, rows, "fsdp", 1)
    copy.wait_recv()
    mine = pl.ds(pl.multiple_of((ctx * 2 + x) * rows, rows), rows)
    o_ref[...] = work[mine, :].astype(F32) + land[at : at + rows, :].astype(F32)
    for copy in copies:
        copy.wait_send()


def scatter_pairs(part, rows, n_ctx, collective_id):
    vmem = pl.BlockSpec(memory_space=pltpu.VMEM)
    return pl.pallas_call(
        functools.partial(scatter_kernel, n_ctx),
        out_shape=jax.ShapeDtypeStruct((rows, part.shape[1]), F32),
        in_specs=[vmem],
        out_specs=vmem,
        scratch_shapes=[
            pltpu.VMEM(part.shape, BF),
            pltpu.VMEM(part.shape, BF),
            pltpu.SemaphoreType.DMA((n_ctx,)),
            pltpu.SemaphoreType.DMA((n_ctx,)),
        ],
        compiler_params=pltpu.CompilerParams(collective_id=collective_id, has_side_effects=True),
        name="scatter_pairs",
    )(part)


def project_kernel(
    n_ctx,
    x_ref,
    w_ref,
    gain_ref,
    cos_ref,
    sin_ref,
    wo_ref,
    down_ref,
    q_ref,
    p_ref,
    n_ref,
    w_other,
    gain_other,
    wo_other,
    down_other,
    acc_ref,
    send,
    recv,
    relay_send,
    relay_recv,
    gain_send,
    gain_recv,
):
    rows, width = x_ref.shape
    half = width // 2
    q_width = q_ref.shape[1]
    x_at = lax.axis_index("fsdp")
    block = lax.axis_index("ctx") * 2 + x_at
    barrier = greet(n_ctx)
    pl.semaphore_wait(barrier, len(partners(n_ctx)))
    gains = pltpu.make_async_remote_copy(
        src_ref=gain_ref,
        dst_ref=gain_other,
        send_sem=gain_send,
        recv_sem=gain_recv,
        device_id={"fsdp": 1 - x_at},
        device_id_type=MESH,
    )
    gains.start()
    part = half // 2
    first = [
        Relay(
            n_ctx,
            w_ref.at[pl.ds(i * part, part)],
            w_other.at[pl.ds(i * part, part)],
            relay_send.at[i],
            relay_recv.at[i],
        )
        for i in range(2)
    ]
    second = Relay(n_ctx, wo_ref, wo_other, relay_send.at[2], relay_recv.at[2])
    third = Relay(n_ctx, down_ref, down_other, relay_send.at[3], relay_recv.at[3])
    for relay in first:
        relay.start()
    second.start()
    gains.wait_recv()
    parts = 8
    size = rows // parts
    own = pl.ds(pl.multiple_of(x_at * half, half), half)
    other = pl.ds(pl.multiple_of((1 - x_at) * half, half), half)

    def cut_of(i):
        return pl.ds(pl.multiple_of(i * size, size), size)

    def norm(i, carry):
        cut = cut_of(i)
        left = x_ref[cut, own].astype(F32)
        right = x_ref[cut, other].astype(F32)
        total = jnp.sum(left * left, axis=1, keepdims=True) + jnp.sum(right * right, axis=1, keepdims=True)
        scale = lax.rsqrt(total / width + EPSILON)
        n_ref[cut, :half] = (left * scale * gain_ref[0:1, :]).astype(BF)
        n_ref[cut, half:] = (right * scale * gain_other[0:1, :]).astype(BF)
        return carry

    lax.fori_loop(0, parts, norm, 0)
    for relay in first:
        relay.hop(0)
    third.start()
    second.hop(0)

    def local(i, carry):
        cut = cut_of(i)
        acc_ref[cut, :] = matmul(n_ref[cut, :half], w_ref[...])
        return carry

    lax.fori_loop(0, parts, local, 0)
    for j in range(1, len(high_bits(n_ctx))):
        for relay in first:
            relay.hop(j)
    for relay in first:
        relay.landed()

    def rotated(wide, cut):
        low = lax.rem(lanes(wide.shape), HEAD_DIM) < HEAD_DIM // 2
        turned = jnp.where(low, pltpu.roll(wide, 128 - HEAD_DIM // 2, 1), pltpu.roll(wide, HEAD_DIM // 2, 1))
        return wide * cos_ref[cut, :] + turned * sin_ref[cut, :]

    def pairs(i, carry):
        cut = cut_of(i)
        both = acc_ref[cut, q_width:] + matmul(n_ref[cut, half:], w_other[:, q_width:])
        pair = jnp.where(lanes(both.shape) < HEAD_DIM, rotated(both, cut), both)
        p_ref[pl.ds(pl.multiple_of(block * rows + i * size, size), size), :] = pair.astype(BF)
        return carry

    def queries(i, carry):
        cut = cut_of(i)
        whole = acc_ref[cut, :q_width] + matmul(n_ref[cut, half:], w_other[:, :q_width])
        for j in range(q_width // 128):
            sl = slice(j * 128, (j + 1) * 128)
            q_ref[cut, sl] = (rotated(whole[:, sl], cut) * 0.125).astype(BF)
        return carry

    lax.fori_loop(0, parts, pairs, 0)
    finish = gather_pairs(n_ctx, rows, p_ref, send, recv)
    lax.fori_loop(0, parts, queries, 0)
    finish()
    for j in range(1, len(high_bits(n_ctx))):
        second.hop(j)
    second.landed()
    third.landed()
    for relay in first + [second, third]:
        relay.drain()
    gains.wait_send()


def project(inputs, w_local, gains, cosine, sine, w_out, w_down, q_width, n_ctx, collective_id):
    rows, width = inputs.shape
    vmem = pl.BlockSpec(memory_space=pltpu.VMEM)
    anywhere = pl.BlockSpec(memory_space=pl.ANY)
    return pl.pallas_call(
        functools.partial(project_kernel, n_ctx),
        out_shape=(
            jax.ShapeDtypeStruct((rows, q_width), BF),
            jax.ShapeDtypeStruct((rows * 2 * n_ctx, 2 * HEAD_DIM), BF),
            jax.ShapeDtypeStruct((rows, width), BF),
            jax.ShapeDtypeStruct(w_local.shape, BF),
            jax.ShapeDtypeStruct(gains.shape, F32),
            jax.ShapeDtypeStruct(w_out.shape, BF),
            jax.ShapeDtypeStruct(w_down.shape, BF),
        ),
        in_specs=[vmem] * 5 + [anywhere] * 2,
        out_specs=(vmem,) * 5 + (anywhere,) * 2,
        scratch_shapes=[
            pltpu.VMEM((rows, w_local.shape[1]), F32),
            pltpu.SemaphoreType.DMA((n_ctx,)),
            pltpu.SemaphoreType.DMA((n_ctx,)),
            pltpu.SemaphoreType.DMA((4, n_ctx)),
            pltpu.SemaphoreType.DMA((4, n_ctx)),
            pltpu.SemaphoreType.DMA,
            pltpu.SemaphoreType.DMA,
        ],
        compiler_params=pltpu.CompilerParams(collective_id=collective_id, has_side_effects=True),
        name="project",
    )(inputs, w_local, gains, cosine, sine, w_out, w_down)


def line_sum(n, left, right, work_l, work_r, o_ref, from_lo, from_hi, sems):
    s_up, r_up, s_dn, r_dn, s_a, r_a, s_b, r_b = sems
    me = lax.axis_index("head")
    rows, cols = left.shape
    size = rows // CHUNKS
    has_lo = me > 0
    has_hi = me < n - 1
    middle = jnp.logical_and(has_lo, has_hi)

    def at(k):
        return pl.ds(pl.multiple_of(k * size, size), size)

    def remote(src, dst, send, recv, target):
        return pltpu.make_async_remote_copy(
            src_ref=src,
            dst_ref=dst,
            send_sem=send,
            recv_sem=recv,
            device_id={"head": target},
            device_id_type=MESH,
        )

    def up(k, src):
        return remote(src.at[at(k)], from_lo.at[at(k)], s_up.at[k], r_up.at[k], me + 1)

    def down(k, src):
        return remote(src.at[at(k)], from_hi.at[at(k)], s_dn.at[k], r_dn.at[k], me - 1)

    def spread_a(k):
        part = o_ref.at[at(k), pl.ds(0, cols)]
        return remote(part, part, s_a.at[k], r_a.at[k], me + 1)

    def spread_b(k):
        part = o_ref.at[at(k), pl.ds(cols, cols)]
        return remote(part, part, s_b.at[k], r_b.at[k], me - 1)

    def valid(k):
        return jnp.logical_and(k >= 0, k < CHUNKS)

    def added(mine, there, k):
        return (mine[at(k), :].astype(F32) + there[at(k), :].astype(F32)).astype(BF)

    def step(s):
        k1 = s - LAG * me
        k2 = s - LAG * (n - 1 - me)
        k3 = s - LAG * (n - 1 + me)
        k4 = s - LAG * (2 * (n - 1) - me)

        @pl.when(jnp.logical_and(valid(k1), me == 0))
        def _():
            up(k1, right).start()

        @pl.when(jnp.logical_and(valid(k2), me == n - 1))
        def _():
            down(k2, left).start()

        @pl.when(jnp.logical_and(valid(k1), middle))
        def _():
            up(k1, right).wait_recv()
            work_r[at(k1), :] = added(right, from_lo, k1)
            up(k1, work_r).start()

        @pl.when(jnp.logical_and(valid(k1), me == n - 1))
        def _():
            up(k1, right).wait_recv()
            o_ref[at(k1), cols:] = added(right, from_lo, k1)
            spread_b(k1).start()

        @pl.when(jnp.logical_and(valid(k2), middle))
        def _():
            down(k2, left).wait_recv()
            work_l[at(k2), :] = added(left, from_hi, k2)
            down(k2, work_l).start()

        @pl.when(jnp.logical_and(valid(k2), me == 0))
        def _():
            down(k2, left).wait_recv()
            o_ref[at(k2), :cols] = added(left, from_hi, k2)
            spread_a(k2).start()

        @pl.when(jnp.logical_and(valid(k3), has_lo))
        def _():
            spread_a(k3).wait_recv()

            @pl.when(has_hi)
            def _():
                spread_a(k3).start()

        @pl.when(jnp.logical_and(valid(k4), has_hi))
        def _():
            spread_b(k4).wait_recv()

            @pl.when(has_lo)
            def _():
                spread_b(k4).start()

    def drain():
        def one(k, carry):
            @pl.when(has_hi)
            def _():
                up(k, right).wait_send()
                spread_a(k).wait_send()

            @pl.when(has_lo)
            def _():
                down(k, left).wait_send()
                spread_b(k).wait_send()

            return carry

        lax.fori_loop(0, CHUNKS, one, 0)

    return step, CHUNKS + 2 * LAG * (n - 1), drain


def line_greet(n):
    me = lax.axis_index("head")
    barrier = pltpu.get_barrier_semaphore()

    @pl.when(me > 0)
    def _():
        pl.semaphore_signal(barrier, inc=1, device_id={"head": me - 1}, device_id_type=MESH)

    @pl.when(me < n - 1)
    def _():
        pl.semaphore_signal(barrier, inc=1, device_id={"head": me + 1}, device_id_type=MESH)

    return barrier


def line_peers(n):
    me = lax.axis_index("head")
    return jnp.where(me > 0, 1, 0) + jnp.where(me < n - 1, 1, 0)


def line_scratch(rows, width):
    return [pltpu.VMEM((rows, width // 2), BF)] * 4 + [pltpu.SemaphoreType.DMA((CHUNKS,))] * 8


def head_sum_kernel(n, left_ref, right_ref, o_ref, work_l, work_r, from_lo, from_hi, *sems):
    barrier = line_greet(n)
    pl.semaphore_wait(barrier, line_peers(n))
    step, steps, drain = line_sum(n, left_ref, right_ref, work_l, work_r, o_ref, from_lo, from_hi, sems)

    def run(s, carry):
        step(s)
        return carry

    lax.fori_loop(0, steps, run, 0)
    drain()


def head_sum(left, right, n, collective_id):
    rows, cols = left.shape
    return pl.pallas_call(
        functools.partial(head_sum_kernel, n),
        out_shape=jax.ShapeDtypeStruct((rows, 2 * cols), BF),
        in_specs=[pl.BlockSpec(memory_space=pltpu.VMEM)] * 2,
        out_specs=pl.BlockSpec(memory_space=pltpu.VMEM),
        scratch_shapes=line_scratch(rows, 2 * cols),
        compiler_params=pltpu.CompilerParams(collective_id=collective_id, has_side_effects=True),
        cost_estimate=pl.CostEstimate(
            flops=40_000_000_000, bytes_accessed=8 * rows * cols, transcendentals=0
        ),
        name="head_sum",
    )(left, right)


def flip(array, axis, bit, size):
    return lax.ppermute(array, axis, [(i, i ^ bit) for i in range(size)])


def shards(
    n_ctx,
    n_head,
    inputs,
    query_weight,
    key_weight,
    value_weight,
    output_weight,
    gate_weight,
    up_weight,
    down_weight,
    attn_gain,
    ffn_gain,
    cotangent,
):
    rows, width = inputs.shape
    half = width // 2
    quarter = half // 2
    x_at = lax.axis_index("fsdp")
    ctx_at = lax.axis_index("ctx")
    core = lax.rem(ctx_at, 2)
    block = ctx_at * 2 + x_at
    block_arr = jnp.reshape(block, (1,)).astype(jnp.int32)

    def own_first(array):
        swapped = jnp.concatenate([array[:, half:], array[:, :half]], axis=1)
        return jnp.where(x_at == 0, array, swapped)

    every = high_bits(n_ctx)

    def columns_of(array, which):
        first = jnp.concatenate([array[:, :quarter], array[:, half : half + quarter]], axis=1)
        second = jnp.concatenate([array[:, quarter:half], array[:, half + quarter :]], axis=1)
        return jnp.where(which == 0, first, second)

    def trade(array):
        return jnp.concatenate([array, flip(array, "ctx", 1, n_ctx)], axis=0)

    def trade_columns(array):
        got = flip(columns_of(array, 1 - core), "ctx", 1, n_ctx)
        return jnp.concatenate([columns_of(array, core), got], axis=0)

    q_width = query_weight.shape[1]
    half_dim = HEAD_DIM // 2
    positions = block * rows + jnp.arange(rows, dtype=jnp.int32)
    lane = lax.broadcasted_iota(jnp.int32, (rows, 2 * HEAD_DIM), 1)
    freqs = 10000.0 ** (-2.0 * (lane % half_dim).astype(F32) / HEAD_DIM)
    angles = positions.astype(F32)[:, None] * freqs
    cosine = jnp.cos(angles)
    sine = jnp.sin(angles)
    signed = jnp.where(lane % HEAD_DIM < half_dim, -sine, sine)
    qkv_local = jnp.concatenate([query_weight, key_weight, value_weight], axis=1)
    gains_local = jnp.concatenate([attn_gain[None], ffn_gain[None], jnp.zeros((6, half), BF)]).astype(F32)
    queries, pair, normed_one, qkv_other, gains_other, out_other, down_begun = project(
        inputs, qkv_local, gains_local, cosine, signed, output_weight, down_weight, q_width, n_ctx, 4
    )
    attended, lse, mixed, gate_other, up_other, down_other = attend_sum(
        queries, pair, output_weight, out_other, gate_weight, up_weight, down_begun, n_ctx, n_head, 1
    )
    gain_one = jnp.concatenate([gains_local[0], gains_other[0]])
    gain_two = jnp.concatenate([gains_local[1], gains_other[1]])
    late_inputs, late_cot, normed_one, mixed = lax.optimization_barrier(
        (inputs, cotangent, normed_one, mixed)
    )
    in_float = own_first(late_inputs).astype(F32)
    cot = own_first(late_cot)
    scale_one = lax.rsqrt(jnp.mean(in_float * in_float, axis=-1, keepdims=True) + EPSILON)
    unit_one = in_float * scale_one
    one_pair = trade_columns(normed_one)

    hidden = in_float + mixed.astype(F32)
    scale_two = lax.rsqrt(jnp.mean(hidden * hidden, axis=-1, keepdims=True) + EPSILON)
    unit_two = hidden * scale_two
    normed_two = (unit_two * gain_two).astype(BF)

    act_grad = mat_trans(cot[:, :half], down_weight) + mat_trans(cot[:, half:], down_other)
    gate_pre = matmul(normed_two[:, :half], gate_weight) + matmul(normed_two[:, half:], gate_other)
    up_pre = matmul(normed_two[:, :half], up_weight) + matmul(normed_two[:, half:], up_other)
    sigma = jax.nn.sigmoid(gate_pre)
    silu_gate = gate_pre * sigma
    activated = (silu_gate * up_pre).astype(BF)
    gate_in_grad = (act_grad * up_pre * sigma * (1.0 + gate_pre * (1.0 - sigma))).astype(BF)
    up_in_grad = (act_grad * silu_gate).astype(BF)
    low_left = (mat_trans(gate_in_grad, gate_weight) + mat_trans(up_in_grad, up_weight)).astype(BF)
    low_right = (mat_trans(gate_in_grad, gate_other) + mat_trans(up_in_grad, up_other)).astype(BF)
    cot_pair = trade_columns(cot)
    two_pair = trade_columns(normed_two)
    down_part = trans_mat(trade(activated), cot_pair).astype(BF)
    gate_part = trans_mat(two_pair, trade(gate_in_grad)).astype(BF)
    low_left, low_right, down_part, gate_part = lax.optimization_barrier(
        (low_left, low_right, down_part, gate_part)
    )
    normed_two_grad = head_sum(low_left, low_right, n_head, 2).astype(F32)
    up_part = trans_mat(two_pair, trade(up_in_grad)).astype(BF)
    scaled_two = normed_two_grad * gain_two
    gain_two_part = jnp.sum(normed_two_grad * unit_two, axis=0)
    hidden_grad = cot.astype(F32) + scale_two * (
        scaled_two - unit_two * jnp.mean(scaled_two * unit_two, axis=-1, keepdims=True)
    )
    hidden_low = hidden_grad.astype(BF)

    down_left = matmul(activated, down_weight).astype(BF)
    down_right = matmul(activated, down_other).astype(BF)
    attended_grad = (
        mat_trans(hidden_low[:, :half], output_weight) + mat_trans(hidden_low[:, half:], out_other)
    ).astype(BF)
    out_part = trans_mat(trade(attended), trade_columns(hidden_low)).astype(BF)
    attended_grad, up_part, out_part = lax.optimization_barrier((attended_grad, up_part, out_part))
    query_acc, pair_acc, ffn_out = attend_back(
        queries, attended_grad, attended, lse, pair, down_left, down_right, n_head, 6
    )
    outputs = own_first((hidden + ffn_out.astype(F32)).astype(BF))
    pair_mine = scatter_pairs(pair_acc, rows, n_ctx, 5)

    def unrotate(values):
        count = values.shape[1] // 128
        cos = jnp.concatenate([cosine] * count, axis=1)
        sin = jnp.concatenate([signed] * count, axis=1)
        low = lax.broadcasted_iota(jnp.int32, values.shape, 1) % HEAD_DIM < half_dim
        turned = jnp.where(low, jnp.roll(values, -half_dim, axis=1), jnp.roll(values, half_dim, axis=1))
        return values * cos - turned * sin

    q_raw = unrotate(query_acc * 0.125)
    pair_raw = jnp.where(lane < HEAD_DIM, unrotate(pair_mine), pair_mine)
    qkv_raw = jnp.concatenate([q_raw, pair_raw], axis=1).astype(BF)
    last_left = mat_trans(qkv_raw, qkv_local).astype(BF)
    last_right = mat_trans(qkv_raw, qkv_other).astype(BF)
    qkv_part = trans_mat(one_pair, trade(qkv_raw)).astype(BF)
    last_left, last_right, qkv_part = lax.optimization_barrier((last_left, last_right, qkv_part))
    normed_one_grad = head_sum(last_left, last_right, n_head, 3).astype(F32)
    gain_one_part = jnp.sum(normed_one_grad * unit_one, axis=0)
    scaled_one = normed_one_grad * gain_one
    input_grad = own_first(
        hidden_grad
        + scale_one
        * (scaled_one - unit_one * jnp.mean(scaled_one * unit_one, axis=-1, keepdims=True))
    )

    def total(kept, sent):
        kept = (kept.astype(F32) + flip(sent, "fsdp", 1, 2).astype(F32)).astype(BF)
        for bit in every[:-1]:
            kept = (kept.astype(F32) + flip(kept, "ctx", bit, n_ctx).astype(F32)).astype(BF)
        return kept

    def spread(kept, dim):
        got = flip(kept, "ctx", 1, n_ctx)
        first = jnp.where(core == 0, kept, got)
        second = jnp.where(core == 0, got, kept)
        return jnp.concatenate([first, second], axis=dim).astype(F32)

    def by_rows(part):
        return spread(total(part[:quarter], part[quarter:]), 0)

    def by_columns(part):
        return spread(total(part[:, :quarter], part[:, quarter:]), 1)

    down_grad = by_columns(down_part)
    gate_grad = by_rows(gate_part)
    up_grad = by_rows(up_part)
    output_grad = by_columns(out_part)
    qkv_grad = by_rows(qkv_part)
    query_grad = qkv_grad[:, :q_width]
    key_grad = qkv_grad[:, q_width : q_width + HEAD_DIM]
    value_grad = qkv_grad[:, q_width + HEAD_DIM :]

    def gain_total(part):
        kept = part[:half].reshape(8, -1) + flip(part[half:].reshape(8, -1), "fsdp", 1, 2)
        for bit in every:
            kept = kept + flip(kept, "ctx", bit, n_ctx)
        return kept.reshape(half)

    return (
        outputs,
        input_grad,
        query_grad,
        key_grad,
        value_grad,
        output_grad,
        gate_grad,
        up_grad,
        down_grad,
        gain_total(gain_one_part),
        gain_total(gain_two_part),
    )


def solution(mesh):
    n_ctx = mesh.shape["ctx"]

    def body(*args):
        return shards(n_ctx, mesh.shape["head"], *args)

    return jax.shard_map(
        body,
        mesh=mesh,
        in_specs=(
            P(("ctx", "fsdp"), None),
            P("fsdp", "head"),
            P("fsdp", "head"),
            P("fsdp", "head"),
            P("head", "fsdp"),
            P("fsdp", "head"),
            P("fsdp", "head"),
            P("head", "fsdp"),
            P("fsdp"),
            P("fsdp"),
            P(("ctx", "fsdp"), None),
        ),
        out_specs=(
            P(("ctx", "fsdp"), None),
            P(("ctx", "fsdp"), None),
            P("fsdp", "head"),
            P("fsdp", "head"),
            P("fsdp", "head"),
            P("head", "fsdp"),
            P("fsdp", "head"),
            P("fsdp", "head"),
            P("head", "fsdp"),
            P("fsdp"),
            P("fsdp"),
        ),
        check_vma=False,
    )
```

```python
import functools

import jax
import jax.numpy as jnp
from jax import lax
from jax.experimental import pallas as pl
from jax.experimental.pallas import tpu as pltpu
from jax.sharding import PartitionSpec as P


HEAD_DIM = 64
EPSILON = 1e-05
NEG = -1e30
BF = jnp.bfloat16
F32 = jnp.float32
MESH = pl.DeviceIdType.MESH
CHUNKS = 16
LAG = 3
GROUPS = 4
FFN_GROUPS = 2


def matmul(left, right):
    return jnp.dot(left, right, preferred_element_type=F32)


def mat_trans(left, right):
    return lax.dot_general(left, right, (((1,), (1,)), ((), ())), preferred_element_type=F32)


def trans_mat(left, right):
    return lax.dot_general(left, right, (((0,), (0,)), ((), ())), preferred_element_type=F32)


def high_bits(size):
    bits = []
    bit = size // 2
    while bit >= 1:
        bits.append(bit)
        bit //= 2
    return bits


def lanes(shape):
    return lax.broadcasted_iota(jnp.int32, shape, 1)


def head_lanes(ref, h, upper):
    wide = ref[:, (h // 2) * 128 : (h // 2) * 128 + 128]
    if (h % 2 == 1) != upper:
        wide = pltpu.roll(wide.astype(F32), HEAD_DIM, 1).astype(BF)
    keep = (lanes(wide.shape) >= HEAD_DIM) if upper else (lanes(wide.shape) < HEAD_DIM)
    return jnp.where(keep, wide, jnp.zeros_like(wide))


class Relay:
    def __init__(self, n_ctx, src, dst, send, recv):
        self.src, self.dst, self.send, self.recv = src, dst, send, recv
        self.piece = src.shape[0] // n_ctx
        self.ctx = lax.axis_index("ctx")
        self.bits = high_bits(n_ctx)
        self.count = 0
        self.all = []
        self.last = []

    def _copy(self, src, dst, axis, bit):
        e = self.count
        self.count += 1
        copy = pltpu.make_async_remote_copy(
            src_ref=src,
            dst_ref=dst,
            send_sem=self.send.at[e],
            recv_sem=self.recv.at[e],
            device_id={axis: lax.axis_index(axis) ^ bit},
            device_id_type=MESH,
        )
        copy.start()
        self.all.append(copy)
        return copy

    def _cut(self, which):
        return pl.ds(pl.multiple_of(which * self.piece, self.piece), self.piece)

    def start(self):
        mine = self._cut(self.ctx)
        self.last = [self._copy(self.src.at[mine], self.dst.at[mine], "fsdp", 1)]

    def hop(self, j):
        self.landed()
        bit = self.bits[j]
        parts = [self.dst.at[self._cut(self.ctx ^ m)] for m in masks_of(self.bits[:j])]
        self.last = [self._copy(part, part, "ctx", bit) for part in parts]

    def landed(self):
        for copy in self.last:
            copy.wait_recv()
        self.last = []

    def drain(self):
        for copy in self.all:
            copy.wait_send()


def forward_kernel(
    n_ctx,
    n_head,
    span,
    q_ref,
    p_ref,
    wl_ref,
    wr_ref,
    gate_ref,
    up_ref,
    down_ref,
    o_ref,
    lse_ref,
    sum_ref,
    gate_other,
    up_other,
    down_other,
    q_pad,
    ext,
    max_ref,
    acc_ref,
    relay_send,
    relay_recv,
    left,
    right,
    from_lo,
    from_hi,
    *sems,
):
    rows, width = q_ref.shape
    heads = width // HEAD_DIM
    block = lax.axis_index("ctx") * 2 + lax.axis_index("fsdp")
    barrier = line_greet(n_head)
    greet(n_ctx)
    ext[...] = jnp.where(lanes(p_ref.shape) < HEAD_DIM, jnp.ones_like(p_ref[...]), p_ref[...])
    pl.semaphore_wait(barrier, line_peers(n_head) + len(partners(n_ctx)))
    gate = Relay(n_ctx, gate_ref, gate_other, relay_send.at[0], relay_recv.at[0])
    up = Relay(n_ctx, up_ref, up_other, relay_send.at[1], relay_recv.at[1])
    down = Relay(n_ctx, down_ref, down_other, relay_send.at[2], relay_recv.at[2])
    gate.start()
    up.start()
    down.hop(0)
    step, steps, drain = line_sum(n_head, left, right, left, right, sum_ref, from_lo, from_hi, sems)
    size = rows // GROUPS
    stack = heads * size
    sub = min(512, stack)
    per_group = CHUNKS // GROUPS

    def tile(start, first_row, masked):
        cut = pl.ds(start, span)
        for j in range(stack // sub):
            part = pl.ds(j * sub, sub)
            scores = mat_trans(q_pad[part, :], p_ref[cut, :])
            if masked:
                row = first_row + lax.rem(lax.broadcasted_iota(jnp.int32, (sub, span), 0), size)
                col = start + lax.broadcasted_iota(jnp.int32, (sub, span), 1)
                scores = jnp.where(col <= row, scores, NEG)
            old = max_ref[part, :]
            new = jnp.maximum(old, jnp.max(scores, axis=1, keepdims=True))
            weights = jnp.exp(scores - jnp.tile(new, (1, span // 128))).astype(BF)
            acc_ref[part, :] = acc_ref[part, :] * jnp.exp(old - new) + matmul(weights, ext[cut, :])
            max_ref[part, :] = new

    def run(s, carry):
        step(s)
        return carry

    def one_group(g, carry):
        mine = pl.ds(pl.multiple_of(g * size, size), size)
        first_row = block * rows + g * size
        for h in range(heads):
            q_pad[h * size : (h + 1) * size, :] = head_lanes(q_ref.at[mine], h, False)
        max_ref[...] = jnp.full_like(max_ref, NEG)
        acc_ref[...] = jnp.zeros_like(acc_ref)

        tiles = (block + 1) * (rows // span)
        base = (g - 1) * per_group

        def sums(i):
            lax.fori_loop((i * per_group) // tiles, ((i + 1) * per_group) // tiles, lambda j, c: run(base + j, c), 0)

        def full(i, c):
            sums(i)
            tile(pl.multiple_of(i * span, span), first_row, False)
            return c

        lax.fori_loop(0, block * (rows // span), full, 0)
        for j in range(rows // span):
            sums(block * (rows // span) + j)
            tile(pl.multiple_of(block * rows + j * span, span), first_row, True)
        for h in range(heads):
            acc = acc_ref[h * size : (h + 1) * size, :]
            total = acc[:, :HEAD_DIM]
            o_ref[mine, h * HEAD_DIM : (h + 1) * HEAD_DIM] = (acc[:, HEAD_DIM:] / total).astype(BF)
            lse = max_ref[h * size : (h + 1) * size, :] + jnp.log(jnp.concatenate([total, total], axis=1))
            lse_ref[h, :, mine] = lse.T[0:1, :]
        att = o_ref[mine, :]
        left[mine, :] = matmul(att, wl_ref[...]).astype(BF)
        right[mine, :] = matmul(att, wr_ref[...]).astype(BF)
        return carry

    lax.fori_loop(0, GROUPS - 1, one_group, 0)
    gate.hop(0)
    down.hop(1)
    lax.fori_loop(GROUPS - 1, GROUPS, one_group, 0)
    hops = len(high_bits(n_ctx))
    later = [(down, j) for j in range(2, hops)] + [(gate, 1), (up, 0)]
    for j in range(1, hops):
        later += [(up, j)] + ([(gate, j + 1)] if j + 1 < hops else [])
    at = CHUNKS - per_group
    rest = steps - at
    for i, (relay, j) in enumerate(later):
        to = CHUNKS - per_group + (rest * (2 * i + 1)) // (2 * len(later))
        lax.fori_loop(at, to, run, 0)
        at = to
        relay.hop(j)
    lax.fori_loop(at, steps, run, 0)
    for relay in (gate, up, down):
        relay.landed()
        relay.drain()
    drain()


def attend_sum(queries, pair, out_left, out_right, gate, up, down, n_ctx, n_head, collective_id):
    rows, width = queries.shape
    heads = width // HEAD_DIM
    seq = pair.shape[0]
    span = min(512, rows)
    wide = 2 * out_left.shape[1]
    vmem = pl.BlockSpec(memory_space=pltpu.VMEM)
    anywhere = pl.BlockSpec(memory_space=pl.ANY)
    stack = heads * rows // GROUPS
    cost = pl.CostEstimate(flops=50_000_000_000, bytes_accessed=8 * rows * wide, transcendentals=0)
    return pl.pallas_call(
        functools.partial(forward_kernel, n_ctx, n_head, span),
        out_shape=(
            jax.ShapeDtypeStruct((rows, width), BF),
            jax.ShapeDtypeStruct((heads, 1, rows), F32),
            jax.ShapeDtypeStruct((rows, wide), BF),
            jax.ShapeDtypeStruct(gate.shape, BF),
            jax.ShapeDtypeStruct(up.shape, BF),
            jax.ShapeDtypeStruct(down.shape, BF),
        ),
        input_output_aliases={6: 5},
        in_specs=[vmem] * 4 + [anywhere] * 3,
        out_specs=(vmem, vmem, vmem, anywhere, anywhere, anywhere),
        scratch_shapes=[
            pltpu.VMEM((stack, 128), BF),
            pltpu.VMEM((seq, 128), BF),
            pltpu.VMEM((stack, 128), F32),
            pltpu.VMEM((stack, 128), F32),
            pltpu.SemaphoreType.DMA((3, n_ctx)),
            pltpu.SemaphoreType.DMA((3, n_ctx)),
        ]
        + line_scratch(rows, wide),
        compiler_params=pltpu.CompilerParams(collective_id=collective_id, has_side_effects=True),
        cost_estimate=cost,
        name="attend_sum",
    )(queries, pair, out_left, out_right, gate, up, down)


def backward_kernel(
    n_head,
    group,
    span,
    q_ref,
    g_ref,
    o_ref,
    lse_ref,
    p_ref,
    left_ref,
    right_ref,
    dq_ref,
    dp_ref,
    sum_ref,
    q_pad,
    g_pad,
    acc_ref,
    dl_ref,
    work_l,
    work_r,
    from_lo,
    from_hi,
    *sems,
):
    rows, width = q_ref.shape
    heads = width // HEAD_DIM
    tiles = rows // span
    block = lax.axis_index("ctx") * 2 + lax.axis_index("fsdp")
    barrier = line_greet(n_head)
    dp_ref[...] = jnp.zeros_like(dp_ref)
    acc_ref[...] = jnp.zeros_like(acc_ref)
    for h in range(heads):
        cut = slice(h * HEAD_DIM, (h + 1) * HEAD_DIM)
        q_pad[h] = head_lanes(q_ref, h, False)
        g_pad[h] = head_lanes(g_ref, h, True)
        product = g_ref[:, cut].astype(F32) * o_ref[:, cut].astype(F32)
        dl_ref[h] = jnp.sum(product.T, axis=0, keepdims=True)
    pl.semaphore_wait(barrier, line_peers(n_head))
    step, steps, drain = line_sum(
        n_head, left_ref, right_ref, work_l, work_r, sum_ref, from_lo, from_hi, sems
    )

    def head_tile(h, pairs, start, masked):
        probs = jnp.exp(mat_trans(pairs, q_pad[h]) - lse_ref[h])
        if masked:
            row = block * rows + lax.broadcasted_iota(jnp.int32, (span, rows), 1)
            col = start + lax.broadcasted_iota(jnp.int32, (span, rows), 0)
            probs = jnp.where(col <= row, probs, 0.0)
        grads = (probs * (mat_trans(pairs, g_pad[h]) - dl_ref[h])).astype(BF)
        acc_ref[h] += trans_mat(grads, pairs)
        return matmul(probs.astype(BF), g_pad[h]) + matmul(grads, q_pad[h])

    groups = heads // group

    def two_steps(t):
        for j in range(2):

            @pl.when(2 * t + j < steps)
            def _():
                step(2 * t + j)

    def full(t, carry):
        two_steps(t)
        first = lax.rem(t, groups) * group
        start = pl.multiple_of((t // groups) * span, span)
        cut = pl.ds(start, span)
        total = head_tile(first, p_ref[cut, :], start, False)
        for h in range(1, group):
            total = total + head_tile(first + h, p_ref[cut, :], start, False)
        dp_ref[cut, :] += total
        return carry

    count = block * tiles * groups
    lax.fori_loop(0, count, full, 0)

    def last(t, carry):
        h = lax.rem(t, heads)

        @pl.when(lax.rem(t, group) == 0)
        def _():
            two_steps(count + t // group)

        start = pl.multiple_of(block * rows + (t // heads) * span, span)
        cut = pl.ds(start, span)
        dp_ref[cut, :] += head_tile(h, p_ref[cut, :], start, True)
        return carry

    lax.fori_loop(0, heads * tiles, last, 0)
    for h in range(heads):
        dq_ref[:, h * HEAD_DIM : (h + 1) * HEAD_DIM] = acc_ref[h][:, :HEAD_DIM]

    def rest(s, carry):
        step(s)
        return carry

    lax.fori_loop(jnp.minimum(2 * (count + groups * tiles), steps), steps, rest, 0)
    drain()


def attend_back(queries, grads, attended, lse, pair, left, right, n_head, collective_id):
    rows, width = queries.shape
    heads = width // HEAD_DIM
    seq = pair.shape[0]
    group = 4 if heads % 4 == 0 else 2
    span = min(512, rows)
    vmem = pl.BlockSpec(memory_space=pltpu.VMEM)
    cost = pl.CostEstimate(
        flops=32 * rows * seq * width, bytes_accessed=8 * rows * width, transcendentals=0
    )
    return pl.pallas_call(
        functools.partial(backward_kernel, n_head, group, span),
        out_shape=(
            jax.ShapeDtypeStruct((rows, width), F32),
            jax.ShapeDtypeStruct((seq, 2 * HEAD_DIM), F32),
            jax.ShapeDtypeStruct((rows, 2 * left.shape[1]), BF),
        ),
        in_specs=[vmem] * 7,
        out_specs=(vmem, vmem, vmem),
        scratch_shapes=[
            pltpu.VMEM((heads, rows, 128), BF),
            pltpu.VMEM((heads, rows, 128), BF),
            pltpu.VMEM((heads, rows, 128), F32),
            pltpu.VMEM((heads, 1, rows), F32),
        ]
        + line_scratch(rows, 2 * left.shape[1]),
        compiler_params=pltpu.CompilerParams(collective_id=collective_id, has_side_effects=True),
        cost_estimate=cost,
        name="attend_backward",
    )(queries, grads, attended, lse, pair, left, right)


def partners(n_ctx):
    return [("fsdp", 1)] + [("ctx", bit) for bit in high_bits(n_ctx)]


def greet(n_ctx):
    barrier = pltpu.get_barrier_semaphore()
    for axis, bit in partners(n_ctx):
        pl.semaphore_signal(
            barrier, inc=1, device_id={axis: lax.axis_index(axis) ^ bit}, device_id_type=MESH
        )
    return barrier


def masks_of(bits):
    masks = [0]
    for bit in bits:
        masks = masks + [m | bit for m in masks]
    return masks


def gather_pairs(n_ctx, rows, all_ref, send, recv):
    x = lax.axis_index("fsdp")
    ctx = lax.axis_index("ctx")
    copies = []

    def part(start, size, axis, bit):
        e = len(copies)
        cut = all_ref.at[pl.ds(pl.multiple_of(start, rows), size)]
        copy = pltpu.make_async_remote_copy(
            src_ref=cut,
            dst_ref=cut,
            send_sem=send.at[e],
            recv_sem=recv.at[e],
            device_id={axis: lax.axis_index(axis) ^ bit},
            device_id_type=MESH,
        )
        copy.start()
        copies.append(copy)
        return copy

    opening = part((ctx * 2 + x) * rows, rows, "fsdp", 1)

    def finish():
        opening.wait_recv()
        done = []
        for bit in high_bits(n_ctx):
            now = [part((ctx ^ m) * 2 * rows, 2 * rows, "ctx", bit) for m in masks_of(done)]
            for copy in now:
                copy.wait_recv()
            done.append(bit)
        for copy in copies:
            copy.wait_send()

    return finish


def scatter_kernel(n_ctx, part_ref, o_ref, work, land, send, recv):
    rows = o_ref.shape[0]
    x = lax.axis_index("fsdp")
    ctx = lax.axis_index("ctx")
    barrier = greet(n_ctx)
    work[...] = part_ref[...].astype(BF)
    pl.semaphore_wait(barrier, len(partners(n_ctx)))
    copies = []
    used = [0]

    def give(start, size, axis, bit):
        e = len(copies)
        cut = pl.ds(pl.multiple_of(start, rows), size)
        copy = pltpu.make_async_remote_copy(
            src_ref=work.at[cut],
            dst_ref=land.at[pl.ds(used[0], size)],
            send_sem=send.at[e],
            recv_sem=recv.at[e],
            device_id={axis: lax.axis_index(axis) ^ bit},
            device_id_type=MESH,
        )
        copy.start()
        copies.append(copy)
        used[0] += size
        return copy, used[0] - size

    def take(start, size, at):
        cut = pl.ds(pl.multiple_of(start, rows), size)
        work[cut, :] = (work[cut, :].astype(F32) + land[at : at + size, :].astype(F32)).astype(BF)

    bits = high_bits(n_ctx)
    for j in range(len(bits)):
        bit = bits[len(bits) - 1 - j]
        masks = masks_of(bits[: len(bits) - 1 - j])
        now = [give((ctx ^ bit ^ m) * 2 * rows, 2 * rows, "ctx", bit) for m in masks]
        for (copy, at), m in zip(now, masks):
            copy.wait_recv()
            take((ctx ^ m) * 2 * rows, 2 * rows, at)
    copy, at = give((ctx * 2 + 1 - x) * rows, rows, "fsdp", 1)
    copy.wait_recv()
    mine = pl.ds(pl.multiple_of((ctx * 2 + x) * rows, rows), rows)
    o_ref[...] = work[mine, :].astype(F32) + land[at : at + rows, :].astype(F32)
    for copy in copies:
        copy.wait_send()


def scatter_pairs(part, rows, n_ctx, collective_id):
    vmem = pl.BlockSpec(memory_space=pltpu.VMEM)
    return pl.pallas_call(
        functools.partial(scatter_kernel, n_ctx),
        out_shape=jax.ShapeDtypeStruct((rows, part.shape[1]), F32),
        in_specs=[vmem],
        out_specs=vmem,
        scratch_shapes=[
            pltpu.VMEM(part.shape, BF),
            pltpu.VMEM(part.shape, BF),
            pltpu.SemaphoreType.DMA((n_ctx,)),
            pltpu.SemaphoreType.DMA((n_ctx,)),
        ],
        compiler_params=pltpu.CompilerParams(collective_id=collective_id, has_side_effects=True),
        name="scatter_pairs",
    )(part)


def project_kernel(
    n_ctx,
    x_ref,
    w_ref,
    gain_ref,
    cos_ref,
    sin_ref,
    wo_ref,
    down_ref,
    q_ref,
    p_ref,
    n_ref,
    w_other,
    gain_other,
    wo_other,
    down_other,
    acc_ref,
    send,
    recv,
    relay_send,
    relay_recv,
    gain_send,
    gain_recv,
):
    rows, width = x_ref.shape
    half = width // 2
    q_width = q_ref.shape[1]
    x_at = lax.axis_index("fsdp")
    block = lax.axis_index("ctx") * 2 + x_at
    barrier = greet(n_ctx)
    pl.semaphore_wait(barrier, len(partners(n_ctx)))
    gains = pltpu.make_async_remote_copy(
        src_ref=gain_ref,
        dst_ref=gain_other,
        send_sem=gain_send,
        recv_sem=gain_recv,
        device_id={"fsdp": 1 - x_at},
        device_id_type=MESH,
    )
    gains.start()
    part = half // 2
    first = [
        Relay(
            n_ctx,
            w_ref.at[pl.ds(i * part, part)],
            w_other.at[pl.ds(i * part, part)],
            relay_send.at[i],
            relay_recv.at[i],
        )
        for i in range(2)
    ]
    second = Relay(n_ctx, wo_ref, wo_other, relay_send.at[2], relay_recv.at[2])
    third = Relay(n_ctx, down_ref, down_other, relay_send.at[3], relay_recv.at[3])
    for relay in first:
        relay.start()
    second.start()
    gains.wait_recv()
    parts = 8
    size = rows // parts
    own = pl.ds(pl.multiple_of(x_at * half, half), half)
    other = pl.ds(pl.multiple_of((1 - x_at) * half, half), half)

    def cut_of(i):
        return pl.ds(pl.multiple_of(i * size, size), size)

    def norm(i, carry):
        cut = cut_of(i)
        left = x_ref[cut, own].astype(F32)
        right = x_ref[cut, other].astype(F32)
        total = jnp.sum(left * left, axis=1, keepdims=True) + jnp.sum(right * right, axis=1, keepdims=True)
        scale = lax.rsqrt(total / width + EPSILON)
        n_ref[cut, :half] = (left * scale * gain_ref[0:1, :]).astype(BF)
        n_ref[cut, half:] = (right * scale * gain_other[0:1, :]).astype(BF)
        return carry

    lax.fori_loop(0, parts, norm, 0)
    for relay in first:
        relay.hop(0)
    third.start()
    second.hop(0)

    def local(i, carry):
        cut = cut_of(i)
        acc_ref[cut, :] = matmul(n_ref[cut, :half], w_ref[...])
        return carry

    lax.fori_loop(0, parts, local, 0)
    for j in range(1, len(high_bits(n_ctx))):
        for relay in first:
            relay.hop(j)
    for relay in first:
        relay.landed()

    def rotated(wide, cut):
        low = lax.rem(lanes(wide.shape), HEAD_DIM) < HEAD_DIM // 2
        turned = jnp.where(low, pltpu.roll(wide, 128 - HEAD_DIM // 2, 1), pltpu.roll(wide, HEAD_DIM // 2, 1))
        return wide * cos_ref[cut, :] + turned * sin_ref[cut, :]

    def pairs(i, carry):
        cut = cut_of(i)
        both = acc_ref[cut, q_width:] + matmul(n_ref[cut, half:], w_other[:, q_width:])
        pair = jnp.where(lanes(both.shape) < HEAD_DIM, rotated(both, cut), both)
        p_ref[pl.ds(pl.multiple_of(block * rows + i * size, size), size), :] = pair.astype(BF)
        return carry

    def queries(i, carry):
        cut = cut_of(i)
        whole = acc_ref[cut, :q_width] + matmul(n_ref[cut, half:], w_other[:, :q_width])
        for j in range(q_width // 128):
            sl = slice(j * 128, (j + 1) * 128)
            q_ref[cut, sl] = (rotated(whole[:, sl], cut) * 0.125).astype(BF)
        return carry

    lax.fori_loop(0, parts, pairs, 0)
    finish = gather_pairs(n_ctx, rows, p_ref, send, recv)
    lax.fori_loop(0, parts, queries, 0)
    finish()
    for j in range(1, len(high_bits(n_ctx))):
        second.hop(j)
    second.landed()
    third.landed()
    for relay in first + [second, third]:
        relay.drain()
    gains.wait_send()


def project(inputs, w_local, gains, cosine, sine, w_out, w_down, q_width, n_ctx, collective_id):
    rows, width = inputs.shape
    vmem = pl.BlockSpec(memory_space=pltpu.VMEM)
    anywhere = pl.BlockSpec(memory_space=pl.ANY)
    return pl.pallas_call(
        functools.partial(project_kernel, n_ctx),
        out_shape=(
            jax.ShapeDtypeStruct((rows, q_width), BF),
            jax.ShapeDtypeStruct((rows * 2 * n_ctx, 2 * HEAD_DIM), BF),
            jax.ShapeDtypeStruct((rows, width), BF),
            jax.ShapeDtypeStruct(w_local.shape, BF),
            jax.ShapeDtypeStruct(gains.shape, F32),
            jax.ShapeDtypeStruct(w_out.shape, BF),
            jax.ShapeDtypeStruct(w_down.shape, BF),
        ),
        in_specs=[vmem] * 5 + [anywhere] * 2,
        out_specs=(vmem,) * 5 + (anywhere,) * 2,
        scratch_shapes=[
            pltpu.VMEM((rows, w_local.shape[1]), F32),
            pltpu.SemaphoreType.DMA((n_ctx,)),
            pltpu.SemaphoreType.DMA((n_ctx,)),
            pltpu.SemaphoreType.DMA((4, n_ctx)),
            pltpu.SemaphoreType.DMA((4, n_ctx)),
            pltpu.SemaphoreType.DMA,
            pltpu.SemaphoreType.DMA,
        ],
        compiler_params=pltpu.CompilerParams(collective_id=collective_id, has_side_effects=True),
        name="project",
    )(inputs, w_local, gains, cosine, sine, w_out, w_down)


def line_sum(n, left, right, work_l, work_r, o_ref, from_lo, from_hi, sems):
    s_up, r_up, s_dn, r_dn, s_a, r_a, s_b, r_b = sems
    me = lax.axis_index("head")
    rows, cols = left.shape
    size = rows // CHUNKS
    has_lo = me > 0
    has_hi = me < n - 1
    middle = jnp.logical_and(has_lo, has_hi)

    def at(k):
        return pl.ds(pl.multiple_of(k * size, size), size)

    def remote(src, dst, send, recv, target):
        return pltpu.make_async_remote_copy(
            src_ref=src,
            dst_ref=dst,
            send_sem=send,
            recv_sem=recv,
            device_id={"head": target},
            device_id_type=MESH,
        )

    def up(k, src):
        return remote(src.at[at(k)], from_lo.at[at(k)], s_up.at[k], r_up.at[k], me + 1)

    def down(k, src):
        return remote(src.at[at(k)], from_hi.at[at(k)], s_dn.at[k], r_dn.at[k], me - 1)

    def spread_a(k):
        part = o_ref.at[at(k), pl.ds(0, cols)]
        return remote(part, part, s_a.at[k], r_a.at[k], me + 1)

    def spread_b(k):
        part = o_ref.at[at(k), pl.ds(cols, cols)]
        return remote(part, part, s_b.at[k], r_b.at[k], me - 1)

    def valid(k):
        return jnp.logical_and(k >= 0, k < CHUNKS)

    def added(mine, there, k):
        return (mine[at(k), :].astype(F32) + there[at(k), :].astype(F32)).astype(BF)

    def step(s):
        k1 = s - LAG * me
        k2 = s - LAG * (n - 1 - me)
        k3 = s - LAG * (n - 1 + me)
        k4 = s - LAG * (2 * (n - 1) - me)

        @pl.when(jnp.logical_and(valid(k1), me == 0))
        def _():
            up(k1, right).start()

        @pl.when(jnp.logical_and(valid(k2), me == n - 1))
        def _():
            down(k2, left).start()

        @pl.when(jnp.logical_and(valid(k1), middle))
        def _():
            up(k1, right).wait_recv()
            work_r[at(k1), :] = added(right, from_lo, k1)
            up(k1, work_r).start()

        @pl.when(jnp.logical_and(valid(k1), me == n - 1))
        def _():
            up(k1, right).wait_recv()
            o_ref[at(k1), cols:] = added(right, from_lo, k1)
            spread_b(k1).start()

        @pl.when(jnp.logical_and(valid(k2), middle))
        def _():
            down(k2, left).wait_recv()
            work_l[at(k2), :] = added(left, from_hi, k2)
            down(k2, work_l).start()

        @pl.when(jnp.logical_and(valid(k2), me == 0))
        def _():
            down(k2, left).wait_recv()
            o_ref[at(k2), :cols] = added(left, from_hi, k2)
            spread_a(k2).start()

        @pl.when(jnp.logical_and(valid(k3), has_lo))
        def _():
            spread_a(k3).wait_recv()

            @pl.when(has_hi)
            def _():
                spread_a(k3).start()

        @pl.when(jnp.logical_and(valid(k4), has_hi))
        def _():
            spread_b(k4).wait_recv()

            @pl.when(has_lo)
            def _():
                spread_b(k4).start()

    def drain():
        def one(k, carry):
            @pl.when(has_hi)
            def _():
                up(k, right).wait_send()
                spread_a(k).wait_send()

            @pl.when(has_lo)
            def _():
                down(k, left).wait_send()
                spread_b(k).wait_send()

            return carry

        lax.fori_loop(0, CHUNKS, one, 0)

    return step, CHUNKS + 2 * LAG * (n - 1), drain


def line_greet(n):
    me = lax.axis_index("head")
    barrier = pltpu.get_barrier_semaphore()

    @pl.when(me > 0)
    def _():
        pl.semaphore_signal(barrier, inc=1, device_id={"head": me - 1}, device_id_type=MESH)

    @pl.when(me < n - 1)
    def _():
        pl.semaphore_signal(barrier, inc=1, device_id={"head": me + 1}, device_id_type=MESH)

    return barrier


def line_peers(n):
    me = lax.axis_index("head")
    return jnp.where(me > 0, 1, 0) + jnp.where(me < n - 1, 1, 0)


def line_scratch(rows, width):
    return [pltpu.VMEM((rows, width // 2), BF)] * 4 + [pltpu.SemaphoreType.DMA((CHUNKS,))] * 8


def head_sum_kernel(n, left_ref, right_ref, o_ref, work_l, work_r, from_lo, from_hi, *sems):
    barrier = line_greet(n)
    pl.semaphore_wait(barrier, line_peers(n))
    step, steps, drain = line_sum(n, left_ref, right_ref, work_l, work_r, o_ref, from_lo, from_hi, sems)

    def run(s, carry):
        step(s)
        return carry

    lax.fori_loop(0, steps, run, 0)
    drain()


def head_sum(left, right, n, collective_id):
    rows, cols = left.shape
    return pl.pallas_call(
        functools.partial(head_sum_kernel, n),
        out_shape=jax.ShapeDtypeStruct((rows, 2 * cols), BF),
        in_specs=[pl.BlockSpec(memory_space=pltpu.VMEM)] * 2,
        out_specs=pl.BlockSpec(memory_space=pltpu.VMEM),
        scratch_shapes=line_scratch(rows, 2 * cols),
        compiler_params=pltpu.CompilerParams(collective_id=collective_id, has_side_effects=True),
        cost_estimate=pl.CostEstimate(
            flops=40_000_000_000, bytes_accessed=8 * rows * cols, transcendentals=0
        ),
        name="head_sum",
    )(left, right)


def ffn_kernel(
    n_head,
    x_ref,
    mix_ref,
    cot_ref,
    gain_ref,
    gain_other,
    gate_l,
    gate_r,
    up_l,
    up_r,
    down_l,
    down_r,
    sum_ref,
    n_ref,
    ffn_left,
    ffn_right,
    down_kept,
    gate_kept,
    gate_sent,
    up_kept,
    up_sent,
    act_ref,
    gig_ref,
    uig_ref,
    cot_land,
    n_land,
    act_land,
    gig_land,
    uig_land,
    down_sent,
    down_land,
    out_tile,
    out_sem,
    trade_send,
    trade_recv,
    cross_send,
    cross_recv,
    left,
    right,
    from_lo,
    from_hi,
    *sems,
):
    rows, width = x_ref.shape
    half = width // 2
    quarter = half // 2
    units = act_ref.shape[1]
    x_at = lax.axis_index("fsdp")
    ctx_at = lax.axis_index("ctx")
    core = lax.rem(ctx_at, 2)
    own = pl.ds(pl.multiple_of(x_at * half, half), half)
    other = pl.ds(pl.multiple_of((1 - x_at) * half, half), half)
    barrier = line_greet(n_head)
    pl.semaphore_signal(barrier, inc=1, device_id={"fsdp": 1 - x_at}, device_id_type=MESH)
    pl.semaphore_signal(barrier, inc=1, device_id={"ctx": ctx_at ^ 1}, device_id_type=MESH)
    pl.semaphore_wait(barrier, line_peers(n_head) + 2)

    def trade(src, dst, at):
        return pltpu.make_async_remote_copy(
            src_ref=src,
            dst_ref=dst,
            send_sem=trade_send.at[at],
            recv_sem=trade_recv.at[at],
            device_id={"ctx": ctx_at ^ 1},
            device_id_type=MESH,
        )

    def absolute(side, c):
        start = (x_at if side == 0 else 1 - x_at) * half + c * quarter
        return pl.ds(pl.multiple_of(start, quarter), quarter)

    def relative(side, c):
        return pl.ds(pl.multiple_of(side * half + c * quarter, quarter), quarter)

    cot_trades = [
        trade(cot_ref.at[:, absolute(j, 1 - core)], cot_land.at[:, pl.ds(j * quarter, quarter)], j)
        for j in range(2)
    ]
    for copy in cot_trades:
        copy.start()

    def row_trades(g):
        mine = pl.ds(pl.multiple_of(g * (rows // FFN_GROUPS), rows // FFN_GROUPS), rows // FFN_GROUPS)
        at = 2 + g * 5
        return [
            trade(act_ref.at[mine], act_land.at[mine], at),
            trade(gig_ref.at[mine], gig_land.at[mine], at + 1),
            trade(uig_ref.at[mine], uig_land.at[mine], at + 2),
            trade(n_ref.at[mine, relative(0, 1 - core)], n_land.at[mine, pl.ds(0, quarter)], at + 3),
            trade(n_ref.at[mine, relative(1, 1 - core)], n_land.at[mine, pl.ds(quarter, quarter)], at + 4),
        ]

    step, steps, drain = line_sum(n_head, left, right, left, right, sum_ref, from_lo, from_hi, sems)

    def run(s, carry):
        step(s)
        return carry

    size = rows // FFN_GROUPS
    per_group = CHUNKS // FFN_GROUPS

    def one_group(g, carry):
        mine = pl.ds(pl.multiple_of(g * size, size), size)
        base = (g - 1) * per_group
        stops = [base + (per_group * i) // 4 for i in range(5)]
        hid_l = x_ref[mine, own].astype(F32) + mix_ref[mine, :half].astype(F32)
        hid_r = x_ref[mine, other].astype(F32) + mix_ref[mine, half:].astype(F32)
        total = jnp.sum(hid_l * hid_l, axis=1, keepdims=True) + jnp.sum(hid_r * hid_r, axis=1, keepdims=True)
        scale = lax.rsqrt(total / width + EPSILON)
        n_ref[mine, :half] = (hid_l * scale * gain_ref[1:2, :]).astype(BF)
        n_ref[mine, half:] = (hid_r * scale * gain_other[1:2, :]).astype(BF)
        lax.fori_loop(stops[0], stops[1], run, 0)
        gate = matmul(n_ref[mine, :half], gate_l[...]) + matmul(n_ref[mine, half:], gate_r[...])
        up = matmul(n_ref[mine, :half], up_l[...]) + matmul(n_ref[mine, half:], up_r[...])
        lax.fori_loop(stops[1], stops[2], run, 0)
        sigma = jax.nn.sigmoid(gate)
        silu = gate * sigma
        act_ref[mine, :] = (silu * up).astype(BF)
        grad = mat_trans(cot_ref[mine, own], down_l[...]) + mat_trans(cot_ref[mine, other], down_r[...])
        gig_ref[mine, :] = (grad * up * sigma * (1.0 + gate * (1.0 - sigma))).astype(BF)
        uig_ref[mine, :] = (grad * silu).astype(BF)
        lax.fori_loop(stops[2], stops[3], run, 0)
        gig = gig_ref[mine, :]
        uig = uig_ref[mine, :]
        left[mine, :] = (mat_trans(gig, gate_l[...]) + mat_trans(uig, up_l[...])).astype(BF)
        lax.fori_loop(stops[3], stops[4], run, 0)
        right[mine, :] = (mat_trans(gig, gate_r[...]) + mat_trans(uig, up_r[...])).astype(BF)
        for copy in row_trades(g):
            copy.start()
        return carry

    lax.fori_loop(0, FFN_GROUPS, one_group, 0)
    first = CHUNKS - per_group
    rest = steps - first
    tile = 128
    down_tiles = units // tile
    row_tiles = quarter // tile
    total_work = down_tiles + 4 * row_tiles + 2 * FFN_GROUPS

    def sums(i, weight=1):
        lax.fori_loop(
            first + (rest * i) // total_work, first + (rest * (i + weight)) // total_work, run, 0
        )

    for copy in cot_trades:
        copy.wait_recv()

    def landed(g, carry):
        for copy in row_trades(g):
            copy.wait_recv()
        return carry

    lax.fori_loop(0, FFN_GROUPS, landed, 0)

    def down_tile(t, carry):
        sums(t)
        cut = pl.ds(pl.multiple_of(t * tile, tile), tile)
        mine = act_ref[:, cut]
        theirs = act_land[:, cut]
        for dst, side in ((down_sent, 1), (down_kept, 0)):
            dst[cut, :] = (
                trans_mat(mine, cot_ref[:, absolute(side, core)])
                + trans_mat(theirs, cot_land[:, side * quarter : (side + 1) * quarter])
            ).astype(BF)
        return carry

    lax.fori_loop(0, down_tiles, down_tile, 0)
    cross = pltpu.make_async_remote_copy(
        src_ref=down_sent,
        dst_ref=down_land,
        send_sem=cross_send,
        recv_sem=cross_recv,
        device_id={"fsdp": 1 - x_at},
        device_id_type=MESH,
    )
    cross.start()
    done = down_tiles

    def out_copy(dst, t, slot):
        cut = pl.ds(pl.multiple_of(t * tile, tile), tile)
        return pltpu.make_async_copy(out_tile.at[slot], dst.at[cut], out_sem.at[slot])

    outs = (
        (gate_sent, 1, gig_ref, gig_land),
        (gate_kept, 0, gig_ref, gig_land),
        (up_sent, 1, uig_ref, uig_land),
        (up_kept, 0, uig_ref, uig_land),
    )
    for dst, side, own_grad, their_grad in outs:

        def row_tile(t, carry):
            sums(done + t)
            slot = lax.rem(t, 2)
            there = pl.ds(pl.multiple_of(side * half + core * quarter + t * tile, tile), tile)
            landing = pl.ds(pl.multiple_of(side * quarter + t * tile, tile), tile)
            value = (
                trans_mat(n_ref[:, there], own_grad[...]) + trans_mat(n_land[:, landing], their_grad[...])
            ).astype(BF)

            @pl.when(t >= 2)
            def _():
                out_copy(dst, t - 2, slot).wait()

            out_tile[slot] = value
            out_copy(dst, t, slot).start()
            return carry

        lax.fori_loop(0, row_tiles, row_tile, 0)
        for t in range(max(row_tiles - 2, 0), row_tiles):
            out_copy(dst, t, t % 2).wait()
        done += row_tiles

    def project_down(g, carry):
        mine = pl.ds(pl.multiple_of(g * size, size), size)
        sums(done + 2 * g, 2)
        ffn_left[mine, :] = matmul(act_ref[mine, :], down_l[...]).astype(BF)
        ffn_right[mine, :] = matmul(act_ref[mine, :], down_r[...]).astype(BF)
        return carry

    lax.fori_loop(0, FFN_GROUPS, project_down, 0)
    cross.wait_recv()

    def finish(t, carry):
        cut = pl.ds(pl.multiple_of(t * tile, tile), tile)
        down_kept[cut, :] = (down_kept[cut, :].astype(F32) + down_land[cut, :].astype(F32)).astype(BF)
        return carry

    lax.fori_loop(0, down_tiles, finish, 0)
    cross.wait_send()
    for copy in cot_trades:
        copy.wait_send()

    def sent(g, carry):
        for copy in row_trades(g):
            copy.wait_send()
        return carry

    lax.fori_loop(0, FFN_GROUPS, sent, 0)
    drain()


def ffn_sum(inputs, mixed, cot, gains, gains_other, gate, gate_o, up, up_o, down, down_o, n_head, collective_id):
    rows, width = inputs.shape
    units = gate.shape[1]
    vmem = pl.BlockSpec(memory_space=pltpu.VMEM)
    wide = jax.ShapeDtypeStruct((rows, width), BF)
    narrow = jax.ShapeDtypeStruct((rows, width // 2), BF)
    quarter = width // 4
    flat = jax.ShapeDtypeStruct((quarter, units), BF)
    trades = 2 + 5 * FFN_GROUPS
    return pl.pallas_call(
        functools.partial(ffn_kernel, n_head),
        out_shape=(wide, wide, narrow, narrow, jax.ShapeDtypeStruct((units, quarter), BF)) + (flat,) * 4,
        in_specs=[vmem] * 11,
        out_specs=(vmem,) * 5 + (pl.BlockSpec(memory_space=pl.ANY),) * 4,
        scratch_shapes=[pltpu.VMEM((rows, units), BF)] * 3
        + [pltpu.VMEM((rows, width // 2), BF)] * 2
        + [pltpu.VMEM((rows, units), BF)] * 3
        + [pltpu.VMEM((units, quarter), BF)] * 2
        + [
            pltpu.VMEM((2, 128, units), BF),
            pltpu.SemaphoreType.DMA((2,)),
            pltpu.SemaphoreType.DMA((trades,)),
            pltpu.SemaphoreType.DMA((trades,)),
            pltpu.SemaphoreType.DMA,
            pltpu.SemaphoreType.DMA,
        ]
        + line_scratch(rows, width),
        compiler_params=pltpu.CompilerParams(
            collective_id=collective_id, has_side_effects=True, vmem_limit_bytes=66_000_000
        ),
        cost_estimate=pl.CostEstimate(
            flops=50_000_000_000, bytes_accessed=8 * rows * width, transcendentals=0
        ),
        name="ffn_sum",
    )(inputs, mixed, cot, gains, gains_other, gate, gate_o, up, up_o, down, down_o)


def flip(array, axis, bit, size):
    return lax.ppermute(array, axis, [(i, i ^ bit) for i in range(size)])


def shards(
    n_ctx,
    n_head,
    inputs,
    query_weight,
    key_weight,
    value_weight,
    output_weight,
    gate_weight,
    up_weight,
    down_weight,
    attn_gain,
    ffn_gain,
    cotangent,
):
    rows, width = inputs.shape
    half = width // 2
    quarter = half // 2
    x_at = lax.axis_index("fsdp")
    ctx_at = lax.axis_index("ctx")
    core = lax.rem(ctx_at, 2)
    block = ctx_at * 2 + x_at
    block_arr = jnp.reshape(block, (1,)).astype(jnp.int32)

    def own_first(array):
        swapped = jnp.concatenate([array[:, half:], array[:, :half]], axis=1)
        return jnp.where(x_at == 0, array, swapped)

    every = high_bits(n_ctx)

    def columns_of(array, which):
        first = jnp.concatenate([array[:, :quarter], array[:, half : half + quarter]], axis=1)
        second = jnp.concatenate([array[:, quarter:half], array[:, half + quarter :]], axis=1)
        return jnp.where(which == 0, first, second)

    def trade(array):
        return jnp.concatenate([array, flip(array, "ctx", 1, n_ctx)], axis=0)

    def trade_columns(array):
        got = flip(columns_of(array, 1 - core), "ctx", 1, n_ctx)
        return jnp.concatenate([columns_of(array, core), got], axis=0)

    q_width = query_weight.shape[1]
    half_dim = HEAD_DIM // 2
    positions = block * rows + jnp.arange(rows, dtype=jnp.int32)
    lane = lax.broadcasted_iota(jnp.int32, (rows, 2 * HEAD_DIM), 1)
    freqs = 10000.0 ** (-2.0 * (lane % half_dim).astype(F32) / HEAD_DIM)
    angles = positions.astype(F32)[:, None] * freqs
    cosine = jnp.cos(angles)
    sine = jnp.sin(angles)
    signed = jnp.where(lane % HEAD_DIM < half_dim, -sine, sine)
    qkv_local = jnp.concatenate([query_weight, key_weight, value_weight], axis=1)
    gains_local = jnp.concatenate([attn_gain[None], ffn_gain[None], jnp.zeros((6, half), BF)]).astype(F32)
    queries, pair, normed_one, qkv_other, gains_other, out_other, down_begun = project(
        inputs, qkv_local, gains_local, cosine, signed, output_weight, down_weight, q_width, n_ctx, 4
    )
    attended, lse, mixed, gate_other, up_other, down_other = attend_sum(
        queries, pair, output_weight, out_other, gate_weight, up_weight, down_begun, n_ctx, n_head, 1
    )
    low_sum, _, down_left, down_right, down_kept, gate_kept, gate_sent, up_kept, up_sent = ffn_sum(
        inputs,
        mixed,
        cotangent,
        gains_local,
        gains_other,
        gate_weight,
        gate_other,
        up_weight,
        up_other,
        down_weight,
        down_other,
        n_head,
        2,
    )
    normed_two_grad = low_sum.astype(F32)
    gain_one = jnp.concatenate([gains_local[0], gains_other[0]])
    gain_two = jnp.concatenate([gains_local[1], gains_other[1]])
    late_inputs, late_cot, normed_one, _ = lax.optimization_barrier((inputs, cotangent, normed_one, low_sum))
    in_float = own_first(late_inputs).astype(F32)
    cot = own_first(late_cot)
    scale_one = lax.rsqrt(jnp.mean(in_float * in_float, axis=-1, keepdims=True) + EPSILON)
    unit_one = in_float * scale_one
    hidden = in_float + mixed.astype(F32)
    scale_two = lax.rsqrt(jnp.mean(hidden * hidden, axis=-1, keepdims=True) + EPSILON)
    unit_two = hidden * scale_two
    one_pair = trade_columns(normed_one)
    scaled_two = normed_two_grad * gain_two
    gain_two_part = jnp.sum(normed_two_grad * unit_two, axis=0)
    hidden_grad = cot.astype(F32) + scale_two * (
        scaled_two - unit_two * jnp.mean(scaled_two * unit_two, axis=-1, keepdims=True)
    )
    hidden_low = hidden_grad.astype(BF)

    attended_grad = (
        mat_trans(hidden_low[:, :half], output_weight) + mat_trans(hidden_low[:, half:], out_other)
    ).astype(BF)
    out_part = trans_mat(trade(attended), trade_columns(hidden_low)).astype(BF)
    attended_grad, out_part = lax.optimization_barrier((attended_grad, out_part))
    query_acc, pair_acc, ffn_out = attend_back(
        queries, attended_grad, attended, lse, pair, down_left, down_right, n_head, 6
    )
    outputs = own_first((hidden + ffn_out.astype(F32)).astype(BF))
    pair_mine = scatter_pairs(pair_acc, rows, n_ctx, 5)

    def unrotate(values):
        count = values.shape[1] // 128
        cos = jnp.concatenate([cosine] * count, axis=1)
        sin = jnp.concatenate([signed] * count, axis=1)
        low = lax.broadcasted_iota(jnp.int32, values.shape, 1) % HEAD_DIM < half_dim
        turned = jnp.where(low, jnp.roll(values, -half_dim, axis=1), jnp.roll(values, half_dim, axis=1))
        return values * cos - turned * sin

    q_raw = unrotate(query_acc * 0.125)
    pair_raw = jnp.where(lane < HEAD_DIM, unrotate(pair_mine), pair_mine)
    qkv_raw = jnp.concatenate([q_raw, pair_raw], axis=1).astype(BF)
    last_left = mat_trans(qkv_raw, qkv_local).astype(BF)
    last_right = mat_trans(qkv_raw, qkv_other).astype(BF)
    qkv_part = trans_mat(one_pair, trade(qkv_raw)).astype(BF)
    last_left, last_right, qkv_part = lax.optimization_barrier((last_left, last_right, qkv_part))
    normed_one_grad = head_sum(last_left, last_right, n_head, 3).astype(F32)
    gain_one_part = jnp.sum(normed_one_grad * unit_one, axis=0)
    scaled_one = normed_one_grad * gain_one
    input_grad = own_first(
        hidden_grad
        + scale_one
        * (scaled_one - unit_one * jnp.mean(scaled_one * unit_one, axis=-1, keepdims=True))
    )

    def total(kept, sent):
        if sent is not None:
            kept = (kept.astype(F32) + flip(sent, "fsdp", 1, 2).astype(F32)).astype(BF)
        for bit in every[:-1]:
            kept = (kept.astype(F32) + flip(kept, "ctx", bit, n_ctx).astype(F32)).astype(BF)
        return kept

    def spread(kept, dim):
        got = flip(kept, "ctx", 1, n_ctx)
        first = jnp.where(core == 0, kept, got)
        second = jnp.where(core == 0, got, kept)
        return jnp.concatenate([first, second], axis=dim).astype(F32)

    down_grad = spread(total(down_kept, None), 1)
    gate_grad = spread(total(gate_kept, gate_sent), 0)
    up_grad = spread(total(up_kept, up_sent), 0)
    output_grad = spread(total(out_part[:, :quarter], out_part[:, quarter:]), 1)
    qkv_grad = spread(total(qkv_part[:quarter], qkv_part[quarter:]), 0)
    query_grad = qkv_grad[:, :q_width]
    key_grad = qkv_grad[:, q_width : q_width + HEAD_DIM]
    value_grad = qkv_grad[:, q_width + HEAD_DIM :]

    gain_parts = jnp.stack([gain_one_part, gain_two_part])
    gain_kept = gain_parts[:, :half] + flip(gain_parts[:, half:], "fsdp", 1, 2)
    for bit in every:
        gain_kept = gain_kept + flip(gain_kept, "ctx", bit, n_ctx)

    return (
        outputs,
        input_grad,
        query_grad,
        key_grad,
        value_grad,
        output_grad,
        gate_grad,
        up_grad,
        down_grad,
        gain_kept[0],
        gain_kept[1],
    )


def solution(mesh):
    n_ctx = mesh.shape["ctx"]

    def body(*args):
        return shards(n_ctx, mesh.shape["head"], *args)

    return jax.shard_map(
        body,
        mesh=mesh,
        in_specs=(
            P(("ctx", "fsdp"), None),
            P("fsdp", "head"),
            P("fsdp", "head"),
            P("fsdp", "head"),
            P("head", "fsdp"),
            P("fsdp", "head"),
            P("fsdp", "head"),
            P("head", "fsdp"),
            P("fsdp"),
            P("fsdp"),
            P(("ctx", "fsdp"), None),
        ),
        out_specs=(
            P(("ctx", "fsdp"), None),
            P(("ctx", "fsdp"), None),
            P("fsdp", "head"),
            P("fsdp", "head"),
            P("fsdp", "head"),
            P("head", "fsdp"),
            P("fsdp", "head"),
            P("fsdp", "head"),
            P("head", "fsdp"),
            P("fsdp"),
            P("fsdp"),
        ),
        check_vma=False,
    )
```

```python
import functools

import jax
import jax.numpy as jnp
from jax import lax
from jax.experimental import pallas as pl
from jax.experimental.pallas import tpu as pltpu
from jax.sharding import PartitionSpec as P


HEAD_DIM = 64
EPSILON = 1e-05
NEG = -1e30
BF = jnp.bfloat16
F32 = jnp.float32
MESH = pl.DeviceIdType.MESH
CHUNKS = 16
LAG = 3
GROUPS = 4
FFN_GROUPS = 2


def matmul(left, right):
    return jnp.dot(left, right, preferred_element_type=F32)


def mat_trans(left, right):
    return lax.dot_general(left, right, (((1,), (1,)), ((), ())), preferred_element_type=F32)


def trans_mat(left, right):
    return lax.dot_general(left, right, (((0,), (0,)), ((), ())), preferred_element_type=F32)


def exchange(src, dst, axis, bit, send, recv):
    return pltpu.make_async_remote_copy(
        src_ref=src,
        dst_ref=dst,
        send_sem=send,
        recv_sem=recv,
        device_id={axis: lax.axis_index(axis) ^ bit},
        device_id_type=MESH,
    )


def add_into(dst, left, right):
    size = 64

    def one(i, carry):
        cut = pl.ds(pl.multiple_of(i * size, size), size)
        dst[cut, :] = (left[cut, :].astype(F32) + right[cut, :].astype(F32)).astype(BF)
        return carry

    lax.fori_loop(0, dst.shape[0] // size, one, 0)


class Chain:
    def __init__(self, n_ctx, ref, land, send, recv):
        self.ref, self.land, self.send, self.recv = ref, land, send, recv
        self.bits = high_bits(n_ctx)[:-1]

    def _copy(self, j):
        return exchange(self.ref, self.land.at[j], "ctx", self.bits[j], self.send.at[j], self.recv.at[j])

    def start(self):
        self._copy(0).start()

    def finish(self):
        for j in range(len(self.bits)):
            if j > 0:
                self._copy(j).start()
            self._copy(j).wait()
            add_into(self.ref, self.ref, self.land.at[j])


def high_bits(size):
    bits = []
    bit = size // 2
    while bit >= 1:
        bits.append(bit)
        bit //= 2
    return bits


def lanes(shape):
    return lax.broadcasted_iota(jnp.int32, shape, 1)


def head_lanes(ref, h, upper):
    wide = ref[:, (h // 2) * 128 : (h // 2) * 128 + 128]
    if (h % 2 == 1) != upper:
        wide = pltpu.roll(wide.astype(F32), HEAD_DIM, 1).astype(BF)
    keep = (lanes(wide.shape) >= HEAD_DIM) if upper else (lanes(wide.shape) < HEAD_DIM)
    return jnp.where(keep, wide, jnp.zeros_like(wide))


class Relay:
    def __init__(self, n_ctx, src, dst, send, recv):
        self.src, self.dst, self.send, self.recv = src, dst, send, recv
        self.piece = src.shape[0] // n_ctx
        self.ctx = lax.axis_index("ctx")
        self.bits = high_bits(n_ctx)
        self.count = 0
        self.all = []
        self.last = []

    def _copy(self, src, dst, axis, bit):
        e = self.count
        self.count += 1
        copy = pltpu.make_async_remote_copy(
            src_ref=src,
            dst_ref=dst,
            send_sem=self.send.at[e],
            recv_sem=self.recv.at[e],
            device_id={axis: lax.axis_index(axis) ^ bit},
            device_id_type=MESH,
        )
        copy.start()
        self.all.append(copy)
        return copy

    def _cut(self, which):
        return pl.ds(pl.multiple_of(which * self.piece, self.piece), self.piece)

    def start(self):
        mine = self._cut(self.ctx)
        self.last = [self._copy(self.src.at[mine], self.dst.at[mine], "fsdp", 1)]

    def hop(self, j):
        self.landed()
        bit = self.bits[j]
        parts = [self.dst.at[self._cut(self.ctx ^ m)] for m in masks_of(self.bits[:j])]
        self.last = [self._copy(part, part, "ctx", bit) for part in parts]

    def landed(self):
        for copy in self.last:
            copy.wait_recv()
        self.last = []

    def drain(self):
        for copy in self.all:
            copy.wait_send()


def forward_kernel(
    n_ctx,
    n_head,
    span,
    q_ref,
    p_ref,
    wl_ref,
    wr_ref,
    gate_ref,
    up_ref,
    down_ref,
    o_ref,
    lse_ref,
    sum_ref,
    gate_other,
    up_other,
    down_other,
    q_pad,
    ext,
    max_ref,
    acc_ref,
    relay_send,
    relay_recv,
    left,
    right,
    from_lo,
    from_hi,
    *sems,
):
    rows, width = q_ref.shape
    heads = width // HEAD_DIM
    block = lax.axis_index("ctx") * 2 + lax.axis_index("fsdp")
    barrier = line_greet(n_head)
    greet(n_ctx)
    ext[...] = jnp.where(lanes(p_ref.shape) < HEAD_DIM, jnp.ones_like(p_ref[...]), p_ref[...])
    pl.semaphore_wait(barrier, line_peers(n_head) + len(partners(n_ctx)))
    gate = Relay(n_ctx, gate_ref, gate_other, relay_send.at[0], relay_recv.at[0])
    up = Relay(n_ctx, up_ref, up_other, relay_send.at[1], relay_recv.at[1])
    down = Relay(n_ctx, down_ref, down_other, relay_send.at[2], relay_recv.at[2])
    gate.start()
    up.start()
    down.hop(0)
    step, steps, drain = line_sum(n_head, left, right, left, right, sum_ref, from_lo, from_hi, sems)
    size = rows // GROUPS
    stack = heads * size
    sub = min(512, stack)
    per_group = CHUNKS // GROUPS

    def tile(start, first_row, masked):
        cut = pl.ds(start, span)
        for j in range(stack // sub):
            part = pl.ds(j * sub, sub)
            scores = mat_trans(q_pad[part, :], p_ref[cut, :])
            if masked:
                row = first_row + lax.rem(lax.broadcasted_iota(jnp.int32, (sub, span), 0), size)
                col = start + lax.broadcasted_iota(jnp.int32, (sub, span), 1)
                scores = jnp.where(col <= row, scores, NEG)
            old = max_ref[part, :]
            new = jnp.maximum(old, jnp.max(scores, axis=1, keepdims=True))
            weights = jnp.exp(scores - jnp.tile(new, (1, span // 128))).astype(BF)
            acc_ref[part, :] = acc_ref[part, :] * jnp.exp(old - new) + matmul(weights, ext[cut, :])
            max_ref[part, :] = new

    def run(s, carry):
        step(s)
        return carry

    def one_group(g, carry):
        mine = pl.ds(pl.multiple_of(g * size, size), size)
        first_row = block * rows + g * size
        for h in range(heads):
            q_pad[h * size : (h + 1) * size, :] = head_lanes(q_ref.at[mine], h, False)
        max_ref[...] = jnp.full_like(max_ref, NEG)
        acc_ref[...] = jnp.zeros_like(acc_ref)

        tiles = (block + 1) * (rows // span)
        base = (g - 1) * per_group

        def sums(i):
            lax.fori_loop((i * per_group) // tiles, ((i + 1) * per_group) // tiles, lambda j, c: run(base + j, c), 0)

        def full(i, c):
            sums(i)
            tile(pl.multiple_of(i * span, span), first_row, False)
            return c

        lax.fori_loop(0, block * (rows // span), full, 0)
        for j in range(rows // span):
            sums(block * (rows // span) + j)
            tile(pl.multiple_of(block * rows + j * span, span), first_row, True)
        for h in range(heads):
            acc = acc_ref[h * size : (h + 1) * size, :]
            total = acc[:, :HEAD_DIM]
            o_ref[mine, h * HEAD_DIM : (h + 1) * HEAD_DIM] = (acc[:, HEAD_DIM:] / total).astype(BF)
            lse = max_ref[h * size : (h + 1) * size, :] + jnp.log(jnp.concatenate([total, total], axis=1))
            lse_ref[h, :, mine] = lse.T[0:1, :]
        att = o_ref[mine, :]
        left[mine, :] = matmul(att, wl_ref[...]).astype(BF)
        right[mine, :] = matmul(att, wr_ref[...]).astype(BF)
        return carry

    lax.fori_loop(0, GROUPS - 1, one_group, 0)
    gate.hop(0)
    down.hop(1)
    lax.fori_loop(GROUPS - 1, GROUPS, one_group, 0)
    hops = len(high_bits(n_ctx))
    later = [(down, j) for j in range(2, hops)] + [(gate, 1), (up, 0)]
    for j in range(1, hops):
        later += [(up, j)] + ([(gate, j + 1)] if j + 1 < hops else [])
    at = CHUNKS - per_group
    rest = steps - at
    for i, (relay, j) in enumerate(later):
        to = CHUNKS - per_group + (rest * (2 * i + 1)) // (2 * len(later))
        lax.fori_loop(at, to, run, 0)
        at = to
        relay.hop(j)
    lax.fori_loop(at, steps, run, 0)
    for relay in (gate, up, down):
        relay.landed()
        relay.drain()
    drain()


def attend_sum(queries, pair, out_left, out_right, gate, up, down, n_ctx, n_head, collective_id):
    rows, width = queries.shape
    heads = width // HEAD_DIM
    seq = pair.shape[0]
    span = min(512, rows)
    wide = 2 * out_left.shape[1]
    vmem = pl.BlockSpec(memory_space=pltpu.VMEM)
    anywhere = pl.BlockSpec(memory_space=pl.ANY)
    stack = heads * rows // GROUPS
    cost = pl.CostEstimate(flops=50_000_000_000, bytes_accessed=8 * rows * wide, transcendentals=0)
    return pl.pallas_call(
        functools.partial(forward_kernel, n_ctx, n_head, span),
        out_shape=(
            jax.ShapeDtypeStruct((rows, width), BF),
            jax.ShapeDtypeStruct((heads, 1, rows), F32),
            jax.ShapeDtypeStruct((rows, wide), BF),
            jax.ShapeDtypeStruct(gate.shape, BF),
            jax.ShapeDtypeStruct(up.shape, BF),
            jax.ShapeDtypeStruct(down.shape, BF),
        ),
        input_output_aliases={6: 5},
        in_specs=[vmem] * 4 + [anywhere] * 3,
        out_specs=(vmem, vmem, vmem, anywhere, anywhere, anywhere),
        scratch_shapes=[
            pltpu.VMEM((stack, 128), BF),
            pltpu.VMEM((seq, 128), BF),
            pltpu.VMEM((stack, 128), F32),
            pltpu.VMEM((stack, 128), F32),
            pltpu.SemaphoreType.DMA((3, n_ctx)),
            pltpu.SemaphoreType.DMA((3, n_ctx)),
        ]
        + line_scratch(rows, wide),
        compiler_params=pltpu.CompilerParams(collective_id=collective_id, has_side_effects=True),
        cost_estimate=cost,
        name="attend_sum",
    )(queries, pair, out_left, out_right, gate, up, down)


def backward_kernel(
    n_ctx,
    n_head,
    group,
    span,
    q_ref,
    g_ref,
    o_ref,
    lse_ref,
    p_ref,
    left_ref,
    right_ref,
    gate_sent,
    gate_kept,
    up_sent,
    up_kept,
    dq_ref,
    dp_ref,
    sum_ref,
    gate_out,
    up_out,
    q_pad,
    g_pad,
    acc_ref,
    dl_ref,
    gate_land,
    up_land,
    far_land,
    cross_send,
    cross_recv,
    far_send,
    far_recv,
    work_l,
    work_r,
    from_lo,
    from_hi,
    *sems,
):
    rows, width = q_ref.shape
    heads = width // HEAD_DIM
    tiles = rows // span
    block = lax.axis_index("ctx") * 2 + lax.axis_index("fsdp")
    barrier = line_greet(n_head)
    greet(n_ctx)
    dp_ref[...] = jnp.zeros_like(dp_ref)
    acc_ref[...] = jnp.zeros_like(acc_ref)
    for h in range(heads):
        cut = slice(h * HEAD_DIM, (h + 1) * HEAD_DIM)
        q_pad[h] = head_lanes(q_ref, h, False)
        g_pad[h] = head_lanes(g_ref, h, True)
        product = g_ref[:, cut].astype(F32) * o_ref[:, cut].astype(F32)
        dl_ref[h] = jnp.sum(product.T, axis=0, keepdims=True)
    pl.semaphore_wait(barrier, line_peers(n_head) + len(partners(n_ctx)))
    crosses = [
        exchange(sent, land, "fsdp", 1, cross_send.at[i], cross_recv.at[i])
        for i, (sent, land) in enumerate(((gate_sent, gate_land), (up_sent, up_land)))
    ]
    for cross in crosses:
        cross.start()
    far = Chain(n_ctx, gate_out, far_land, far_send, far_recv)
    hop_at = CHUNKS + 2
    step, steps, drain = line_sum(
        n_head, left_ref, right_ref, work_l, work_r, sum_ref, from_lo, from_hi, sems
    )

    def hop():
        crosses[0].wait_recv()
        add_into(gate_out, gate_kept, gate_land)
        far.start()

    def head_tile(h, pairs, start, masked):
        probs = jnp.exp(mat_trans(pairs, q_pad[h]) - lse_ref[h])
        if masked:
            row = block * rows + lax.broadcasted_iota(jnp.int32, (span, rows), 1)
            col = start + lax.broadcasted_iota(jnp.int32, (span, rows), 0)
            probs = jnp.where(col <= row, probs, 0.0)
        grads = (probs * (mat_trans(pairs, g_pad[h]) - dl_ref[h])).astype(BF)
        acc_ref[h] += trans_mat(grads, pairs)
        return matmul(probs.astype(BF), g_pad[h]) + matmul(grads, q_pad[h])

    groups = heads // group

    def two_steps(t):
        for j in range(2):

            @pl.when(2 * t + j < steps)
            def _():
                step(2 * t + j)

        @pl.when(2 * t == hop_at)
        def _():
            hop()

    def full(t, carry):
        two_steps(t)
        first = lax.rem(t, groups) * group
        start = pl.multiple_of((t // groups) * span, span)
        cut = pl.ds(start, span)
        total = head_tile(first, p_ref[cut, :], start, False)
        for h in range(1, group):
            total = total + head_tile(first + h, p_ref[cut, :], start, False)
        dp_ref[cut, :] += total
        return carry

    count = block * tiles * groups
    lax.fori_loop(0, count, full, 0)

    def last(t, carry):
        h = lax.rem(t, heads)

        @pl.when(lax.rem(t, group) == 0)
        def _():
            two_steps(count + t // group)

        start = pl.multiple_of(block * rows + (t // heads) * span, span)
        cut = pl.ds(start, span)
        dp_ref[cut, :] += head_tile(h, p_ref[cut, :], start, True)
        return carry

    lax.fori_loop(0, heads * tiles, last, 0)
    for h in range(heads):
        dq_ref[:, h * HEAD_DIM : (h + 1) * HEAD_DIM] = acc_ref[h][:, :HEAD_DIM]

    begun = 2 * (count + groups * tiles)

    def rest(s, carry):
        step(s)

        @pl.when(s == hop_at)
        def _():
            hop()

        return carry

    lax.fori_loop(jnp.minimum(begun, steps), steps, rest, 0)
    drain()
    crosses[1].wait_recv()
    add_into(up_out, up_kept, up_land)
    for cross in crosses:
        cross.wait_send()
    far.finish()


def attend_back(queries, grads, attended, lse, pair, left, right, parts, n_ctx, n_head, collective_id):
    rows, width = queries.shape
    heads = width // HEAD_DIM
    seq = pair.shape[0]
    group = 4 if heads % 4 == 0 else 2
    span = min(512, rows)
    vmem = pl.BlockSpec(memory_space=pltpu.VMEM)
    flat = jax.ShapeDtypeStruct(parts[0].shape, BF)
    n_far = len(high_bits(n_ctx)) - 1
    cost = pl.CostEstimate(
        flops=32 * rows * seq * width, bytes_accessed=8 * rows * width, transcendentals=0
    )
    return pl.pallas_call(
        functools.partial(backward_kernel, n_ctx, n_head, group, span),
        out_shape=(
            jax.ShapeDtypeStruct((rows, width), F32),
            jax.ShapeDtypeStruct((seq, 2 * HEAD_DIM), F32),
            jax.ShapeDtypeStruct((rows, 2 * left.shape[1]), BF),
            flat,
            flat,
        ),
        in_specs=[vmem] * 11,
        out_specs=(vmem,) * 5,
        scratch_shapes=[
            pltpu.VMEM((heads, rows, 128), BF),
            pltpu.VMEM((heads, rows, 128), BF),
            pltpu.VMEM((heads, rows, 128), F32),
            pltpu.VMEM((heads, 1, rows), F32),
            pltpu.VMEM(flat.shape, BF),
            pltpu.VMEM(flat.shape, BF),
            pltpu.VMEM((n_far,) + flat.shape, BF),
            pltpu.SemaphoreType.DMA((2,)),
            pltpu.SemaphoreType.DMA((2,)),
            pltpu.SemaphoreType.DMA((n_far,)),
            pltpu.SemaphoreType.DMA((n_far,)),
        ]
        + line_scratch(rows, 2 * left.shape[1]),
        compiler_params=pltpu.CompilerParams(collective_id=collective_id, has_side_effects=True),
        cost_estimate=cost,
        name="attend_backward",
    )(queries, grads, attended, lse, pair, left, right, *parts)


def partners(n_ctx):
    return [("fsdp", 1)] + [("ctx", bit) for bit in high_bits(n_ctx)]


def greet(n_ctx):
    barrier = pltpu.get_barrier_semaphore()
    for axis, bit in partners(n_ctx):
        pl.semaphore_signal(
            barrier, inc=1, device_id={axis: lax.axis_index(axis) ^ bit}, device_id_type=MESH
        )
    return barrier


def masks_of(bits):
    masks = [0]
    for bit in bits:
        masks = masks + [m | bit for m in masks]
    return masks


def gather_pairs(n_ctx, rows, all_ref, send, recv):
    x = lax.axis_index("fsdp")
    ctx = lax.axis_index("ctx")
    copies = []

    def part(start, size, axis, bit):
        e = len(copies)
        cut = all_ref.at[pl.ds(pl.multiple_of(start, rows), size)]
        copy = pltpu.make_async_remote_copy(
            src_ref=cut,
            dst_ref=cut,
            send_sem=send.at[e],
            recv_sem=recv.at[e],
            device_id={axis: lax.axis_index(axis) ^ bit},
            device_id_type=MESH,
        )
        copy.start()
        copies.append(copy)
        return copy

    opening = part((ctx * 2 + x) * rows, rows, "fsdp", 1)

    def finish():
        opening.wait_recv()
        done = []
        for bit in high_bits(n_ctx):
            now = [part((ctx ^ m) * 2 * rows, 2 * rows, "ctx", bit) for m in masks_of(done)]
            for copy in now:
                copy.wait_recv()
            done.append(bit)
        for copy in copies:
            copy.wait_send()

    return finish


def project_kernel(
    n_ctx,
    x_ref,
    w_ref,
    gain_ref,
    cos_ref,
    sin_ref,
    wo_ref,
    down_ref,
    q_ref,
    p_ref,
    n_ref,
    w_other,
    gain_other,
    wo_other,
    down_other,
    acc_ref,
    send,
    recv,
    relay_send,
    relay_recv,
    gain_send,
    gain_recv,
):
    rows, width = x_ref.shape
    half = width // 2
    q_width = q_ref.shape[1]
    x_at = lax.axis_index("fsdp")
    block = lax.axis_index("ctx") * 2 + x_at
    barrier = greet(n_ctx)
    pl.semaphore_wait(barrier, len(partners(n_ctx)))
    gains = pltpu.make_async_remote_copy(
        src_ref=gain_ref,
        dst_ref=gain_other,
        send_sem=gain_send,
        recv_sem=gain_recv,
        device_id={"fsdp": 1 - x_at},
        device_id_type=MESH,
    )
    gains.start()
    part = half // 2
    first = [
        Relay(
            n_ctx,
            w_ref.at[pl.ds(i * part, part)],
            w_other.at[pl.ds(i * part, part)],
            relay_send.at[i],
            relay_recv.at[i],
        )
        for i in range(2)
    ]
    second = Relay(n_ctx, wo_ref, wo_other, relay_send.at[2], relay_recv.at[2])
    third = Relay(n_ctx, down_ref, down_other, relay_send.at[3], relay_recv.at[3])
    for relay in first:
        relay.start()
    second.start()
    gains.wait_recv()
    parts = 8
    size = rows // parts
    own = pl.ds(pl.multiple_of(x_at * half, half), half)
    other = pl.ds(pl.multiple_of((1 - x_at) * half, half), half)

    def cut_of(i):
        return pl.ds(pl.multiple_of(i * size, size), size)

    def norm(i, carry):
        cut = cut_of(i)
        left = x_ref[cut, own].astype(F32)
        right = x_ref[cut, other].astype(F32)
        total = jnp.sum(left * left, axis=1, keepdims=True) + jnp.sum(right * right, axis=1, keepdims=True)
        scale = lax.rsqrt(total / width + EPSILON)
        n_ref[cut, :half] = (left * scale * gain_ref[0:1, :]).astype(BF)
        n_ref[cut, half:] = (right * scale * gain_other[0:1, :]).astype(BF)
        return carry

    lax.fori_loop(0, parts, norm, 0)
    for relay in first:
        relay.hop(0)
    third.start()
    second.hop(0)

    def local(i, carry):
        cut = cut_of(i)
        acc_ref[cut, :] = matmul(n_ref[cut, :half], w_ref[...])
        return carry

    lax.fori_loop(0, parts, local, 0)
    for j in range(1, len(high_bits(n_ctx))):
        for relay in first:
            relay.hop(j)
    for relay in first:
        relay.landed()

    def rotated(wide, cut):
        low = lax.rem(lanes(wide.shape), HEAD_DIM) < HEAD_DIM // 2
        turned = jnp.where(low, pltpu.roll(wide, 128 - HEAD_DIM // 2, 1), pltpu.roll(wide, HEAD_DIM // 2, 1))
        return wide * cos_ref[cut, :] + turned * sin_ref[cut, :]

    def pairs(i, carry):
        cut = cut_of(i)
        both = acc_ref[cut, q_width:] + matmul(n_ref[cut, half:], w_other[:, q_width:])
        pair = jnp.where(lanes(both.shape) < HEAD_DIM, rotated(both, cut), both)
        p_ref[pl.ds(pl.multiple_of(block * rows + i * size, size), size), :] = pair.astype(BF)
        return carry

    def queries(i, carry):
        cut = cut_of(i)
        whole = acc_ref[cut, :q_width] + matmul(n_ref[cut, half:], w_other[:, :q_width])
        for j in range(q_width // 128):
            sl = slice(j * 128, (j + 1) * 128)
            q_ref[cut, sl] = (rotated(whole[:, sl], cut) * 0.125).astype(BF)
        return carry

    lax.fori_loop(0, parts, pairs, 0)
    finish = gather_pairs(n_ctx, rows, p_ref, send, recv)
    lax.fori_loop(0, parts, queries, 0)
    finish()
    for j in range(1, len(high_bits(n_ctx))):
        second.hop(j)
    second.landed()
    third.landed()
    for relay in first + [second, third]:
        relay.drain()
    gains.wait_send()


def project(inputs, w_local, gains, cosine, sine, w_out, w_down, q_width, n_ctx, collective_id):
    rows, width = inputs.shape
    vmem = pl.BlockSpec(memory_space=pltpu.VMEM)
    anywhere = pl.BlockSpec(memory_space=pl.ANY)
    return pl.pallas_call(
        functools.partial(project_kernel, n_ctx),
        out_shape=(
            jax.ShapeDtypeStruct((rows, q_width), BF),
            jax.ShapeDtypeStruct((rows * 2 * n_ctx, 2 * HEAD_DIM), BF),
            jax.ShapeDtypeStruct((rows, width), BF),
            jax.ShapeDtypeStruct(w_local.shape, BF),
            jax.ShapeDtypeStruct(gains.shape, F32),
            jax.ShapeDtypeStruct(w_out.shape, BF),
            jax.ShapeDtypeStruct(w_down.shape, BF),
        ),
        in_specs=[vmem] * 5 + [anywhere] * 2,
        out_specs=(vmem,) * 5 + (anywhere,) * 2,
        scratch_shapes=[
            pltpu.VMEM((rows, w_local.shape[1]), F32),
            pltpu.SemaphoreType.DMA((n_ctx,)),
            pltpu.SemaphoreType.DMA((n_ctx,)),
            pltpu.SemaphoreType.DMA((4, n_ctx)),
            pltpu.SemaphoreType.DMA((4, n_ctx)),
            pltpu.SemaphoreType.DMA,
            pltpu.SemaphoreType.DMA,
        ],
        compiler_params=pltpu.CompilerParams(collective_id=collective_id, has_side_effects=True),
        name="project",
    )(inputs, w_local, gains, cosine, sine, w_out, w_down)


def line_sum(n, left, right, work_l, work_r, o_ref, from_lo, from_hi, sems):
    s_up, r_up, s_dn, r_dn, s_a, r_a, s_b, r_b = sems
    me = lax.axis_index("head")
    rows, cols = left.shape
    size = rows // CHUNKS
    has_lo = me > 0
    has_hi = me < n - 1
    middle = jnp.logical_and(has_lo, has_hi)

    def at(k):
        return pl.ds(pl.multiple_of(k * size, size), size)

    def remote(src, dst, send, recv, target):
        return pltpu.make_async_remote_copy(
            src_ref=src,
            dst_ref=dst,
            send_sem=send,
            recv_sem=recv,
            device_id={"head": target},
            device_id_type=MESH,
        )

    def up(k, src):
        return remote(src.at[at(k)], from_lo.at[at(k)], s_up.at[k], r_up.at[k], me + 1)

    def down(k, src):
        return remote(src.at[at(k)], from_hi.at[at(k)], s_dn.at[k], r_dn.at[k], me - 1)

    def spread_a(k):
        part = o_ref.at[at(k), pl.ds(0, cols)]
        return remote(part, part, s_a.at[k], r_a.at[k], me + 1)

    def spread_b(k):
        part = o_ref.at[at(k), pl.ds(cols, cols)]
        return remote(part, part, s_b.at[k], r_b.at[k], me - 1)

    def valid(k):
        return jnp.logical_and(k >= 0, k < CHUNKS)

    def added(mine, there, k):
        return (mine[at(k), :].astype(F32) + there[at(k), :].astype(F32)).astype(BF)

    def step(s):
        k1 = s - LAG * me
        k2 = s - LAG * (n - 1 - me)
        k3 = s - LAG * (n - 1 + me)
        k4 = s - LAG * (2 * (n - 1) - me)

        @pl.when(jnp.logical_and(valid(k1), me == 0))
        def _():
            up(k1, right).start()

        @pl.when(jnp.logical_and(valid(k2), me == n - 1))
        def _():
            down(k2, left).start()

        @pl.when(jnp.logical_and(valid(k1), middle))
        def _():
            up(k1, right).wait_recv()
            work_r[at(k1), :] = added(right, from_lo, k1)
            up(k1, work_r).start()

        @pl.when(jnp.logical_and(valid(k1), me == n - 1))
        def _():
            up(k1, right).wait_recv()
            o_ref[at(k1), cols:] = added(right, from_lo, k1)
            spread_b(k1).start()

        @pl.when(jnp.logical_and(valid(k2), middle))
        def _():
            down(k2, left).wait_recv()
            work_l[at(k2), :] = added(left, from_hi, k2)
            down(k2, work_l).start()

        @pl.when(jnp.logical_and(valid(k2), me == 0))
        def _():
            down(k2, left).wait_recv()
            o_ref[at(k2), :cols] = added(left, from_hi, k2)
            spread_a(k2).start()

        @pl.when(jnp.logical_and(valid(k3), has_lo))
        def _():
            spread_a(k3).wait_recv()

            @pl.when(has_hi)
            def _():
                spread_a(k3).start()

        @pl.when(jnp.logical_and(valid(k4), has_hi))
        def _():
            spread_b(k4).wait_recv()

            @pl.when(has_lo)
            def _():
                spread_b(k4).start()

    def drain():
        def one(k, carry):
            @pl.when(has_hi)
            def _():
                up(k, right).wait_send()
                spread_a(k).wait_send()

            @pl.when(has_lo)
            def _():
                down(k, left).wait_send()
                spread_b(k).wait_send()

            return carry

        lax.fori_loop(0, CHUNKS, one, 0)

    return step, CHUNKS + 2 * LAG * (n - 1), drain


def line_greet(n):
    me = lax.axis_index("head")
    barrier = pltpu.get_barrier_semaphore()

    @pl.when(me > 0)
    def _():
        pl.semaphore_signal(barrier, inc=1, device_id={"head": me - 1}, device_id_type=MESH)

    @pl.when(me < n - 1)
    def _():
        pl.semaphore_signal(barrier, inc=1, device_id={"head": me + 1}, device_id_type=MESH)

    return barrier


def line_peers(n):
    me = lax.axis_index("head")
    return jnp.where(me > 0, 1, 0) + jnp.where(me < n - 1, 1, 0)


def line_scratch(rows, width):
    return [pltpu.VMEM((rows, width // 2), BF)] * 4 + [pltpu.SemaphoreType.DMA((CHUNKS,))] * 8


def last_kernel(
    n_ctx,
    n_head,
    dq_ref,
    part_ref,
    cos_ref,
    sin_ref,
    w_l,
    w_r,
    n_ref,
    att_ref,
    low_ref,
    up_ref,
    gate_ref,
    down_ref,
    sum_ref,
    qkv_full,
    out_full,
    gate_full,
    up_full,
    down_full,
    work,
    land,
    raw,
    raw_land,
    n_land,
    low_land,
    att_land,
    up_sum,
    out_sent,
    out_kept,
    out_land,
    qkv_sent,
    qkv_kept,
    qkv_land,
    up_far,
    out_far,
    qkv_far,
    pair_send,
    pair_recv,
    trade_send,
    trade_recv,
    cross_send,
    cross_recv,
    far_send,
    far_recv,
    full_send,
    full_recv,
    full_local,
    left,
    right,
    from_lo,
    from_hi,
    *sems,
):
    rows, q_width = dq_ref.shape
    half = n_ref.shape[1] // 2
    quarter = half // 2
    x_at = lax.axis_index("fsdp")
    ctx = lax.axis_index("ctx")
    core = lax.rem(ctx, 2)
    barrier = line_greet(n_head)
    greet(n_ctx)
    work[...] = part_ref[...].astype(BF)
    up_sum[...] = up_ref[...]
    pl.semaphore_wait(barrier, line_peers(n_head) + len(partners(n_ctx)))

    def relative(side, c):
        return pl.ds(pl.multiple_of(side * half + c * quarter, quarter), quarter)

    def trade(src, dst, at):
        return exchange(src, dst, "ctx", 1, trade_send.at[at], trade_recv.at[at])

    pairs = []
    used = [0]

    def give(start, size, axis, bit):
        e = len(pairs)
        cut = pl.ds(pl.multiple_of(start, rows), size)
        copy = exchange(
            work.at[cut], land.at[pl.ds(used[0], size)], axis, bit, pair_send.at[e], pair_recv.at[e]
        )
        copy.start()
        pairs.append(copy)
        used[0] += size
        return copy, used[0] - size

    def take(start, size, at):
        cut = pl.ds(pl.multiple_of(start, rows), size)
        work[cut, :] = (work[cut, :].astype(F32) + land[at : at + size, :].astype(F32)).astype(BF)

    up_chain = Chain(n_ctx, up_sum, up_far, far_send.at[0], far_recv.at[0])
    out_chain = Chain(n_ctx, out_kept, out_far, far_send.at[1], far_recv.at[1])
    qkv_chain = Chain(n_ctx, qkv_kept, qkv_far, far_send.at[2], far_recv.at[2])

    def turned(wide, cut):
        low = lax.rem(lanes(wide.shape), HEAD_DIM) < HEAD_DIM // 2
        swapped = jnp.where(low, pltpu.roll(wide, 128 - HEAD_DIM // 2, 1), pltpu.roll(wide, HEAD_DIM // 2, 1))
        return wide * cos_ref[cut, :] - swapped * sin_ref[cut, :]

    def rotate_rows(i, carry):
        cut = pl.ds(pl.multiple_of(i * 128, 128), 128)
        for j in range(q_width // 128):
            sl = slice(j * 128, (j + 1) * 128)
            raw[cut, sl] = turned(dq_ref[cut, sl] * 0.125, cut).astype(BF)
        return carry

    bits = high_bits(n_ctx)
    trades = []
    for j in range(len(bits)):
        bit = bits[len(bits) - 1 - j]
        masks = masks_of(bits[: len(bits) - 1 - j])
        now = [give((ctx ^ bit ^ m) * 2 * rows, 2 * rows, "ctx", bit) for m in masks]
        if j == 0:
            lax.fori_loop(0, rows // 128, rotate_rows, 0)
        for (copy, at), m in zip(now, masks):
            copy.wait_recv()
            take((ctx ^ m) * 2 * rows, 2 * rows, at)
    copy, at = give((ctx * 2 + 1 - x_at) * rows, rows, "fsdp", 1)
    up_chain.start()
    trades = [trade(att_ref, att_land, 0)]
    for side in range(2):
        trades.append(trade(low_ref.at[:, relative(side, 1 - core)], low_land.at[:, pl.ds(side * quarter, quarter)], 1 + side))
        trades.append(trade(n_ref.at[:, relative(side, 1 - core)], n_land.at[:, pl.ds(side * quarter, quarter)], 3 + side))
    for t in trades:
        t.start()
    copy.wait_recv()
    base = pl.multiple_of((ctx * 2 + x_at) * rows, rows)

    def finish_pair(i, carry):
        cut = pl.ds(pl.multiple_of(i * 128, 128), 128)
        mine = work[pl.ds(base + i * 128, 128), :].astype(F32) + land[pl.ds(at + i * 128, 128), :].astype(F32)
        raw[cut, q_width:] = jnp.where(lanes(mine.shape) < HEAD_DIM, turned(mine, cut), mine).astype(BF)
        left[cut, :] = mat_trans(raw[cut, :], w_l[...]).astype(BF)
        right[cut, :] = mat_trans(raw[cut, :], w_r[...]).astype(BF)
        return carry

    lax.fori_loop(0, rows // 128, finish_pair, 0)
    raw_trade = trade(raw, raw_land, 5)
    raw_trade.start()
    trades.append(raw_trade)
    step, steps, drain = line_sum(n_head, left, right, left, right, sum_ref, from_lo, from_hi, sems)

    def run(s, carry):
        step(s)
        return carry

    def spread(src, whole, by_rows, e):
        size = src.shape[0 if by_rows else 1]
        cut = pl.ds(pl.multiple_of(core * size, size), size)
        dst = whole.at[cut] if by_rows else whole.at[:, cut]
        return (
            pltpu.make_async_copy(src, dst, full_local.at[e]),
            exchange(src, dst, "ctx", 1, full_send.at[e], full_recv.at[e]),
        )

    spreads = [spread(gate_ref, gate_full, True, 0), spread(down_ref, down_full, False, 1)]
    for pair in spreads:
        for copy in pair:
            copy.start()

    def out_tiles(dst, side):
        def one(t, carry):
            cut = pl.ds(pl.multiple_of(t * 128, 128), 128)
            dst[cut, :] = (
                trans_mat(att_ref[:, cut], low_ref[:, relative(side, core)])
                + trans_mat(att_land[:, cut], low_land[:, side * quarter : (side + 1) * quarter])
            ).astype(BF)
            step(steps_at + t)
            return carry

        lax.fori_loop(0, q_width // 128, one, 0)

    def qkv_tiles(dst, side):
        def one(t, carry):
            cut = pl.ds(pl.multiple_of(t * 128, 128), 128)
            there = pl.ds(pl.multiple_of(side * half + core * quarter + t * 128, 128), 128)
            landing = pl.ds(pl.multiple_of(side * quarter + t * 128, 128), 128)
            dst[cut, :] = (
                trans_mat(n_ref[:, there], raw[...]) + trans_mat(n_land[:, landing], raw_land[...])
            ).astype(BF)
            step(steps_at + t)
            return carry

        lax.fori_loop(0, quarter // 128, one, 0)

    lax.fori_loop(0, 2, run, 0)
    for t in trades:
        t.wait_recv()
    steps_at = 2
    out_tiles(out_sent, 1)
    out_cross = exchange(out_sent, out_land, "fsdp", 1, cross_send.at[0], cross_recv.at[0])
    out_cross.start()
    steps_at += q_width // 128
    qkv_tiles(qkv_sent, 1)
    qkv_cross = exchange(qkv_sent, qkv_land, "fsdp", 1, cross_send.at[1], cross_recv.at[1])
    qkv_cross.start()
    steps_at += quarter // 128
    out_tiles(out_kept, 0)
    steps_at += q_width // 128
    qkv_tiles(qkv_kept, 0)
    steps_at += quarter // 128
    out_cross.wait_recv()
    add_into(out_kept, out_kept, out_land)
    out_chain.start()
    rest = steps - steps_at
    lax.fori_loop(steps_at, steps_at + rest // 4, run, 0)
    qkv_cross.wait_recv()
    add_into(qkv_kept, qkv_kept, qkv_land)
    qkv_chain.start()
    lax.fori_loop(steps_at + rest // 4, steps_at + rest // 2, run, 0)
    up_chain.finish()
    spreads.append(spread(up_sum, up_full, True, 2))
    for copy in spreads[-1]:
        copy.start()
    lax.fori_loop(steps_at + rest // 2, steps, run, 0)
    out_chain.finish()
    spreads.append(spread(out_kept, out_full, False, 3))
    for copy in spreads[-1]:
        copy.start()
    qkv_chain.finish()
    spreads.append(spread(qkv_kept, qkv_full, True, 4))
    for copy in spreads[-1]:
        copy.start()
    drain()
    for t in pairs + trades + [out_cross, qkv_cross]:
        t.wait_send()
    for local, remote in spreads:
        local.wait()
        remote.wait()


def last_sum(
    dq, part, cosine, sine, w_left, w_right, normed, attended, low, up, gate, down, n_ctx, n_head, collective_id
):
    rows, q_width = dq.shape
    width = normed.shape[1]
    half = width // 2
    quarter = half // 2
    narrow = w_left.shape[1]
    units = gate.shape[1]
    n_far = len(high_bits(n_ctx)) - 1
    vmem = pl.BlockSpec(memory_space=pltpu.VMEM)
    anywhere = pl.BlockSpec(memory_space=pl.ANY)
    dma = pltpu.SemaphoreType.DMA
    return pl.pallas_call(
        functools.partial(last_kernel, n_ctx, n_head),
        out_shape=(
            jax.ShapeDtypeStruct((rows, width), BF),
            jax.ShapeDtypeStruct((half, narrow), BF),
            jax.ShapeDtypeStruct((q_width, half), BF),
            jax.ShapeDtypeStruct((half, units), BF),
            jax.ShapeDtypeStruct((half, units), BF),
            jax.ShapeDtypeStruct((units, half), BF),
        ),
        in_specs=[vmem] * 12,
        out_specs=(vmem,) + (anywhere,) * 5,
        scratch_shapes=[
            pltpu.VMEM(part.shape, BF),
            pltpu.VMEM(part.shape, BF),
            pltpu.VMEM((rows, narrow), BF),
            pltpu.VMEM((rows, narrow), BF),
            pltpu.VMEM((rows, half), BF),
            pltpu.VMEM((rows, half), BF),
            pltpu.VMEM((rows, q_width), BF),
            pltpu.VMEM(up.shape, BF),
            pltpu.VMEM((q_width, quarter), BF),
            pltpu.VMEM((q_width, quarter), BF),
            pltpu.VMEM((q_width, quarter), BF),
            pltpu.VMEM((quarter, narrow), BF),
            pltpu.VMEM((quarter, narrow), BF),
            pltpu.VMEM((quarter, narrow), BF),
            pltpu.VMEM((n_far,) + up.shape, BF),
            pltpu.VMEM((n_far, q_width, quarter), BF),
            pltpu.VMEM((n_far, quarter, narrow), BF),
            dma((n_ctx,)),
            dma((n_ctx,)),
            dma((6,)),
            dma((6,)),
            dma((2,)),
            dma((2,)),
            dma((3, n_far)),
            dma((3, n_far)),
            dma((5,)),
            dma((5,)),
            dma((5,)),
        ]
        + line_scratch(rows, width),
        compiler_params=pltpu.CompilerParams(
            collective_id=collective_id, has_side_effects=True, vmem_limit_bytes=66_000_000
        ),
        cost_estimate=pl.CostEstimate(
            flops=50_000_000_000, bytes_accessed=8 * rows * width, transcendentals=0
        ),
        name="last_sum",
    )(dq, part, cosine, sine, w_left, w_right, normed, attended, low, up, gate, down)


def ffn_kernel(
    n_head,
    x_ref,
    mix_ref,
    cot_ref,
    gain_ref,
    gain_other,
    gate_l,
    gate_r,
    up_l,
    up_r,
    down_l,
    down_r,
    sum_ref,
    n_ref,
    ffn_left,
    ffn_right,
    down_kept,
    gate_kept,
    gate_sent,
    up_kept,
    up_sent,
    act_ref,
    gig_ref,
    uig_ref,
    cot_land,
    n_land,
    act_land,
    gig_land,
    uig_land,
    down_sent,
    down_land,
    out_tile,
    out_sem,
    trade_send,
    trade_recv,
    cross_send,
    cross_recv,
    left,
    right,
    from_lo,
    from_hi,
    *sems,
):
    rows, width = x_ref.shape
    half = width // 2
    quarter = half // 2
    units = act_ref.shape[1]
    x_at = lax.axis_index("fsdp")
    ctx_at = lax.axis_index("ctx")
    core = lax.rem(ctx_at, 2)
    own = pl.ds(pl.multiple_of(x_at * half, half), half)
    other = pl.ds(pl.multiple_of((1 - x_at) * half, half), half)
    barrier = line_greet(n_head)
    pl.semaphore_signal(barrier, inc=1, device_id={"fsdp": 1 - x_at}, device_id_type=MESH)
    pl.semaphore_signal(barrier, inc=1, device_id={"ctx": ctx_at ^ 1}, device_id_type=MESH)
    pl.semaphore_wait(barrier, line_peers(n_head) + 2)

    def trade(src, dst, at):
        return pltpu.make_async_remote_copy(
            src_ref=src,
            dst_ref=dst,
            send_sem=trade_send.at[at],
            recv_sem=trade_recv.at[at],
            device_id={"ctx": ctx_at ^ 1},
            device_id_type=MESH,
        )

    def absolute(side, c):
        start = (x_at if side == 0 else 1 - x_at) * half + c * quarter
        return pl.ds(pl.multiple_of(start, quarter), quarter)

    def relative(side, c):
        return pl.ds(pl.multiple_of(side * half + c * quarter, quarter), quarter)

    cot_trades = [
        trade(cot_ref.at[:, absolute(j, 1 - core)], cot_land.at[:, pl.ds(j * quarter, quarter)], j)
        for j in range(2)
    ]
    for copy in cot_trades:
        copy.start()

    def row_trades(g):
        mine = pl.ds(pl.multiple_of(g * (rows // FFN_GROUPS), rows // FFN_GROUPS), rows // FFN_GROUPS)
        at = 2 + g * 5
        return [
            trade(act_ref.at[mine], act_land.at[mine], at),
            trade(gig_ref.at[mine], gig_land.at[mine], at + 1),
            trade(uig_ref.at[mine], uig_land.at[mine], at + 2),
            trade(n_ref.at[mine, relative(0, 1 - core)], n_land.at[mine, pl.ds(0, quarter)], at + 3),
            trade(n_ref.at[mine, relative(1, 1 - core)], n_land.at[mine, pl.ds(quarter, quarter)], at + 4),
        ]

    step, steps, drain = line_sum(n_head, left, right, left, right, sum_ref, from_lo, from_hi, sems)

    def run(s, carry):
        step(s)
        return carry

    size = rows // FFN_GROUPS
    per_group = CHUNKS // FFN_GROUPS

    def one_group(g, carry):
        mine = pl.ds(pl.multiple_of(g * size, size), size)
        base = (g - 1) * per_group
        stops = [base + (per_group * i) // 4 for i in range(5)]
        hid_l = x_ref[mine, own].astype(F32) + mix_ref[mine, :half].astype(F32)
        hid_r = x_ref[mine, other].astype(F32) + mix_ref[mine, half:].astype(F32)
        total = jnp.sum(hid_l * hid_l, axis=1, keepdims=True) + jnp.sum(hid_r * hid_r, axis=1, keepdims=True)
        scale = lax.rsqrt(total / width + EPSILON)
        n_ref[mine, :half] = (hid_l * scale * gain_ref[1:2, :]).astype(BF)
        n_ref[mine, half:] = (hid_r * scale * gain_other[1:2, :]).astype(BF)
        lax.fori_loop(stops[0], stops[1], run, 0)
        gate = matmul(n_ref[mine, :half], gate_l[...]) + matmul(n_ref[mine, half:], gate_r[...])
        up = matmul(n_ref[mine, :half], up_l[...]) + matmul(n_ref[mine, half:], up_r[...])
        lax.fori_loop(stops[1], stops[2], run, 0)
        sigma = jax.nn.sigmoid(gate)
        silu = gate * sigma
        act_ref[mine, :] = (silu * up).astype(BF)
        grad = mat_trans(cot_ref[mine, own], down_l[...]) + mat_trans(cot_ref[mine, other], down_r[...])
        gig_ref[mine, :] = (grad * up * sigma * (1.0 + gate * (1.0 - sigma))).astype(BF)
        uig_ref[mine, :] = (grad * silu).astype(BF)
        lax.fori_loop(stops[2], stops[3], run, 0)
        gig = gig_ref[mine, :]
        uig = uig_ref[mine, :]
        left[mine, :] = (mat_trans(gig, gate_l[...]) + mat_trans(uig, up_l[...])).astype(BF)
        lax.fori_loop(stops[3], stops[4], run, 0)
        right[mine, :] = (mat_trans(gig, gate_r[...]) + mat_trans(uig, up_r[...])).astype(BF)
        for copy in row_trades(g):
            copy.start()
        return carry

    lax.fori_loop(0, FFN_GROUPS, one_group, 0)
    first = CHUNKS - per_group
    rest = steps - first
    tile = 128
    down_tiles = units // tile
    row_tiles = quarter // tile
    total_work = down_tiles + 4 * row_tiles + 2 * FFN_GROUPS

    def sums(i, weight=1):
        lax.fori_loop(
            first + (rest * i) // total_work, first + (rest * (i + weight)) // total_work, run, 0
        )

    for copy in cot_trades:
        copy.wait_recv()

    def landed(g, carry):
        for copy in row_trades(g):
            copy.wait_recv()
        return carry

    lax.fori_loop(0, FFN_GROUPS, landed, 0)

    def down_tile(t, carry):
        sums(t)
        cut = pl.ds(pl.multiple_of(t * tile, tile), tile)
        mine = act_ref[:, cut]
        theirs = act_land[:, cut]
        for dst, side in ((down_sent, 1), (down_kept, 0)):
            dst[cut, :] = (
                trans_mat(mine, cot_ref[:, absolute(side, core)])
                + trans_mat(theirs, cot_land[:, side * quarter : (side + 1) * quarter])
            ).astype(BF)
        return carry

    lax.fori_loop(0, down_tiles, down_tile, 0)
    cross = pltpu.make_async_remote_copy(
        src_ref=down_sent,
        dst_ref=down_land,
        send_sem=cross_send,
        recv_sem=cross_recv,
        device_id={"fsdp": 1 - x_at},
        device_id_type=MESH,
    )
    cross.start()
    done = down_tiles

    def out_copy(dst, t, slot):
        cut = pl.ds(pl.multiple_of(t * tile, tile), tile)
        return pltpu.make_async_copy(out_tile.at[slot], dst.at[cut], out_sem.at[slot])

    outs = (
        (gate_sent, 1, gig_ref, gig_land),
        (gate_kept, 0, gig_ref, gig_land),
        (up_sent, 1, uig_ref, uig_land),
        (up_kept, 0, uig_ref, uig_land),
    )
    for dst, side, own_grad, their_grad in outs:

        def row_tile(t, carry):
            sums(done + t)
            slot = lax.rem(t, 2)
            there = pl.ds(pl.multiple_of(side * half + core * quarter + t * tile, tile), tile)
            landing = pl.ds(pl.multiple_of(side * quarter + t * tile, tile), tile)
            value = (
                trans_mat(n_ref[:, there], own_grad[...]) + trans_mat(n_land[:, landing], their_grad[...])
            ).astype(BF)

            @pl.when(t >= 2)
            def _():
                out_copy(dst, t - 2, slot).wait()

            out_tile[slot] = value
            out_copy(dst, t, slot).start()
            return carry

        lax.fori_loop(0, row_tiles, row_tile, 0)
        for t in range(max(row_tiles - 2, 0), row_tiles):
            out_copy(dst, t, t % 2).wait()
        done += row_tiles

    def project_down(g, carry):
        mine = pl.ds(pl.multiple_of(g * size, size), size)
        sums(done + 2 * g, 2)
        ffn_left[mine, :] = matmul(act_ref[mine, :], down_l[...]).astype(BF)
        ffn_right[mine, :] = matmul(act_ref[mine, :], down_r[...]).astype(BF)
        return carry

    lax.fori_loop(0, FFN_GROUPS, project_down, 0)
    cross.wait_recv()

    def finish(t, carry):
        cut = pl.ds(pl.multiple_of(t * tile, tile), tile)
        down_kept[cut, :] = (down_kept[cut, :].astype(F32) + down_land[cut, :].astype(F32)).astype(BF)
        return carry

    lax.fori_loop(0, down_tiles, finish, 0)
    cross.wait_send()
    for copy in cot_trades:
        copy.wait_send()

    def sent(g, carry):
        for copy in row_trades(g):
            copy.wait_send()
        return carry

    lax.fori_loop(0, FFN_GROUPS, sent, 0)
    drain()


def ffn_sum(inputs, mixed, cot, gains, gains_other, gate, gate_o, up, up_o, down, down_o, n_head, collective_id):
    rows, width = inputs.shape
    units = gate.shape[1]
    vmem = pl.BlockSpec(memory_space=pltpu.VMEM)
    wide = jax.ShapeDtypeStruct((rows, width), BF)
    narrow = jax.ShapeDtypeStruct((rows, width // 2), BF)
    quarter = width // 4
    flat = jax.ShapeDtypeStruct((quarter, units), BF)
    trades = 2 + 5 * FFN_GROUPS
    return pl.pallas_call(
        functools.partial(ffn_kernel, n_head),
        out_shape=(wide, wide, narrow, narrow, jax.ShapeDtypeStruct((units, quarter), BF)) + (flat,) * 4,
        in_specs=[vmem] * 11,
        out_specs=(vmem,) * 5 + (pl.BlockSpec(memory_space=pl.ANY),) * 4,
        scratch_shapes=[pltpu.VMEM((rows, units), BF)] * 3
        + [pltpu.VMEM((rows, width // 2), BF)] * 2
        + [pltpu.VMEM((rows, units), BF)] * 3
        + [pltpu.VMEM((units, quarter), BF)] * 2
        + [
            pltpu.VMEM((2, 128, units), BF),
            pltpu.SemaphoreType.DMA((2,)),
            pltpu.SemaphoreType.DMA((trades,)),
            pltpu.SemaphoreType.DMA((trades,)),
            pltpu.SemaphoreType.DMA,
            pltpu.SemaphoreType.DMA,
        ]
        + line_scratch(rows, width),
        compiler_params=pltpu.CompilerParams(
            collective_id=collective_id, has_side_effects=True, vmem_limit_bytes=66_000_000
        ),
        cost_estimate=pl.CostEstimate(
            flops=50_000_000_000, bytes_accessed=8 * rows * width, transcendentals=0
        ),
        name="ffn_sum",
    )(inputs, mixed, cot, gains, gains_other, gate, gate_o, up, up_o, down, down_o)


def flip(array, axis, bit, size):
    return lax.ppermute(array, axis, [(i, i ^ bit) for i in range(size)])


def shards(
    n_ctx,
    n_head,
    inputs,
    query_weight,
    key_weight,
    value_weight,
    output_weight,
    gate_weight,
    up_weight,
    down_weight,
    attn_gain,
    ffn_gain,
    cotangent,
):
    rows, width = inputs.shape
    half = width // 2
    x_at = lax.axis_index("fsdp")
    ctx_at = lax.axis_index("ctx")
    core = lax.rem(ctx_at, 2)
    block = ctx_at * 2 + x_at
    block_arr = jnp.reshape(block, (1,)).astype(jnp.int32)

    def own_first(array):
        swapped = jnp.concatenate([array[:, half:], array[:, :half]], axis=1)
        return jnp.where(x_at == 0, array, swapped)

    every = high_bits(n_ctx)

    q_width = query_weight.shape[1]
    half_dim = HEAD_DIM // 2
    positions = block * rows + jnp.arange(rows, dtype=jnp.int32)
    lane = lax.broadcasted_iota(jnp.int32, (rows, 2 * HEAD_DIM), 1)
    freqs = 10000.0 ** (-2.0 * (lane % half_dim).astype(F32) / HEAD_DIM)
    angles = positions.astype(F32)[:, None] * freqs
    cosine = jnp.cos(angles)
    sine = jnp.sin(angles)
    signed = jnp.where(lane % HEAD_DIM < half_dim, -sine, sine)
    qkv_local = jnp.concatenate([query_weight, key_weight, value_weight], axis=1)
    gains_local = jnp.concatenate([attn_gain[None], ffn_gain[None], jnp.zeros((6, half), BF)]).astype(F32)
    queries, pair, normed_one, qkv_other, gains_other, out_other, down_begun = project(
        inputs, qkv_local, gains_local, cosine, signed, output_weight, down_weight, q_width, n_ctx, 4
    )
    attended, lse, mixed, gate_other, up_other, down_other = attend_sum(
        queries, pair, output_weight, out_other, gate_weight, up_weight, down_begun, n_ctx, n_head, 1
    )
    low_sum, _, down_left, down_right, down_kept, gate_kept, gate_sent, up_kept, up_sent = ffn_sum(
        inputs,
        mixed,
        cotangent,
        gains_local,
        gains_other,
        gate_weight,
        gate_other,
        up_weight,
        up_other,
        down_weight,
        down_other,
        n_head,
        2,
    )
    normed_two_grad = low_sum.astype(F32)
    gain_one = jnp.concatenate([gains_local[0], gains_other[0]])
    gain_two = jnp.concatenate([gains_local[1], gains_other[1]])
    late_inputs, late_cot, normed_one, _ = lax.optimization_barrier((inputs, cotangent, normed_one, low_sum))
    in_float = own_first(late_inputs).astype(F32)
    cot = own_first(late_cot)
    scale_one = lax.rsqrt(jnp.mean(in_float * in_float, axis=-1, keepdims=True) + EPSILON)
    unit_one = in_float * scale_one
    hidden = in_float + mixed.astype(F32)
    scale_two = lax.rsqrt(jnp.mean(hidden * hidden, axis=-1, keepdims=True) + EPSILON)
    unit_two = hidden * scale_two
    scaled_two = normed_two_grad * gain_two
    gain_two_part = jnp.sum(normed_two_grad * unit_two, axis=0)
    hidden_grad = cot.astype(F32) + scale_two * (
        scaled_two - unit_two * jnp.mean(scaled_two * unit_two, axis=-1, keepdims=True)
    )
    hidden_low = hidden_grad.astype(BF)

    attended_grad = (
        mat_trans(hidden_low[:, :half], output_weight) + mat_trans(hidden_low[:, half:], out_other)
    ).astype(BF)
    down_far = down_kept
    for bit in every[:-1]:
        down_far = (down_far.astype(F32) + flip(down_far, "ctx", bit, n_ctx).astype(F32)).astype(BF)
    query_acc, pair_acc, ffn_out, gate_far, up_kept = attend_back(
        queries,
        attended_grad,
        attended,
        lse,
        pair,
        down_left,
        down_right,
        (gate_sent, gate_kept, up_sent, up_kept),
        n_ctx,
        n_head,
        6,
    )
    outputs = own_first((hidden + ffn_out.astype(F32)).astype(BF))
    last, qkv_full, out_full, gate_full, up_full, down_full = last_sum(
        query_acc,
        pair_acc,
        cosine,
        signed,
        qkv_local,
        qkv_other,
        normed_one,
        attended,
        hidden_low,
        up_kept,
        gate_far,
        down_far,
        n_ctx,
        n_head,
        3,
    )
    normed_one_grad = last.astype(F32)
    gain_one_part = jnp.sum(normed_one_grad * unit_one, axis=0)
    scaled_one = normed_one_grad * gain_one
    input_grad = own_first(
        hidden_grad
        + scale_one
        * (scaled_one - unit_one * jnp.mean(scaled_one * unit_one, axis=-1, keepdims=True))
    )

    query_grad = qkv_full[:, :q_width].astype(F32)
    key_grad = qkv_full[:, q_width : q_width + HEAD_DIM].astype(F32)
    value_grad = qkv_full[:, q_width + HEAD_DIM :].astype(F32)

    gain_parts = jnp.stack([gain_one_part, gain_two_part])
    gain_kept = gain_parts[:, :half] + flip(gain_parts[:, half:], "fsdp", 1, 2)
    for bit in every:
        gain_kept = gain_kept + flip(gain_kept, "ctx", bit, n_ctx)

    return (
        outputs,
        input_grad,
        query_grad,
        key_grad,
        value_grad,
        out_full.astype(F32),
        gate_full.astype(F32),
        up_full.astype(F32),
        down_full.astype(F32),
        gain_kept[0],
        gain_kept[1],
    )


def solution(mesh):
    n_ctx = mesh.shape["ctx"]

    def body(*args):
        return shards(n_ctx, mesh.shape["head"], *args)

    return jax.shard_map(
        body,
        mesh=mesh,
        in_specs=(
            P(("ctx", "fsdp"), None),
            P("fsdp", "head"),
            P("fsdp", "head"),
            P("fsdp", "head"),
            P("head", "fsdp"),
            P("fsdp", "head"),
            P("fsdp", "head"),
            P("head", "fsdp"),
            P("fsdp"),
            P("fsdp"),
            P(("ctx", "fsdp"), None),
        ),
        out_specs=(
            P(("ctx", "fsdp"), None),
            P(("ctx", "fsdp"), None),
            P("fsdp", "head"),
            P("fsdp", "head"),
            P("fsdp", "head"),
            P("head", "fsdp"),
            P("fsdp", "head"),
            P("fsdp", "head"),
            P("head", "fsdp"),
            P("fsdp"),
            P("fsdp"),
        ),
        check_vma=False,
    )
```

```python
import functools

import jax
import jax.numpy as jnp
from jax import lax
from jax.experimental import pallas as pl
from jax.experimental.pallas import tpu as pltpu
from jax.sharding import PartitionSpec as P


HEAD_DIM = 64
EPSILON = 1e-05
NEG = -1e30
BF = jnp.bfloat16
F32 = jnp.float32
MESH = pl.DeviceIdType.MESH
CHUNKS = 16
LAG = 3
GROUPS = 4
FFN_GROUPS = 2


def matmul(left, right):
    return jnp.dot(left, right, preferred_element_type=F32)


def mat_trans(left, right):
    return lax.dot_general(left, right, (((1,), (1,)), ((), ())), preferred_element_type=F32)


def trans_mat(left, right):
    return lax.dot_general(left, right, (((0,), (0,)), ((), ())), preferred_element_type=F32)


def exchange(src, dst, axis, bit, send, recv):
    return pltpu.make_async_remote_copy(
        src_ref=src,
        dst_ref=dst,
        send_sem=send,
        recv_sem=recv,
        device_id={axis: lax.axis_index(axis) ^ bit},
        device_id_type=MESH,
    )


def add_into(dst, left, right):
    size = 64

    def one(i, carry):
        cut = pl.ds(pl.multiple_of(i * size, size), size)
        dst[cut, :] = (left[cut, :].astype(F32) + right[cut, :].astype(F32)).astype(BF)
        return carry

    lax.fori_loop(0, dst.shape[0] // size, one, 0)


class Chain:
    def __init__(self, n_ctx, ref, land, send, recv):
        self.ref, self.land, self.send, self.recv = ref, land, send, recv
        self.bits = high_bits(n_ctx)[:-1]

    def _copy(self, j):
        return exchange(self.ref, self.land.at[j], "ctx", self.bits[j], self.send.at[j], self.recv.at[j])

    def start(self):
        self._copy(0).start()

    def finish(self):
        for j in range(len(self.bits)):
            if j > 0:
                self._copy(j).start()
            self._copy(j).wait()
            add_into(self.ref, self.ref, self.land.at[j])


def high_bits(size):
    bits = []
    bit = size // 2
    while bit >= 1:
        bits.append(bit)
        bit //= 2
    return bits


def lanes(shape):
    return lax.broadcasted_iota(jnp.int32, shape, 1)


def head_lanes(ref, h, upper):
    wide = ref[:, (h // 2) * 128 : (h // 2) * 128 + 128]
    if (h % 2 == 1) != upper:
        wide = pltpu.roll(wide.astype(F32), HEAD_DIM, 1).astype(BF)
    keep = (lanes(wide.shape) >= HEAD_DIM) if upper else (lanes(wide.shape) < HEAD_DIM)
    return jnp.where(keep, wide, jnp.zeros_like(wide))


class Relay:
    def __init__(self, n_ctx, src, dst, send, recv):
        piece = src.shape[0] // n_ctx
        ctx = lax.axis_index("ctx")
        bits = high_bits(n_ctx)

        def cut(which):
            return pl.ds(pl.multiple_of(which * piece, piece), piece)

        self.levels = [[exchange(src.at[cut(ctx)], dst.at[cut(ctx)], "fsdp", 1, send.at[0], recv.at[0])]]
        e = 1
        for j, bit in enumerate(bits):
            level = []
            for m in masks_of(bits[:j]):
                part = dst.at[cut(ctx ^ m)]
                level.append(exchange(part, part, "ctx", bit, send.at[e], recv.at[e]))
                e += 1
            self.levels.append(level)

    def start(self):
        self.levels[0][0].start()

    def hop(self, j, landed=True):
        if landed:
            for copy in self.levels[j]:
                copy.wait_recv()
        for copy in self.levels[j + 1]:
            copy.start()

    def landed(self, j=-1):
        for copy in self.levels[j]:
            copy.wait_recv()

    def drain(self, levels=slice(None)):
        for level in self.levels[levels]:
            for copy in level:
                copy.wait_send()


def forward_kernel(
    n_ctx,
    n_head,
    span,
    q_ref,
    p_ref,
    wl_ref,
    wr_ref,
    gate_ref,
    up_ref,
    down_ref,
    o_ref,
    lse_ref,
    sum_ref,
    gate_other,
    up_other,
    down_other,
    q_pad,
    ext,
    max_ref,
    acc_ref,
    relay_send,
    relay_recv,
    left,
    right,
    from_lo,
    from_hi,
    *sems,
):
    rows, width = q_ref.shape
    heads = width // HEAD_DIM
    block = lax.axis_index("ctx") * 2 + lax.axis_index("fsdp")
    barrier = line_greet(n_head)
    greet(n_ctx)
    ext[...] = jnp.where(lanes(p_ref.shape) < HEAD_DIM, jnp.ones_like(p_ref[...]), p_ref[...])
    pl.semaphore_wait(barrier, line_peers(n_head) + len(partners(n_ctx)))
    gate = Relay(n_ctx, gate_ref, gate_other, relay_send.at[0], relay_recv.at[0])
    up = Relay(n_ctx, up_ref, up_other, relay_send.at[1], relay_recv.at[1])
    down = Relay(n_ctx, down_ref, down_other, relay_send.at[2], relay_recv.at[2])
    gate.start()
    up.start()
    down.hop(0, landed=False)
    step, steps, drain = line_sum(n_head, left, right, left, right, sum_ref, from_lo, from_hi, sems)
    size = rows // GROUPS
    stack = heads * size
    sub = min(512, stack)
    per_group = CHUNKS // GROUPS

    def tile(start, first_row, masked):
        cut = pl.ds(start, span)
        for j in range(stack // sub):
            part = pl.ds(j * sub, sub)
            scores = mat_trans(q_pad[part, :], p_ref[cut, :])
            if masked:
                row = first_row + lax.rem(lax.broadcasted_iota(jnp.int32, (sub, span), 0), size)
                col = start + lax.broadcasted_iota(jnp.int32, (sub, span), 1)
                scores = jnp.where(col <= row, scores, NEG)
            old = max_ref[part, :]
            new = jnp.maximum(old, jnp.max(scores, axis=1, keepdims=True))
            weights = jnp.exp(scores - jnp.tile(new, (1, span // 128))).astype(BF)
            acc_ref[part, :] = acc_ref[part, :] * jnp.exp(old - new) + matmul(weights, ext[cut, :])
            max_ref[part, :] = new

    def run(s, carry):
        step(s)
        return carry

    def one_group(g, carry):
        @pl.when(g == GROUPS - 1)
        def _():
            gate.hop(0)
            down.hop(1)

        mine = pl.ds(pl.multiple_of(g * size, size), size)
        first_row = block * rows + g * size
        for h in range(heads):
            q_pad[h * size : (h + 1) * size, :] = head_lanes(q_ref.at[mine], h, False)
        max_ref[...] = jnp.full_like(max_ref, NEG)
        acc_ref[...] = jnp.zeros_like(acc_ref)

        tiles = (block + 1) * (rows // span)
        base = (g - 1) * per_group

        def sums(i):
            lax.fori_loop((i * per_group) // tiles, ((i + 1) * per_group) // tiles, lambda j, c: run(base + j, c), 0)

        def full(i, c):
            sums(i)
            tile(pl.multiple_of(i * span, span), first_row, False)
            return c

        lax.fori_loop(0, block * (rows // span), full, 0)
        for j in range(rows // span):
            sums(block * (rows // span) + j)
            tile(pl.multiple_of(block * rows + j * span, span), first_row, True)
        for h in range(heads):
            acc = acc_ref[h * size : (h + 1) * size, :]
            total = acc[:, :HEAD_DIM]
            o_ref[mine, h * HEAD_DIM : (h + 1) * HEAD_DIM] = (acc[:, HEAD_DIM:] / total).astype(BF)
            lse = max_ref[h * size : (h + 1) * size, :] + jnp.log(jnp.concatenate([total, total], axis=1))
            lse_ref[h, :, mine] = lse.T[0:1, :]
        att = o_ref[mine, :]
        left[mine, :] = matmul(att, wl_ref[...]).astype(BF)
        right[mine, :] = matmul(att, wr_ref[...]).astype(BF)
        return carry

    lax.fori_loop(0, GROUPS, one_group, 0)
    hops = len(high_bits(n_ctx))
    later = [(down, j) for j in range(2, hops)] + [(gate, 1), (up, 0)]
    for j in range(1, hops):
        later += [(up, j)] + ([(gate, j + 1)] if j + 1 < hops else [])
    at = CHUNKS - per_group
    rest = steps - at
    for i, (relay, j) in enumerate(later):
        to = CHUNKS - per_group + (rest * (2 * i + 1)) // (2 * len(later))
        lax.fori_loop(at, to, run, 0)
        at = to
        relay.hop(j)
    lax.fori_loop(at, steps, run, 0)
    for relay in (gate, up, down):
        relay.landed()
    gate.drain()
    up.drain()
    down.drain(slice(1, None))
    drain()


def attend_sum(queries, pair, out_left, out_right, gate, up, down, n_ctx, n_head, collective_id):
    rows, width = queries.shape
    heads = width // HEAD_DIM
    seq = pair.shape[0]
    span = min(512, rows)
    wide = 2 * out_left.shape[1]
    vmem = pl.BlockSpec(memory_space=pltpu.VMEM)
    anywhere = pl.BlockSpec(memory_space=pl.ANY)
    stack = heads * rows // GROUPS
    cost = pl.CostEstimate(flops=50_000_000_000, bytes_accessed=8 * rows * wide, transcendentals=0)
    return pl.pallas_call(
        functools.partial(forward_kernel, n_ctx, n_head, span),
        out_shape=(
            jax.ShapeDtypeStruct((rows, width), BF),
            jax.ShapeDtypeStruct((heads, 1, rows), F32),
            jax.ShapeDtypeStruct((rows, wide), BF),
            jax.ShapeDtypeStruct(gate.shape, BF),
            jax.ShapeDtypeStruct(up.shape, BF),
            jax.ShapeDtypeStruct(down.shape, BF),
        ),
        input_output_aliases={6: 5},
        in_specs=[vmem] * 4 + [anywhere] * 3,
        out_specs=(vmem, vmem, vmem, anywhere, anywhere, anywhere),
        scratch_shapes=[
            pltpu.VMEM((stack, 128), BF),
            pltpu.VMEM((seq, 128), BF),
            pltpu.VMEM((stack, 128), F32),
            pltpu.VMEM((stack, 128), F32),
            pltpu.SemaphoreType.DMA((3, n_ctx)),
            pltpu.SemaphoreType.DMA((3, n_ctx)),
        ]
        + line_scratch(rows, wide),
        compiler_params=pltpu.CompilerParams(collective_id=collective_id, has_side_effects=True),
        cost_estimate=cost,
        name="attend_sum",
    )(queries, pair, out_left, out_right, gate, up, down)


def backward_kernel(
    n_ctx,
    n_head,
    group,
    span,
    q_ref,
    g_ref,
    o_ref,
    lse_ref,
    p_ref,
    left_ref,
    right_ref,
    gate_both,
    up_both,
    dq_ref,
    dp_ref,
    sum_ref,
    gate_out,
    up_out,
    q_pad,
    g_pad,
    acc_ref,
    dl_ref,
    gate_land,
    up_land,
    far_land,
    cross_send,
    cross_recv,
    far_send,
    far_recv,
    work_l,
    work_r,
    from_lo,
    from_hi,
    *sems,
):
    rows, width = q_ref.shape
    heads = width // HEAD_DIM
    tiles = rows // span
    block = lax.axis_index("ctx") * 2 + lax.axis_index("fsdp")
    barrier = line_greet(n_head)
    greet(n_ctx)
    dp_ref[...] = jnp.zeros_like(dp_ref)
    acc_ref[...] = jnp.zeros_like(acc_ref)
    for h in range(heads):
        cut = slice(h * HEAD_DIM, (h + 1) * HEAD_DIM)
        q_pad[h] = head_lanes(q_ref, h, False)
        g_pad[h] = head_lanes(g_ref, h, True)
        product = g_ref[:, cut].astype(F32) * o_ref[:, cut].astype(F32)
        dl_ref[h] = jnp.sum(product.T, axis=0, keepdims=True)
    pl.semaphore_wait(barrier, line_peers(n_head) + len(partners(n_ctx)))
    crosses = [
        exchange(sent, land, "fsdp", 1, cross_send.at[i], cross_recv.at[i])
        for i, (sent, land) in enumerate(((gate_both.at[1], gate_land), (up_both.at[1], up_land)))
    ]
    for cross in crosses:
        cross.start()
    far = Chain(n_ctx, gate_out, far_land, far_send, far_recv)
    hop_at = CHUNKS + 2
    step, steps, drain = line_sum(
        n_head, left_ref, right_ref, work_l, work_r, sum_ref, from_lo, from_hi, sems
    )

    def hop():
        crosses[0].wait_recv()
        add_into(gate_out, gate_both.at[0], gate_land)
        far.start()

    def head_tile(h, pairs, start, masked):
        probs = jnp.exp(mat_trans(pairs, q_pad[h]) - lse_ref[h])
        if masked:
            row = block * rows + lax.broadcasted_iota(jnp.int32, (span, rows), 1)
            col = start + lax.broadcasted_iota(jnp.int32, (span, rows), 0)
            probs = jnp.where(col <= row, probs, 0.0)
        grads = (probs * (mat_trans(pairs, g_pad[h]) - dl_ref[h])).astype(BF)
        acc_ref[h] += trans_mat(grads, pairs)
        return matmul(probs.astype(BF), g_pad[h]) + matmul(grads, q_pad[h])

    groups = heads // group

    def two_steps(t):
        for j in range(2):

            @pl.when(2 * t + j < steps)
            def _():
                step(2 * t + j)

        @pl.when(2 * t == hop_at)
        def _():
            hop()

    def full(t, carry):
        two_steps(t)
        first = lax.rem(t, groups) * group
        start = pl.multiple_of((t // groups) * span, span)
        cut = pl.ds(start, span)
        total = head_tile(first, p_ref[cut, :], start, False)
        for h in range(1, group):
            total = total + head_tile(first + h, p_ref[cut, :], start, False)
        dp_ref[cut, :] += total
        return carry

    count = block * tiles * groups
    lax.fori_loop(0, count, full, 0)

    def last(t, carry):
        h = lax.rem(t, heads)

        @pl.when(lax.rem(t, group) == 0)
        def _():
            two_steps(count + t // group)

        start = pl.multiple_of(block * rows + (t // heads) * span, span)
        cut = pl.ds(start, span)
        dp_ref[cut, :] += head_tile(h, p_ref[cut, :], start, True)
        return carry

    lax.fori_loop(0, heads * tiles, last, 0)
    for h in range(heads):
        dq_ref[:, h * HEAD_DIM : (h + 1) * HEAD_DIM] = acc_ref[h][:, :HEAD_DIM]

    begun = 2 * (count + groups * tiles)

    def rest(s, carry):
        step(s)

        @pl.when(s == hop_at)
        def _():
            hop()

        return carry

    lax.fori_loop(jnp.minimum(begun, steps), steps, rest, 0)
    drain()
    crosses[1].wait_recv()
    add_into(up_out, up_both.at[0], up_land)
    for cross in crosses:
        cross.wait_send()
    far.finish()


def attend_back(queries, grads, attended, lse, pair, left, right, parts, n_ctx, n_head, collective_id):
    rows, width = queries.shape
    heads = width // HEAD_DIM
    seq = pair.shape[0]
    group = 4 if heads % 4 == 0 else 2
    span = min(512, rows)
    vmem = pl.BlockSpec(memory_space=pltpu.VMEM)
    flat = jax.ShapeDtypeStruct(parts[0].shape[1:], BF)
    n_far = len(high_bits(n_ctx)) - 1
    cost = pl.CostEstimate(
        flops=32 * rows * seq * width, bytes_accessed=8 * rows * width, transcendentals=0
    )
    return pl.pallas_call(
        functools.partial(backward_kernel, n_ctx, n_head, group, span),
        out_shape=(
            jax.ShapeDtypeStruct((rows, width), F32),
            jax.ShapeDtypeStruct((seq, 2 * HEAD_DIM), F32),
            jax.ShapeDtypeStruct((rows, 2 * left.shape[1]), BF),
            flat,
            flat,
        ),
        in_specs=[vmem] * 9,
        out_specs=(vmem,) * 5,
        scratch_shapes=[
            pltpu.VMEM((heads, rows, 128), BF),
            pltpu.VMEM((heads, rows, 128), BF),
            pltpu.VMEM((heads, rows, 128), F32),
            pltpu.VMEM((heads, 1, rows), F32),
            pltpu.VMEM(flat.shape, BF),
            pltpu.VMEM(flat.shape, BF),
            pltpu.VMEM((n_far,) + flat.shape, BF),
            pltpu.SemaphoreType.DMA((2,)),
            pltpu.SemaphoreType.DMA((2,)),
            pltpu.SemaphoreType.DMA((n_far,)),
            pltpu.SemaphoreType.DMA((n_far,)),
        ]
        + line_scratch(rows, 2 * left.shape[1]),
        compiler_params=pltpu.CompilerParams(collective_id=collective_id, has_side_effects=True),
        cost_estimate=cost,
        name="attend_backward",
    )(queries, grads, attended, lse, pair, left, right, *parts)


def partners(n_ctx):
    return [("fsdp", 1)] + [("ctx", bit) for bit in high_bits(n_ctx)]


def greet(n_ctx):
    barrier = pltpu.get_barrier_semaphore()
    for axis, bit in partners(n_ctx):
        pl.semaphore_signal(
            barrier, inc=1, device_id={axis: lax.axis_index(axis) ^ bit}, device_id_type=MESH
        )
    return barrier


def masks_of(bits):
    masks = [0]
    for bit in bits:
        masks = masks + [m | bit for m in masks]
    return masks


def gather_pairs(n_ctx, rows, all_ref, send, recv):
    x = lax.axis_index("fsdp")
    ctx = lax.axis_index("ctx")
    copies = []

    def part(start, size, axis, bit):
        e = len(copies)
        cut = all_ref.at[pl.ds(pl.multiple_of(start, rows), size)]
        copy = pltpu.make_async_remote_copy(
            src_ref=cut,
            dst_ref=cut,
            send_sem=send.at[e],
            recv_sem=recv.at[e],
            device_id={axis: lax.axis_index(axis) ^ bit},
            device_id_type=MESH,
        )
        copy.start()
        copies.append(copy)
        return copy

    opening = part((ctx * 2 + x) * rows, rows, "fsdp", 1)

    def finish():
        opening.wait_recv()
        done = []
        for bit in high_bits(n_ctx):
            now = [part((ctx ^ m) * 2 * rows, 2 * rows, "ctx", bit) for m in masks_of(done)]
            for copy in now:
                copy.wait_recv()
            done.append(bit)
        for copy in copies:
            copy.wait_send()

    return finish


def project_kernel(
    n_ctx,
    x_ref,
    w_ref,
    gain_ref,
    cos_ref,
    sin_ref,
    wo_ref,
    down_ref,
    q_ref,
    p_ref,
    n_ref,
    w_other,
    gain_other,
    wo_other,
    down_other,
    acc_ref,
    send,
    recv,
    relay_send,
    relay_recv,
    gain_send,
    gain_recv,
):
    rows, width = x_ref.shape
    half = width // 2
    q_width = q_ref.shape[1]
    x_at = lax.axis_index("fsdp")
    block = lax.axis_index("ctx") * 2 + x_at
    barrier = greet(n_ctx)
    pl.semaphore_wait(barrier, len(partners(n_ctx)))
    gains = pltpu.make_async_remote_copy(
        src_ref=gain_ref,
        dst_ref=gain_other,
        send_sem=gain_send,
        recv_sem=gain_recv,
        device_id={"fsdp": 1 - x_at},
        device_id_type=MESH,
    )
    gains.start()
    part = half // 2
    first = [
        Relay(
            n_ctx,
            w_ref.at[pl.ds(i * part, part)],
            w_other.at[pl.ds(i * part, part)],
            relay_send.at[i],
            relay_recv.at[i],
        )
        for i in range(2)
    ]
    second = Relay(n_ctx, wo_ref, wo_other, relay_send.at[2], relay_recv.at[2])
    third = Relay(n_ctx, down_ref, down_other, relay_send.at[3], relay_recv.at[3])
    for relay in first:
        relay.start()
    second.start()
    gains.wait_recv()
    parts = 8
    size = rows // parts
    own = pl.ds(pl.multiple_of(x_at * half, half), half)
    other = pl.ds(pl.multiple_of((1 - x_at) * half, half), half)

    def cut_of(i):
        return pl.ds(pl.multiple_of(i * size, size), size)

    def norm(i, carry):
        cut = cut_of(i)
        left = x_ref[cut, own].astype(F32)
        right = x_ref[cut, other].astype(F32)
        total = jnp.sum(left * left, axis=1, keepdims=True) + jnp.sum(right * right, axis=1, keepdims=True)
        scale = lax.rsqrt(total / width + EPSILON)
        n_ref[cut, :half] = (left * scale * gain_ref[0:1, :]).astype(BF)
        n_ref[cut, half:] = (right * scale * gain_other[0:1, :]).astype(BF)
        return carry

    lax.fori_loop(0, parts, norm, 0)
    for relay in first:
        relay.hop(0)
    third.start()
    second.hop(0)

    def local(i, carry):
        cut = cut_of(i)
        acc_ref[cut, :] = matmul(n_ref[cut, :half], w_ref[...])
        return carry

    lax.fori_loop(0, parts, local, 0)
    for j in range(1, len(high_bits(n_ctx))):
        for relay in first:
            relay.hop(j)
    for relay in first:
        relay.landed()

    def rotated(wide, cut):
        low = lax.rem(lanes(wide.shape), HEAD_DIM) < HEAD_DIM // 2
        turned = jnp.where(low, pltpu.roll(wide, 128 - HEAD_DIM // 2, 1), pltpu.roll(wide, HEAD_DIM // 2, 1))
        return wide * cos_ref[cut, :] + turned * sin_ref[cut, :]

    def pairs(i, carry):
        cut = cut_of(i)
        both = acc_ref[cut, q_width:] + matmul(n_ref[cut, half:], w_other[:, q_width:])
        pair = jnp.where(lanes(both.shape) < HEAD_DIM, rotated(both, cut), both)
        p_ref[pl.ds(pl.multiple_of(block * rows + i * size, size), size), :] = pair.astype(BF)
        return carry

    def queries(i, carry):
        cut = cut_of(i)
        whole = acc_ref[cut, :q_width] + matmul(n_ref[cut, half:], w_other[:, :q_width])
        for j in range(q_width // 128):
            sl = slice(j * 128, (j + 1) * 128)
            q_ref[cut, sl] = (rotated(whole[:, sl], cut) * 0.125).astype(BF)
        return carry

    lax.fori_loop(0, parts, pairs, 0)
    finish = gather_pairs(n_ctx, rows, p_ref, send, recv)
    lax.fori_loop(0, parts, queries, 0)
    finish()
    for j in range(1, len(high_bits(n_ctx))):
        second.hop(j)
    second.landed()
    third.landed(0)
    for relay in first + [second]:
        relay.drain()
    third.drain(slice(0, 1))
    gains.wait_send()


def project(inputs, w_local, gains, cosine, sine, w_out, w_down, q_width, n_ctx, collective_id):
    rows, width = inputs.shape
    vmem = pl.BlockSpec(memory_space=pltpu.VMEM)
    anywhere = pl.BlockSpec(memory_space=pl.ANY)
    return pl.pallas_call(
        functools.partial(project_kernel, n_ctx),
        out_shape=(
            jax.ShapeDtypeStruct((rows, q_width), BF),
            jax.ShapeDtypeStruct((rows * 2 * n_ctx, 2 * HEAD_DIM), BF),
            jax.ShapeDtypeStruct((rows, width), BF),
            jax.ShapeDtypeStruct(w_local.shape, BF),
            jax.ShapeDtypeStruct(gains.shape, F32),
            jax.ShapeDtypeStruct(w_out.shape, BF),
            jax.ShapeDtypeStruct(w_down.shape, BF),
        ),
        in_specs=[vmem] * 5 + [anywhere] * 2,
        out_specs=(vmem,) * 5 + (anywhere,) * 2,
        scratch_shapes=[
            pltpu.VMEM((rows, w_local.shape[1]), F32),
            pltpu.SemaphoreType.DMA((n_ctx,)),
            pltpu.SemaphoreType.DMA((n_ctx,)),
            pltpu.SemaphoreType.DMA((4, n_ctx)),
            pltpu.SemaphoreType.DMA((4, n_ctx)),
            pltpu.SemaphoreType.DMA,
            pltpu.SemaphoreType.DMA,
        ],
        compiler_params=pltpu.CompilerParams(collective_id=collective_id, has_side_effects=True),
        name="project",
    )(inputs, w_local, gains, cosine, sine, w_out, w_down)


def line_sum(n, left, right, work_l, work_r, o_ref, from_lo, from_hi, sems):
    s_up, r_up, s_dn, r_dn, s_a, r_a, s_b, r_b = sems
    me = lax.axis_index("head")
    rows, cols = left.shape
    size = rows // CHUNKS
    has_lo = me > 0
    has_hi = me < n - 1
    middle = jnp.logical_and(has_lo, has_hi)

    def at(k):
        return pl.ds(pl.multiple_of(k * size, size), size)

    def remote(src, dst, send, recv, target):
        return pltpu.make_async_remote_copy(
            src_ref=src,
            dst_ref=dst,
            send_sem=send,
            recv_sem=recv,
            device_id={"head": target},
            device_id_type=MESH,
        )

    def up(k, src):
        return remote(src.at[at(k)], from_lo.at[at(k)], s_up.at[k], r_up.at[k], me + 1)

    def down(k, src):
        return remote(src.at[at(k)], from_hi.at[at(k)], s_dn.at[k], r_dn.at[k], me - 1)

    def spread_a(k):
        part = o_ref.at[at(k), pl.ds(0, cols)]
        return remote(part, part, s_a.at[k], r_a.at[k], me + 1)

    def spread_b(k):
        part = o_ref.at[at(k), pl.ds(cols, cols)]
        return remote(part, part, s_b.at[k], r_b.at[k], me - 1)

    def valid(k):
        return jnp.logical_and(k >= 0, k < CHUNKS)

    def added(mine, there, k):
        return (mine[at(k), :].astype(F32) + there[at(k), :].astype(F32)).astype(BF)

    def step(s):
        k1 = s - LAG * me
        k2 = s - LAG * (n - 1 - me)
        k3 = s - LAG * (n - 1 + me)
        k4 = s - LAG * (2 * (n - 1) - me)

        @pl.when(jnp.logical_and(valid(k1), me == 0))
        def _():
            up(k1, right).start()

        @pl.when(jnp.logical_and(valid(k2), me == n - 1))
        def _():
            down(k2, left).start()

        @pl.when(jnp.logical_and(valid(k1), middle))
        def _():
            up(k1, right).wait_recv()
            work_r[at(k1), :] = added(right, from_lo, k1)
            up(k1, work_r).start()

        @pl.when(jnp.logical_and(valid(k1), me == n - 1))
        def _():
            up(k1, right).wait_recv()
            o_ref[at(k1), cols:] = added(right, from_lo, k1)
            spread_b(k1).start()

        @pl.when(jnp.logical_and(valid(k2), middle))
        def _():
            down(k2, left).wait_recv()
            work_l[at(k2), :] = added(left, from_hi, k2)
            down(k2, work_l).start()

        @pl.when(jnp.logical_and(valid(k2), me == 0))
        def _():
            down(k2, left).wait_recv()
            o_ref[at(k2), :cols] = added(left, from_hi, k2)
            spread_a(k2).start()

        @pl.when(jnp.logical_and(valid(k3), has_lo))
        def _():
            spread_a(k3).wait_recv()

            @pl.when(has_hi)
            def _():
                spread_a(k3).start()

        @pl.when(jnp.logical_and(valid(k4), has_hi))
        def _():
            spread_b(k4).wait_recv()

            @pl.when(has_lo)
            def _():
                spread_b(k4).start()

    def drain():
        def one(k, carry):
            @pl.when(has_hi)
            def _():
                up(k, right).wait_send()
                spread_a(k).wait_send()

            @pl.when(has_lo)
            def _():
                down(k, left).wait_send()
                spread_b(k).wait_send()

            return carry

        lax.fori_loop(0, CHUNKS, one, 0)

    return step, CHUNKS + 2 * LAG * (n - 1), drain


def line_greet(n):
    me = lax.axis_index("head")
    barrier = pltpu.get_barrier_semaphore()

    @pl.when(me > 0)
    def _():
        pl.semaphore_signal(barrier, inc=1, device_id={"head": me - 1}, device_id_type=MESH)

    @pl.when(me < n - 1)
    def _():
        pl.semaphore_signal(barrier, inc=1, device_id={"head": me + 1}, device_id_type=MESH)

    return barrier


def line_peers(n):
    me = lax.axis_index("head")
    return jnp.where(me > 0, 1, 0) + jnp.where(me < n - 1, 1, 0)


def line_scratch(rows, width):
    return [pltpu.VMEM((rows, width // 2), BF)] * 4 + [pltpu.SemaphoreType.DMA((CHUNKS,))] * 8


def last_kernel(
    n_ctx,
    n_head,
    dq_ref,
    part_ref,
    cos_ref,
    sin_ref,
    w_l,
    w_r,
    n_ref,
    att_ref,
    low_ref,
    up_ref,
    gate_ref,
    down_ref,
    sum_ref,
    qkv_full,
    out_full,
    gate_full,
    up_full,
    down_full,
    work,
    land,
    raw,
    raw_land,
    n_land,
    low_land,
    att_land,
    up_sum,
    out_sent,
    out_kept,
    out_land,
    qkv_sent,
    qkv_kept,
    qkv_land,
    up_far,
    out_far,
    qkv_far,
    pair_send,
    pair_recv,
    trade_send,
    trade_recv,
    cross_send,
    cross_recv,
    far_send,
    far_recv,
    full_send,
    full_recv,
    full_local,
    left,
    right,
    from_lo,
    from_hi,
    *sems,
):
    rows, q_width = dq_ref.shape
    half = n_ref.shape[1] // 2
    quarter = half // 2
    x_at = lax.axis_index("fsdp")
    ctx = lax.axis_index("ctx")
    core = lax.rem(ctx, 2)
    barrier = line_greet(n_head)
    greet(n_ctx)
    work[...] = part_ref[...].astype(BF)
    up_sum[...] = up_ref[...]
    pl.semaphore_wait(barrier, line_peers(n_head) + len(partners(n_ctx)))

    def relative(side, c):
        return pl.ds(pl.multiple_of(side * half + c * quarter, quarter), quarter)

    def trade(src, dst, at):
        return exchange(src, dst, "ctx", 1, trade_send.at[at], trade_recv.at[at])

    pairs = []
    used = [0]

    def give(start, size, axis, bit):
        e = len(pairs)
        cut = pl.ds(pl.multiple_of(start, rows), size)
        copy = exchange(
            work.at[cut], land.at[pl.ds(used[0], size)], axis, bit, pair_send.at[e], pair_recv.at[e]
        )
        copy.start()
        pairs.append(copy)
        used[0] += size
        return copy, used[0] - size

    def take(start, size, at):
        cut = pl.ds(pl.multiple_of(start, rows), size)
        work[cut, :] = (work[cut, :].astype(F32) + land[at : at + size, :].astype(F32)).astype(BF)

    up_chain = Chain(n_ctx, up_sum, up_far, far_send.at[0], far_recv.at[0])
    out_chain = Chain(n_ctx, out_kept, out_far, far_send.at[1], far_recv.at[1])
    qkv_chain = Chain(n_ctx, qkv_kept, qkv_far, far_send.at[2], far_recv.at[2])

    def turned(wide, cut):
        low = lax.rem(lanes(wide.shape), HEAD_DIM) < HEAD_DIM // 2
        swapped = jnp.where(low, pltpu.roll(wide, 128 - HEAD_DIM // 2, 1), pltpu.roll(wide, HEAD_DIM // 2, 1))
        return wide * cos_ref[cut, :] - swapped * sin_ref[cut, :]

    def rotate_rows(i, carry):
        cut = pl.ds(pl.multiple_of(i * 128, 128), 128)
        for j in range(q_width // 128):
            sl = slice(j * 128, (j + 1) * 128)
            raw[cut, sl] = turned(dq_ref[cut, sl] * 0.125, cut).astype(BF)
        return carry

    bits = high_bits(n_ctx)
    trades = []
    for j in range(len(bits)):
        bit = bits[len(bits) - 1 - j]
        masks = masks_of(bits[: len(bits) - 1 - j])
        now = [give((ctx ^ bit ^ m) * 2 * rows, 2 * rows, "ctx", bit) for m in masks]
        if j == 0:
            lax.fori_loop(0, rows // 128, rotate_rows, 0)
        for (copy, at), m in zip(now, masks):
            copy.wait_recv()
            take((ctx ^ m) * 2 * rows, 2 * rows, at)
    copy, at = give((ctx * 2 + 1 - x_at) * rows, rows, "fsdp", 1)
    up_chain.start()
    trades = [trade(att_ref, att_land, 0)]
    for side in range(2):
        trades.append(trade(low_ref.at[:, relative(side, 1 - core)], low_land.at[:, pl.ds(side * quarter, quarter)], 1 + side))
        trades.append(trade(n_ref.at[:, relative(side, 1 - core)], n_land.at[:, pl.ds(side * quarter, quarter)], 3 + side))
    for t in trades:
        t.start()
    copy.wait_recv()
    base = pl.multiple_of((ctx * 2 + x_at) * rows, rows)

    def finish_pair(i, carry):
        cut = pl.ds(pl.multiple_of(i * 128, 128), 128)
        mine = work[pl.ds(base + i * 128, 128), :].astype(F32) + land[pl.ds(at + i * 128, 128), :].astype(F32)
        raw[cut, q_width:] = jnp.where(lanes(mine.shape) < HEAD_DIM, turned(mine, cut), mine).astype(BF)
        left[cut, :] = mat_trans(raw[cut, :], w_l[...]).astype(BF)
        right[cut, :] = mat_trans(raw[cut, :], w_r[...]).astype(BF)
        return carry

    lax.fori_loop(0, rows // 128, finish_pair, 0)
    raw_trade = trade(raw, raw_land, 5)
    raw_trade.start()
    trades.append(raw_trade)
    step, steps, drain = line_sum(n_head, left, right, left, right, sum_ref, from_lo, from_hi, sems)

    def run(s, carry):
        step(s)
        return carry

    def spread(src, whole, by_rows, e):
        size = src.shape[0 if by_rows else 1]
        cut = pl.ds(pl.multiple_of(core * size, size), size)
        dst = whole.at[cut] if by_rows else whole.at[:, cut]
        return (
            pltpu.make_async_copy(src, dst, full_local.at[e]),
            exchange(src, dst, "ctx", 1, full_send.at[e], full_recv.at[e]),
        )

    spreads = [spread(gate_ref, gate_full, True, 0), spread(down_ref, down_full, False, 1)]
    for pair in spreads:
        for copy in pair:
            copy.start()

    def out_tiles(dst, side):
        def one(t, carry):
            cut = pl.ds(pl.multiple_of(t * 128, 128), 128)
            dst[cut, :] = (
                trans_mat(att_ref[:, cut], low_ref[:, relative(side, core)])
                + trans_mat(att_land[:, cut], low_land[:, side * quarter : (side + 1) * quarter])
            ).astype(BF)
            step(steps_at + t)
            return carry

        lax.fori_loop(0, q_width // 128, one, 0)

    def qkv_tiles(dst, side):
        def one(t, carry):
            cut = pl.ds(pl.multiple_of(t * 128, 128), 128)
            there = pl.ds(pl.multiple_of(side * half + core * quarter + t * 128, 128), 128)
            landing = pl.ds(pl.multiple_of(side * quarter + t * 128, 128), 128)
            dst[cut, :] = (
                trans_mat(n_ref[:, there], raw[...]) + trans_mat(n_land[:, landing], raw_land[...])
            ).astype(BF)
            step(steps_at + t)
            return carry

        lax.fori_loop(0, quarter // 128, one, 0)

    lax.fori_loop(0, 2, run, 0)
    for t in trades:
        t.wait_recv()
    steps_at = 2
    out_tiles(out_sent, 1)
    out_cross = exchange(out_sent, out_land, "fsdp", 1, cross_send.at[0], cross_recv.at[0])
    out_cross.start()
    steps_at += q_width // 128
    qkv_tiles(qkv_sent, 1)
    qkv_cross = exchange(qkv_sent, qkv_land, "fsdp", 1, cross_send.at[1], cross_recv.at[1])
    qkv_cross.start()
    steps_at += quarter // 128
    out_tiles(out_kept, 0)
    steps_at += q_width // 128
    qkv_tiles(qkv_kept, 0)
    steps_at += quarter // 128
    out_cross.wait_recv()
    add_into(out_kept, out_kept, out_land)
    out_chain.start()
    rest = steps - steps_at
    lax.fori_loop(steps_at, steps_at + rest // 4, run, 0)
    qkv_cross.wait_recv()
    add_into(qkv_kept, qkv_kept, qkv_land)
    qkv_chain.start()
    lax.fori_loop(steps_at + rest // 4, steps_at + rest // 2, run, 0)
    up_chain.finish()
    spreads.append(spread(up_sum, up_full, True, 2))
    for copy in spreads[-1]:
        copy.start()
    lax.fori_loop(steps_at + rest // 2, steps, run, 0)
    out_chain.finish()
    spreads.append(spread(out_kept, out_full, False, 3))
    for copy in spreads[-1]:
        copy.start()
    qkv_chain.finish()
    spreads.append(spread(qkv_kept, qkv_full, True, 4))
    for copy in spreads[-1]:
        copy.start()
    drain()
    for t in pairs + trades + [out_cross, qkv_cross]:
        t.wait_send()
    for local, remote in spreads:
        local.wait()
        remote.wait()


def last_sum(
    dq, part, cosine, sine, w_left, w_right, normed, attended, low, up, gate, down, n_ctx, n_head, collective_id
):
    rows, q_width = dq.shape
    width = normed.shape[1]
    half = width // 2
    quarter = half // 2
    narrow = w_left.shape[1]
    units = gate.shape[1]
    n_far = len(high_bits(n_ctx)) - 1
    vmem = pl.BlockSpec(memory_space=pltpu.VMEM)
    anywhere = pl.BlockSpec(memory_space=pl.ANY)
    dma = pltpu.SemaphoreType.DMA
    return pl.pallas_call(
        functools.partial(last_kernel, n_ctx, n_head),
        out_shape=(
            jax.ShapeDtypeStruct((rows, width), BF),
            jax.ShapeDtypeStruct((half, narrow), BF),
            jax.ShapeDtypeStruct((q_width, half), BF),
            jax.ShapeDtypeStruct((half, units), BF),
            jax.ShapeDtypeStruct((half, units), BF),
            jax.ShapeDtypeStruct((units, half), BF),
        ),
        in_specs=[vmem] * 12,
        out_specs=(vmem,) + (anywhere,) * 5,
        scratch_shapes=[
            pltpu.VMEM(part.shape, BF),
            pltpu.VMEM(part.shape, BF),
            pltpu.VMEM((rows, narrow), BF),
            pltpu.VMEM((rows, narrow), BF),
            pltpu.VMEM((rows, half), BF),
            pltpu.VMEM((rows, half), BF),
            pltpu.VMEM((rows, q_width), BF),
            pltpu.VMEM(up.shape, BF),
            pltpu.VMEM((q_width, quarter), BF),
            pltpu.VMEM((q_width, quarter), BF),
            pltpu.VMEM((q_width, quarter), BF),
            pltpu.VMEM((quarter, narrow), BF),
            pltpu.VMEM((quarter, narrow), BF),
            pltpu.VMEM((quarter, narrow), BF),
            pltpu.VMEM((n_far,) + up.shape, BF),
            pltpu.VMEM((n_far, q_width, quarter), BF),
            pltpu.VMEM((n_far, quarter, narrow), BF),
            dma((n_ctx,)),
            dma((n_ctx,)),
            dma((6,)),
            dma((6,)),
            dma((2,)),
            dma((2,)),
            dma((3, n_far)),
            dma((3, n_far)),
            dma((5,)),
            dma((5,)),
            dma((5,)),
        ]
        + line_scratch(rows, width),
        compiler_params=pltpu.CompilerParams(
            collective_id=collective_id, has_side_effects=True, vmem_limit_bytes=66_000_000
        ),
        cost_estimate=pl.CostEstimate(
            flops=50_000_000_000, bytes_accessed=8 * rows * width, transcendentals=0
        ),
        name="last_sum",
    )(dq, part, cosine, sine, w_left, w_right, normed, attended, low, up, gate, down)


def ffn_kernel(
    n_head,
    x_ref,
    mix_ref,
    cot_ref,
    gain_ref,
    gain_other,
    gate_l_hbm,
    gate_r_hbm,
    up_l_hbm,
    up_r_hbm,
    down_l_hbm,
    down_r_hbm,
    sum_ref,
    ffn_left,
    ffn_right,
    down_kept,
    gate_both,
    up_both,
    gate_l,
    gate_r,
    up_l,
    up_r,
    down_l,
    down_r,
    load_sem,
    n_ref,
    act_ref,
    gig_ref,
    uig_ref,
    cot_land,
    n_land,
    act_land,
    gig_land,
    uig_land,
    down_sent,
    down_land,
    out_tile,
    out_sem,
    trade_send,
    trade_recv,
    cross_send,
    cross_recv,
    left,
    right,
    from_lo,
    from_hi,
    *sems,
):
    rows, width = x_ref.shape
    half = width // 2
    quarter = half // 2
    units = act_ref.shape[1]
    x_at = lax.axis_index("fsdp")
    ctx_at = lax.axis_index("ctx")
    core = lax.rem(ctx_at, 2)
    own = pl.ds(pl.multiple_of(x_at * half, half), half)
    other = pl.ds(pl.multiple_of((1 - x_at) * half, half), half)
    barrier = line_greet(n_head)
    pl.semaphore_signal(barrier, inc=1, device_id={"fsdp": 1 - x_at}, device_id_type=MESH)
    pl.semaphore_signal(barrier, inc=1, device_id={"ctx": ctx_at ^ 1}, device_id_type=MESH)
    loads = [
        pltpu.make_async_copy(src, dst, load_sem.at[i])
        for i, (src, dst) in enumerate(
            (
                (gate_l_hbm, gate_l),
                (gate_r_hbm, gate_r),
                (up_l_hbm, up_l),
                (up_r_hbm, up_r),
                (down_l_hbm, down_l),
                (down_r_hbm, down_r),
            )
        )
    ]
    for load in loads:
        load.start()
    pl.semaphore_wait(barrier, line_peers(n_head) + 2)

    def trade(src, dst, at):
        return pltpu.make_async_remote_copy(
            src_ref=src,
            dst_ref=dst,
            send_sem=trade_send.at[at],
            recv_sem=trade_recv.at[at],
            device_id={"ctx": ctx_at ^ 1},
            device_id_type=MESH,
        )

    def absolute(side, c):
        start = (x_at if side == 0 else 1 - x_at) * half + c * quarter
        return pl.ds(pl.multiple_of(start, quarter), quarter)

    def relative(side, c):
        return pl.ds(pl.multiple_of(side * half + c * quarter, quarter), quarter)

    cot_trades = [
        trade(cot_ref.at[:, absolute(j, 1 - core)], cot_land.at[:, pl.ds(j * quarter, quarter)], j)
        for j in range(2)
    ]
    for copy in cot_trades:
        copy.start()

    def row_trades(g):
        mine = pl.ds(pl.multiple_of(g * (rows // FFN_GROUPS), rows // FFN_GROUPS), rows // FFN_GROUPS)
        at = 2 + g * 5
        return [
            trade(act_ref.at[mine], act_land.at[mine], at),
            trade(gig_ref.at[mine], gig_land.at[mine], at + 1),
            trade(uig_ref.at[mine], uig_land.at[mine], at + 2),
            trade(n_ref.at[mine, relative(0, 1 - core)], n_land.at[mine, pl.ds(0, quarter)], at + 3),
            trade(n_ref.at[mine, relative(1, 1 - core)], n_land.at[mine, pl.ds(quarter, quarter)], at + 4),
        ]

    step, steps, drain = line_sum(n_head, left, right, left, right, sum_ref, from_lo, from_hi, sems)

    def run(s, carry):
        step(s)
        return carry

    size = rows // FFN_GROUPS
    per_group = CHUNKS // FFN_GROUPS

    def one_group(g, carry):
        mine = pl.ds(pl.multiple_of(g * size, size), size)
        base = (g - 1) * per_group
        stops = [base + (per_group * i) // 4 for i in range(5)]
        hid_l = x_ref[mine, own].astype(F32) + mix_ref[mine, :half].astype(F32)
        hid_r = x_ref[mine, other].astype(F32) + mix_ref[mine, half:].astype(F32)
        total = jnp.sum(hid_l * hid_l, axis=1, keepdims=True) + jnp.sum(hid_r * hid_r, axis=1, keepdims=True)
        scale = lax.rsqrt(total / width + EPSILON)
        n_ref[mine, :half] = (hid_l * scale * gain_ref[1:2, :]).astype(BF)
        n_ref[mine, half:] = (hid_r * scale * gain_other[1:2, :]).astype(BF)
        lax.fori_loop(stops[0], stops[1], run, 0)

        @pl.when(g == 0)
        def _():
            for load in loads[:4]:
                load.wait()

        gate = matmul(n_ref[mine, :half], gate_l[...]) + matmul(n_ref[mine, half:], gate_r[...])
        up = matmul(n_ref[mine, :half], up_l[...]) + matmul(n_ref[mine, half:], up_r[...])
        lax.fori_loop(stops[1], stops[2], run, 0)
        sigma = jax.nn.sigmoid(gate)
        silu = gate * sigma
        act_ref[mine, :] = (silu * up).astype(BF)

        @pl.when(g == 0)
        def _():
            for load in loads[4:]:
                load.wait()

        grad = mat_trans(cot_ref[mine, own], down_l[...]) + mat_trans(cot_ref[mine, other], down_r[...])
        gig_ref[mine, :] = (grad * up * sigma * (1.0 + gate * (1.0 - sigma))).astype(BF)
        uig_ref[mine, :] = (grad * silu).astype(BF)
        lax.fori_loop(stops[2], stops[3], run, 0)
        gig = gig_ref[mine, :]
        uig = uig_ref[mine, :]
        left[mine, :] = (mat_trans(gig, gate_l[...]) + mat_trans(uig, up_l[...])).astype(BF)
        lax.fori_loop(stops[3], stops[4], run, 0)
        right[mine, :] = (mat_trans(gig, gate_r[...]) + mat_trans(uig, up_r[...])).astype(BF)
        for copy in row_trades(g):
            copy.start()
        return carry

    lax.fori_loop(0, FFN_GROUPS, one_group, 0)
    first = CHUNKS - per_group
    rest = steps - first
    tile = 128
    down_tiles = units // tile
    row_tiles = quarter // tile
    total_work = down_tiles + 4 * row_tiles + 2 * FFN_GROUPS

    def sums(i, weight=1):
        lax.fori_loop(
            first + (rest * i) // total_work, first + (rest * (i + weight)) // total_work, run, 0
        )

    for copy in cot_trades:
        copy.wait_recv()

    def landed(g, carry):
        for copy in row_trades(g):
            copy.wait_recv()
        return carry

    lax.fori_loop(0, FFN_GROUPS, landed, 0)

    def down_tile(t, carry):
        sums(t)
        cut = pl.ds(pl.multiple_of(t * tile, tile), tile)
        mine = act_ref[:, cut]
        theirs = act_land[:, cut]
        for dst, side in ((down_sent, 1), (down_kept, 0)):
            dst[cut, :] = (
                trans_mat(mine, cot_ref[:, absolute(side, core)])
                + trans_mat(theirs, cot_land[:, side * quarter : (side + 1) * quarter])
            ).astype(BF)
        return carry

    lax.fori_loop(0, down_tiles, down_tile, 0)
    cross = pltpu.make_async_remote_copy(
        src_ref=down_sent,
        dst_ref=down_land,
        send_sem=cross_send,
        recv_sem=cross_recv,
        device_id={"fsdp": 1 - x_at},
        device_id_type=MESH,
    )
    cross.start()
    done = down_tiles

    def out_copy(dst, t, slot):
        cut = pl.ds(pl.multiple_of(lax.rem(t, row_tiles) * tile, tile), tile)
        return pltpu.make_async_copy(out_tile.at[slot], dst.at[1 - t // row_tiles, cut], out_sem.at[slot])

    for dst, own_grad, their_grad in ((gate_both, gig_ref, gig_land), (up_both, uig_ref, uig_land)):

        def row_tile(t, carry):
            sums(done + t)
            slot = lax.rem(t, 2)
            side = 1 - t // row_tiles
            row = lax.rem(t, row_tiles) * tile
            there = pl.ds(pl.multiple_of(side * half + core * quarter + row, tile), tile)
            landing = pl.ds(pl.multiple_of(side * quarter + row, tile), tile)
            value = (
                trans_mat(n_ref[:, there], own_grad[...]) + trans_mat(n_land[:, landing], their_grad[...])
            ).astype(BF)

            @pl.when(t >= 2)
            def _():
                out_copy(dst, t - 2, slot).wait()

            out_tile[slot] = value
            out_copy(dst, t, slot).start()
            return carry

        lax.fori_loop(0, 2 * row_tiles, row_tile, 0)
        for t in range(2 * row_tiles - 2, 2 * row_tiles):
            out_copy(dst, t, t % 2).wait()
        done += 2 * row_tiles

    def project_down(g, carry):
        mine = pl.ds(pl.multiple_of(g * size, size), size)
        sums(done + 2 * g, 2)
        ffn_left[mine, :] = matmul(act_ref[mine, :], down_l[...]).astype(BF)
        ffn_right[mine, :] = matmul(act_ref[mine, :], down_r[...]).astype(BF)
        return carry

    lax.fori_loop(0, FFN_GROUPS, project_down, 0)
    cross.wait_recv()

    def finish(t, carry):
        cut = pl.ds(pl.multiple_of(t * tile, tile), tile)
        down_kept[cut, :] = (down_kept[cut, :].astype(F32) + down_land[cut, :].astype(F32)).astype(BF)
        return carry

    lax.fori_loop(0, down_tiles, finish, 0)
    cross.wait_send()
    for copy in cot_trades:
        copy.wait_send()

    def sent(g, carry):
        for copy in row_trades(g):
            copy.wait_send()
        return carry

    lax.fori_loop(0, FFN_GROUPS, sent, 0)
    drain()


def ffn_sum(inputs, mixed, cot, gains, gains_other, gate, gate_o, up, up_o, down, down_o, n_head, collective_id):
    rows, width = inputs.shape
    units = gate.shape[1]
    vmem = pl.BlockSpec(memory_space=pltpu.VMEM)
    wide = jax.ShapeDtypeStruct((rows, width), BF)
    narrow = jax.ShapeDtypeStruct((rows, width // 2), BF)
    quarter = width // 4
    flat = jax.ShapeDtypeStruct((2, quarter, units), BF)
    anywhere = pl.BlockSpec(memory_space=pl.ANY)
    trades = 2 + 5 * FFN_GROUPS
    return pl.pallas_call(
        functools.partial(ffn_kernel, n_head),
        out_shape=(wide, narrow, narrow, jax.ShapeDtypeStruct((units, quarter), BF), flat, flat),
        in_specs=[vmem] * 5 + [anywhere] * 6,
        out_specs=(vmem,) * 4 + (anywhere,) * 2,
        scratch_shapes=[pltpu.VMEM(w.shape, BF) for w in (gate, gate, up, up, down, down)]
        + [pltpu.SemaphoreType.DMA((6,)), pltpu.VMEM((rows, width), BF)]
        + [pltpu.VMEM((rows, units), BF)] * 3
        + [pltpu.VMEM((rows, width // 2), BF)] * 2
        + [pltpu.VMEM((rows, units), BF)] * 3
        + [pltpu.VMEM((units, quarter), BF)] * 2
        + [
            pltpu.VMEM((2, 128, units), BF),
            pltpu.SemaphoreType.DMA((2,)),
            pltpu.SemaphoreType.DMA((trades,)),
            pltpu.SemaphoreType.DMA((trades,)),
            pltpu.SemaphoreType.DMA,
            pltpu.SemaphoreType.DMA,
        ]
        + line_scratch(rows, width),
        compiler_params=pltpu.CompilerParams(
            collective_id=collective_id, has_side_effects=True, vmem_limit_bytes=66_000_000
        ),
        cost_estimate=pl.CostEstimate(
            flops=50_000_000_000, bytes_accessed=8 * rows * width, transcendentals=0
        ),
        name="ffn_sum",
    )(inputs, mixed, cot, gains, gains_other, gate, gate_o, up, up_o, down, down_o)


def halves(ref, x_at):
    half = ref.shape[1] // 2
    own = pl.ds(pl.multiple_of(x_at * half, half), half)
    other = pl.ds(pl.multiple_of((1 - x_at) * half, half), half)
    return ref[:, own].astype(F32), ref[:, other].astype(F32)


def norm_back(values, grads, gains, width):
    scale = lax.rsqrt(sum(jnp.sum(v * v, axis=1, keepdims=True) for v in values) / width + EPSILON)
    units = [v * scale for v in values]
    scaled = [g * gain for g, gain in zip(grads, gains)]
    mean = sum(jnp.sum(s * u, axis=1, keepdims=True) for s, u in zip(scaled, units)) / width
    return [scale * (s - u * mean) for s, u in zip(scaled, units)], [g * u for g, u in zip(grads, units)]


def add_gain(gain_ref, products):
    @pl.when(pl.program_id(0) == 0)
    def _():
        gain_ref[...] = jnp.zeros_like(gain_ref)

    half = products[0].shape[1]
    gain_ref[0:1, :half] += jnp.sum(products[0], axis=0, keepdims=True)
    gain_ref[0:1, half:] += jnp.sum(products[1], axis=0, keepdims=True)


def middle_kernel(at_ref, x_ref, mix_ref, grad_ref, cot_ref, gain_ref, other_ref, wl_ref, wr_ref, hid_ref, low_ref, att_ref, part_ref):
    width = x_ref.shape[1]
    half = width // 2
    x_at = at_ref[0]
    x_l, x_r = halves(x_ref, x_at)
    cot_l, cot_r = halves(cot_ref, x_at)
    values = (x_l + mix_ref[:, :half].astype(F32), x_r + mix_ref[:, half:].astype(F32))
    grads = (grad_ref[:, :half].astype(F32), grad_ref[:, half:].astype(F32))
    (d_l, d_r), products = norm_back(values, grads, (gain_ref[1:2, :], other_ref[1:2, :]), width)
    add_gain(part_ref, products)
    hid_l = cot_l + d_l
    hid_r = cot_r + d_r
    hid_ref[:, :half] = hid_l
    hid_ref[:, half:] = hid_r
    low_l = hid_l.astype(BF)
    low_r = hid_r.astype(BF)
    low_ref[:, :half] = low_l
    low_ref[:, half:] = low_r
    att_ref[...] = (mat_trans(low_l, wl_ref[...]) + mat_trans(low_r, wr_ref[...])).astype(BF)


def end_kernel(at_ref, x_ref, mix_ref, ffn_ref, grad_ref, hid_ref, gain_ref, other_ref, out_ref, in_grad_ref, part_ref):
    width = x_ref.shape[1]
    half = width // 2
    x_at = at_ref[0]
    own = pl.ds(pl.multiple_of(x_at * half, half), half)
    other = pl.ds(pl.multiple_of((1 - x_at) * half, half), half)
    x_l, x_r = halves(x_ref, x_at)
    out_ref[:, own] = (x_l + mix_ref[:, :half].astype(F32) + ffn_ref[:, :half].astype(F32)).astype(BF)
    out_ref[:, other] = (x_r + mix_ref[:, half:].astype(F32) + ffn_ref[:, half:].astype(F32)).astype(BF)
    grads = (grad_ref[:, :half].astype(F32), grad_ref[:, half:].astype(F32))
    (d_l, d_r), products = norm_back((x_l, x_r), grads, (gain_ref[0:1, :], other_ref[0:1, :]), width)
    add_gain(part_ref, products)
    in_grad_ref[:, own] = hid_ref[:, :half] + d_l
    in_grad_ref[:, other] = hid_ref[:, half:] + d_r


def by_rows(kernel, x_at, arrays, whole, outs):
    rows, width = arrays[0].shape
    size = min(128, rows)

    def block(shape):
        return pl.BlockSpec((size, shape[1]), lambda i, *_: (i, 0))

    def all_of(shape):
        return pl.BlockSpec(shape, lambda i, *_: (0, 0))

    gain = jax.ShapeDtypeStruct((8, width), F32)
    return pl.pallas_call(
        kernel,
        out_shape=tuple(outs) + (gain,),
        grid_spec=pltpu.PrefetchScalarGridSpec(
            num_scalar_prefetch=1,
            grid=(rows // size,),
            in_specs=[block(a.shape) for a in arrays] + [all_of(a.shape) for a in whole],
            out_specs=[block(o.shape) for o in outs] + [all_of(gain.shape)],
        ),
        cost_estimate=pl.CostEstimate(flops=4_000_000_000, bytes_accessed=24 * rows * width, transcendentals=0),
    )(x_at, *arrays, *whole)


def flip(array, axis, bit, size):
    return lax.ppermute(array, axis, [(i, i ^ bit) for i in range(size)])


def shards(
    n_ctx,
    n_head,
    inputs,
    query_weight,
    key_weight,
    value_weight,
    output_weight,
    gate_weight,
    up_weight,
    down_weight,
    attn_gain,
    ffn_gain,
    cotangent,
):
    rows, width = inputs.shape
    half = width // 2
    x_at = lax.axis_index("fsdp")
    ctx_at = lax.axis_index("ctx")
    core = lax.rem(ctx_at, 2)
    block = ctx_at * 2 + x_at
    block_arr = jnp.reshape(block, (1,)).astype(jnp.int32)

    every = high_bits(n_ctx)

    q_width = query_weight.shape[1]
    half_dim = HEAD_DIM // 2
    positions = block * rows + jnp.arange(rows, dtype=jnp.int32)
    lane = lax.broadcasted_iota(jnp.int32, (rows, 2 * HEAD_DIM), 1)
    freqs = 10000.0 ** (-2.0 * (lane % half_dim).astype(F32) / HEAD_DIM)
    angles = positions.astype(F32)[:, None] * freqs
    cosine = jnp.cos(angles)
    sine = jnp.sin(angles)
    signed = jnp.where(lane % HEAD_DIM < half_dim, -sine, sine)
    qkv_local = jnp.concatenate([query_weight, key_weight, value_weight], axis=1)
    gains_local = jnp.concatenate([attn_gain[None], ffn_gain[None], jnp.zeros((6, half), BF)]).astype(F32)
    queries, pair, normed_one, qkv_other, gains_other, out_other, down_begun = project(
        inputs, qkv_local, gains_local, cosine, signed, output_weight, down_weight, q_width, n_ctx, 4
    )
    attended, lse, mixed, gate_other, up_other, down_other = attend_sum(
        queries, pair, output_weight, out_other, gate_weight, up_weight, down_begun, n_ctx, n_head, 1
    )
    low_sum, down_left, down_right, down_kept, gate_both, up_both = ffn_sum(
        inputs,
        mixed,
        cotangent,
        gains_local,
        gains_other,
        gate_weight,
        gate_other,
        up_weight,
        up_other,
        down_weight,
        down_other,
        n_head,
        2,
    )
    x_arr = jnp.reshape(x_at, (1,)).astype(jnp.int32)
    wide = jax.ShapeDtypeStruct((rows, width), F32)
    flat = jax.ShapeDtypeStruct((rows, width), BF)
    hidden_grad, hidden_low, attended_grad, gain_two_part = by_rows(
        middle_kernel,
        x_arr,
        (inputs, mixed, low_sum, cotangent),
        (gains_local, gains_other, output_weight, out_other),
        (wide, flat, jax.ShapeDtypeStruct(attended.shape, BF)),
    )
    down_far = down_kept
    for bit in every[:-1]:
        down_far = (down_far.astype(F32) + flip(down_far, "ctx", bit, n_ctx).astype(F32)).astype(BF)
    query_acc, pair_acc, ffn_out, gate_far, up_crossed = attend_back(
        queries,
        attended_grad,
        attended,
        lse,
        pair,
        down_left,
        down_right,
        (gate_both, up_both),
        n_ctx,
        n_head,
        6,
    )
    last, qkv_full, out_full, gate_full, up_full, down_full = last_sum(
        query_acc,
        pair_acc,
        cosine,
        signed,
        qkv_local,
        qkv_other,
        normed_one,
        attended,
        hidden_low,
        up_crossed,
        gate_far,
        down_far,
        n_ctx,
        n_head,
        3,
    )
    outputs, input_grad, gain_one_part = by_rows(
        end_kernel, x_arr, (inputs, mixed, ffn_out, last, hidden_grad), (gains_local, gains_other), (flat, wide)
    )
    query_grad = qkv_full[:, :q_width].astype(F32)
    key_grad = qkv_full[:, q_width : q_width + HEAD_DIM].astype(F32)
    value_grad = qkv_full[:, q_width + HEAD_DIM :].astype(F32)

    gain_parts = jnp.stack([gain_one_part[0], gain_two_part[0]])
    gain_kept = gain_parts[:, :half] + flip(gain_parts[:, half:], "fsdp", 1, 2)
    for bit in every:
        gain_kept = gain_kept + flip(gain_kept, "ctx", bit, n_ctx)

    return (
        outputs,
        input_grad,
        query_grad,
        key_grad,
        value_grad,
        out_full.astype(F32),
        gate_full.astype(F32),
        up_full.astype(F32),
        down_full.astype(F32),
        gain_kept[0],
        gain_kept[1],
    )


def solution(mesh):
    n_ctx = mesh.shape["ctx"]

    def body(*args):
        return shards(n_ctx, mesh.shape["head"], *args)

    return jax.shard_map(
        body,
        mesh=mesh,
        in_specs=(
            P(("ctx", "fsdp"), None),
            P("fsdp", "head"),
            P("fsdp", "head"),
            P("fsdp", "head"),
            P("head", "fsdp"),
            P("fsdp", "head"),
            P("fsdp", "head"),
            P("head", "fsdp"),
            P("fsdp"),
            P("fsdp"),
            P(("ctx", "fsdp"), None),
        ),
        out_specs=(
            P(("ctx", "fsdp"), None),
            P(("ctx", "fsdp"), None),
            P("fsdp", "head"),
            P("fsdp", "head"),
            P("fsdp", "head"),
            P("head", "fsdp"),
            P("fsdp", "head"),
            P("fsdp", "head"),
            P("head", "fsdp"),
            P("fsdp"),
            P("fsdp"),
        ),
        check_vma=False,
    )
```

```python
import functools

import jax
import jax.numpy as jnp
from jax import lax
from jax.experimental import pallas as pl
from jax.experimental.pallas import tpu as pltpu
from jax.sharding import PartitionSpec as P


HEAD_DIM = 64
EPSILON = 1e-05
NEG = -1e30
BF = jnp.bfloat16
F32 = jnp.float32
MESH = pl.DeviceIdType.MESH
CHUNKS = 16
LAG = 3
GROUPS = 4
FFN_GROUPS = 2


def matmul(left, right):
    return jnp.dot(left, right, preferred_element_type=F32)


def mat_trans(left, right):
    return lax.dot_general(left, right, (((1,), (1,)), ((), ())), preferred_element_type=F32)


def trans_mat(left, right):
    return lax.dot_general(left, right, (((0,), (0,)), ((), ())), preferred_element_type=F32)


def exchange(src, dst, axis, bit, send, recv):
    return pltpu.make_async_remote_copy(
        src_ref=src,
        dst_ref=dst,
        send_sem=send,
        recv_sem=recv,
        device_id={axis: lax.axis_index(axis) ^ bit},
        device_id_type=MESH,
    )


def add_into(dst, left, right):
    size = 64

    def one(i, carry):
        cut = pl.ds(pl.multiple_of(i * size, size), size)
        dst[cut, :] = (left[cut, :].astype(F32) + right[cut, :].astype(F32)).astype(BF)
        return carry

    lax.fori_loop(0, dst.shape[0] // size, one, 0)


class Chain:
    def __init__(self, n_ctx, ref, land, send, recv):
        self.ref, self.land, self.send, self.recv = ref, land, send, recv
        self.bits = high_bits(n_ctx)[:-1]

    def _copy(self, j):
        return exchange(self.ref, self.land.at[j], "ctx", self.bits[j], self.send.at[j], self.recv.at[j])

    def start(self):
        self._copy(0).start()

    def finish(self):
        for j in range(len(self.bits)):
            if j > 0:
                self._copy(j).start()
            self._copy(j).wait()
            add_into(self.ref, self.ref, self.land.at[j])


def high_bits(size):
    bits = []
    bit = size // 2
    while bit >= 1:
        bits.append(bit)
        bit //= 2
    return bits


def lanes(shape):
    return lax.broadcasted_iota(jnp.int32, shape, 1)


def head_lanes(ref, h, upper):
    wide = ref[:, (h // 2) * 128 : (h // 2) * 128 + 128]
    if (h % 2 == 1) != upper:
        wide = pltpu.roll(wide.astype(F32), HEAD_DIM, 1).astype(BF)
    keep = (lanes(wide.shape) >= HEAD_DIM) if upper else (lanes(wide.shape) < HEAD_DIM)
    return jnp.where(keep, wide, jnp.zeros_like(wide))


class Relay:
    def __init__(self, n_ctx, src, dst, send, recv):
        piece = src.shape[0] // n_ctx
        ctx = lax.axis_index("ctx")
        bits = high_bits(n_ctx)

        def cut(which):
            return pl.ds(pl.multiple_of(which * piece, piece), piece)

        self.levels = [[exchange(src.at[cut(ctx)], dst.at[cut(ctx)], "fsdp", 1, send.at[0], recv.at[0])]]
        e = 1
        for j, bit in enumerate(bits):
            level = []
            for m in masks_of(bits[:j]):
                part = dst.at[cut(ctx ^ m)]
                level.append(exchange(part, part, "ctx", bit, send.at[e], recv.at[e]))
                e += 1
            self.levels.append(level)

    def start(self):
        self.levels[0][0].start()

    def hop(self, j, landed=True):
        if landed:
            for copy in self.levels[j]:
                copy.wait_recv()
        for copy in self.levels[j + 1]:
            copy.start()

    def landed(self, j=-1):
        for copy in self.levels[j]:
            copy.wait_recv()

    def drain(self, levels=slice(None)):
        for level in self.levels[levels]:
            for copy in level:
                copy.wait_send()


def forward_kernel(
    n_ctx,
    n_head,
    span,
    q_ref,
    p_ref,
    wl_ref,
    wr_ref,
    gate_ref,
    up_ref,
    down_ref,
    o_ref,
    lse_ref,
    sum_ref,
    gate_other,
    up_other,
    down_other,
    q_pad,
    ext,
    max_ref,
    acc_ref,
    relay_send,
    relay_recv,
    left,
    right,
    from_lo,
    from_hi,
    *sems,
):
    rows, width = q_ref.shape
    heads = width // HEAD_DIM
    block = lax.axis_index("ctx") * 2 + lax.axis_index("fsdp")
    barrier = line_greet(n_head)
    greet(n_ctx)
    ext[...] = jnp.where(lanes(p_ref.shape) < HEAD_DIM, jnp.ones_like(p_ref[...]), p_ref[...])
    pl.semaphore_wait(barrier, line_peers(n_head) + len(partners(n_ctx)))
    gate = Relay(n_ctx, gate_ref, gate_other, relay_send.at[0], relay_recv.at[0])
    up = Relay(n_ctx, up_ref, up_other, relay_send.at[1], relay_recv.at[1])
    down = Relay(n_ctx, down_ref, down_other, relay_send.at[2], relay_recv.at[2])
    gate.start()
    up.start()
    down.hop(0, landed=False)
    step, steps, drain = line_sum(n_head, left, right, left, right, sum_ref, from_lo, from_hi, sems, 2)
    size = rows // GROUPS
    stack = heads * size
    sub = min(512, stack)
    per_group = CHUNKS // GROUPS

    def tile(start, first_row, masked):
        cut = pl.ds(start, span)
        for j in range(stack // sub):
            part = pl.ds(j * sub, sub)
            scores = mat_trans(q_pad[part, :], p_ref[cut, :])
            if masked:
                row = first_row + lax.rem(lax.broadcasted_iota(jnp.int32, (sub, span), 0), size)
                col = start + lax.broadcasted_iota(jnp.int32, (sub, span), 1)
                scores = jnp.where(col <= row, scores, NEG)
            old = max_ref[part, :]
            new = jnp.maximum(old, jnp.max(scores, axis=1, keepdims=True))
            weights = jnp.exp(scores - jnp.tile(new, (1, span // 128))).astype(BF)
            acc_ref[part, :] = acc_ref[part, :] * jnp.exp(old - new) + matmul(weights, ext[cut, :])
            max_ref[part, :] = new

    def run(s, carry):
        step(s)
        return carry

    def one_group(g, carry):
        @pl.when(g == GROUPS - 1)
        def _():
            gate.hop(0)
            down.hop(1)

        mine = pl.ds(pl.multiple_of(g * size, size), size)
        first_row = block * rows + g * size
        for h in range(heads):
            q_pad[h * size : (h + 1) * size, :] = head_lanes(q_ref.at[mine], h, False)
        max_ref[...] = jnp.full_like(max_ref, NEG)
        acc_ref[...] = jnp.zeros_like(acc_ref)

        tiles = (block + 1) * (rows // span)
        base = (g - 1) * per_group

        def sums(i):
            lax.fori_loop((i * per_group) // tiles, ((i + 1) * per_group) // tiles, lambda j, c: run(base + j, c), 0)

        def full(i, c):
            sums(i)
            tile(pl.multiple_of(i * span, span), first_row, False)
            return c

        lax.fori_loop(0, block * (rows // span), full, 0)
        for j in range(rows // span):
            sums(block * (rows // span) + j)
            tile(pl.multiple_of(block * rows + j * span, span), first_row, True)
        for h in range(heads):
            acc = acc_ref[h * size : (h + 1) * size, :]
            total = acc[:, :HEAD_DIM]
            o_ref[mine, h * HEAD_DIM : (h + 1) * HEAD_DIM] = (acc[:, HEAD_DIM:] / total).astype(BF)
            lse = max_ref[h * size : (h + 1) * size, :] + jnp.log(jnp.concatenate([total, total], axis=1))
            lse_ref[h, :, mine] = lse.T[0:1, :]
        att = o_ref[mine, :]
        left[mine, :] = matmul(att, wl_ref[...]).astype(BF)
        right[mine, :] = matmul(att, wr_ref[...]).astype(BF)
        return carry

    lax.fori_loop(0, GROUPS, one_group, 0)
    hops = len(high_bits(n_ctx))
    later = [(down, j) for j in range(2, hops)] + [(gate, 1), (up, 0)]
    for j in range(1, hops):
        later += [(up, j)] + ([(gate, j + 1)] if j + 1 < hops else [])
    at = CHUNKS - per_group
    rest = steps - at
    for i, (relay, j) in enumerate(later):
        to = CHUNKS - per_group + (rest * (2 * i + 1)) // (2 * len(later))
        lax.fori_loop(at, to, run, 0)
        at = to
        relay.hop(j)
    lax.fori_loop(at, steps, run, 0)
    for relay in (gate, up, down):
        relay.landed()
    gate.drain()
    up.drain()
    down.drain(slice(1, None))
    drain()


def attend_sum(queries, pair, out_left, out_right, gate, up, down, n_ctx, n_head, collective_id):
    rows, width = queries.shape
    heads = width // HEAD_DIM
    seq = pair.shape[0]
    span = min(512, rows)
    wide = 2 * out_left.shape[1]
    vmem = pl.BlockSpec(memory_space=pltpu.VMEM)
    anywhere = pl.BlockSpec(memory_space=pl.ANY)
    stack = heads * rows // GROUPS
    cost = pl.CostEstimate(flops=50_000_000_000, bytes_accessed=8 * rows * wide, transcendentals=0)
    return pl.pallas_call(
        functools.partial(forward_kernel, n_ctx, n_head, span),
        out_shape=(
            jax.ShapeDtypeStruct((rows, width), BF),
            jax.ShapeDtypeStruct((heads, 1, rows), F32),
            jax.ShapeDtypeStruct((rows, wide), BF),
            jax.ShapeDtypeStruct(gate.shape, BF),
            jax.ShapeDtypeStruct(up.shape, BF),
            jax.ShapeDtypeStruct(down.shape, BF),
        ),
        input_output_aliases={6: 5},
        in_specs=[vmem] * 4 + [anywhere] * 3,
        out_specs=(vmem, vmem, vmem, anywhere, anywhere, anywhere),
        scratch_shapes=[
            pltpu.VMEM((stack, 128), BF),
            pltpu.VMEM((seq, 128), BF),
            pltpu.VMEM((stack, 128), F32),
            pltpu.VMEM((stack, 128), F32),
            pltpu.SemaphoreType.DMA((3, n_ctx)),
            pltpu.SemaphoreType.DMA((3, n_ctx)),
        ]
        + line_scratch(rows, wide),
        compiler_params=pltpu.CompilerParams(collective_id=collective_id, has_side_effects=True),
        cost_estimate=cost,
        name="attend_sum",
    )(queries, pair, out_left, out_right, gate, up, down)


def backward_kernel(
    n_ctx,
    n_head,
    group,
    span,
    q_ref,
    g_ref,
    o_ref,
    lse_ref,
    p_ref,
    left_ref,
    right_ref,
    gate_both,
    up_both,
    dq_ref,
    dp_ref,
    sum_ref,
    gate_out,
    up_out,
    q_pad,
    g_pad,
    acc_ref,
    dl_ref,
    gate_land,
    up_land,
    far_land,
    cross_send,
    cross_recv,
    far_send,
    far_recv,
    work_l,
    work_r,
    from_lo,
    from_hi,
    *sems,
):
    rows, width = q_ref.shape
    heads = width // HEAD_DIM
    tiles = rows // span
    block = lax.axis_index("ctx") * 2 + lax.axis_index("fsdp")
    barrier = line_greet(n_head)
    greet(n_ctx)
    pl.semaphore_wait(barrier, line_peers(n_head) + len(partners(n_ctx)))
    part = gate_out.shape[0] // 2
    tops = [pl.ds(i * part, part) for i in range(2)]
    crosses = [
        exchange(gate_both.at[1, top], gate_land.at[top], "fsdp", 1, cross_send.at[i], cross_recv.at[i])
        for i, top in enumerate(tops)
    ] + [exchange(up_both.at[1], up_land, "fsdp", 1, cross_send.at[2], cross_recv.at[2])]
    for cross in crosses:
        cross.start()
    fars = [
        Chain(n_ctx, gate_out.at[top], far_land.at[i], far_send.at[i], far_recv.at[i])
        for i, top in enumerate(tops)
    ]
    hops = (11, 19)
    step, steps, drain = line_sum(
        n_head, left_ref, right_ref, work_l, work_r, sum_ref, from_lo, from_hi, sems
    )

    def hop(i):
        crosses[i].wait_recv()
        add_into(gate_out.at[tops[i]], gate_both.at[0, tops[i]], gate_land.at[tops[i]])
        fars[i].start()

    ahead = 3
    for s in range(ahead):
        step(s)
    dp_ref[...] = jnp.zeros_like(dp_ref)
    acc_ref[...] = jnp.zeros_like(acc_ref)
    for h in range(heads):
        cut = slice(h * HEAD_DIM, (h + 1) * HEAD_DIM)
        q_pad[h] = head_lanes(q_ref, h, False)
        g_pad[h] = head_lanes(g_ref, h, True)
        product = g_ref[:, cut].astype(F32) * o_ref[:, cut].astype(F32)
        dl_ref[h] = jnp.sum(product.T, axis=0, keepdims=True)

    def head_tile(h, pairs, start, masked):
        probs = jnp.exp(mat_trans(pairs, q_pad[h]) - lse_ref[h])
        if masked:
            row = block * rows + lax.broadcasted_iota(jnp.int32, (span, rows), 1)
            col = start + lax.broadcasted_iota(jnp.int32, (span, rows), 0)
            probs = jnp.where(col <= row, probs, 0.0)
        grads = (probs * (mat_trans(pairs, g_pad[h]) - dl_ref[h])).astype(BF)
        acc_ref[h] += trans_mat(grads, pairs)
        return matmul(probs.astype(BF), g_pad[h]) + matmul(grads, q_pad[h])

    groups = heads // group

    def two_steps(t):
        for j in range(2):

            @pl.when(ahead + 2 * t + j < steps)
            def _():
                step(ahead + 2 * t + j)

        for i in range(2):

            @pl.when(ahead + 2 * t == hops[i])
            def _():
                hop(i)

    def full(t, carry):
        two_steps(t)
        first = lax.rem(t, groups) * group
        start = pl.multiple_of((t // groups) * span, span)
        cut = pl.ds(start, span)
        total = head_tile(first, p_ref[cut, :], start, False)
        for h in range(1, group):
            total = total + head_tile(first + h, p_ref[cut, :], start, False)
        dp_ref[cut, :] += total
        return carry

    count = block * tiles * groups
    lax.fori_loop(0, count, full, 0)

    def last(t, carry):
        h = lax.rem(2 * t, heads)

        @pl.when(lax.rem(2 * t, group) == 0)
        def _():
            two_steps(count + 2 * t // group)

        start = pl.multiple_of(block * rows + (2 * t // heads) * span, span)
        cut = pl.ds(start, span)
        dp_ref[cut, :] += head_tile(h, p_ref[cut, :], start, True) + head_tile(h + 1, p_ref[cut, :], start, True)
        return carry

    lax.fori_loop(0, heads * tiles // 2, last, 0)
    for h in range(heads):
        dq_ref[:, h * HEAD_DIM : (h + 1) * HEAD_DIM] = acc_ref[h][:, :HEAD_DIM]

    begun = ahead + 2 * (count + groups * tiles)

    def rest(s, carry):
        step(s)

        for i in range(2):

            @pl.when(s == hops[i])
            def _():
                hop(i)

        return carry

    lax.fori_loop(jnp.minimum(begun, steps), steps, rest, 0)
    drain()
    crosses[2].wait_recv()
    add_into(up_out, up_both.at[0], up_land)
    for cross in crosses:
        cross.wait_send()
    for far in fars:
        far.finish()


def attend_back(queries, grads, attended, lse, pair, left, right, parts, n_ctx, n_head, collective_id):
    rows, width = queries.shape
    heads = width // HEAD_DIM
    seq = pair.shape[0]
    group = 4 if heads % 4 == 0 else 2
    span = min(512, rows)
    vmem = pl.BlockSpec(memory_space=pltpu.VMEM)
    flat = jax.ShapeDtypeStruct(parts[0].shape[1:], BF)
    n_far = len(high_bits(n_ctx)) - 1
    cost = pl.CostEstimate(
        flops=32 * rows * seq * width, bytes_accessed=8 * rows * width, transcendentals=0
    )
    return pl.pallas_call(
        functools.partial(backward_kernel, n_ctx, n_head, group, span),
        out_shape=(
            jax.ShapeDtypeStruct((rows, width), F32),
            jax.ShapeDtypeStruct((seq, 2 * HEAD_DIM), F32),
            jax.ShapeDtypeStruct((rows, 2 * left.shape[1]), BF),
            flat,
            flat,
        ),
        in_specs=[vmem] * 9,
        out_specs=(vmem,) * 5,
        scratch_shapes=[
            pltpu.VMEM((heads, rows, 128), BF),
            pltpu.VMEM((heads, rows, 128), BF),
            pltpu.VMEM((heads, rows, 128), F32),
            pltpu.VMEM((heads, 1, rows), F32),
            pltpu.VMEM(flat.shape, BF),
            pltpu.VMEM(flat.shape, BF),
            pltpu.VMEM((2, n_far, flat.shape[0] // 2, flat.shape[1]), BF),
            pltpu.SemaphoreType.DMA((3,)),
            pltpu.SemaphoreType.DMA((3,)),
            pltpu.SemaphoreType.DMA((2, n_far)),
            pltpu.SemaphoreType.DMA((2, n_far)),
        ]
        + line_scratch(rows, 2 * left.shape[1]),
        compiler_params=pltpu.CompilerParams(collective_id=collective_id, has_side_effects=True),
        cost_estimate=cost,
        name="attend_backward",
    )(queries, grads, attended, lse, pair, left, right, *parts)


def partners(n_ctx):
    return [("fsdp", 1)] + [("ctx", bit) for bit in high_bits(n_ctx)]


def greet(n_ctx):
    barrier = pltpu.get_barrier_semaphore()
    for axis, bit in partners(n_ctx):
        pl.semaphore_signal(
            barrier, inc=1, device_id={axis: lax.axis_index(axis) ^ bit}, device_id_type=MESH
        )
    return barrier


def masks_of(bits):
    masks = [0]
    for bit in bits:
        masks = masks + [m | bit for m in masks]
    return masks


def gather_pairs(n_ctx, rows, all_ref, send, recv):
    x = lax.axis_index("fsdp")
    ctx = lax.axis_index("ctx")
    copies = []

    def part(start, size, axis, bit):
        e = len(copies)
        cut = all_ref.at[pl.ds(pl.multiple_of(start, rows), size)]
        copy = pltpu.make_async_remote_copy(
            src_ref=cut,
            dst_ref=cut,
            send_sem=send.at[e],
            recv_sem=recv.at[e],
            device_id={axis: lax.axis_index(axis) ^ bit},
            device_id_type=MESH,
        )
        copy.start()
        copies.append(copy)
        return copy

    opening = part((ctx * 2 + x) * rows, rows, "fsdp", 1)

    def finish():
        opening.wait_recv()
        done = []
        for bit in high_bits(n_ctx):
            now = [part((ctx ^ m) * 2 * rows, 2 * rows, "ctx", bit) for m in masks_of(done)]
            for copy in now:
                copy.wait_recv()
            done.append(bit)
        for copy in copies:
            copy.wait_send()

    return finish


def project_kernel(
    n_ctx,
    x_ref,
    w_ref,
    gain_ref,
    cos_ref,
    sin_ref,
    wo_ref,
    down_ref,
    q_ref,
    p_ref,
    n_ref,
    w_other,
    gain_other,
    wo_other,
    down_other,
    acc_ref,
    send,
    recv,
    relay_send,
    relay_recv,
    gain_send,
    gain_recv,
):
    rows, width = x_ref.shape
    half = width // 2
    q_width = q_ref.shape[1]
    x_at = lax.axis_index("fsdp")
    block = lax.axis_index("ctx") * 2 + x_at
    barrier = greet(n_ctx)
    pl.semaphore_wait(barrier, len(partners(n_ctx)))
    gains = pltpu.make_async_remote_copy(
        src_ref=gain_ref,
        dst_ref=gain_other,
        send_sem=gain_send,
        recv_sem=gain_recv,
        device_id={"fsdp": 1 - x_at},
        device_id_type=MESH,
    )
    gains.start()
    part = half // 2
    first = [
        Relay(
            n_ctx,
            w_ref.at[pl.ds(i * part, part)],
            w_other.at[pl.ds(i * part, part)],
            relay_send.at[i],
            relay_recv.at[i],
        )
        for i in range(2)
    ]
    second = Relay(n_ctx, wo_ref, wo_other, relay_send.at[2], relay_recv.at[2])
    third = Relay(n_ctx, down_ref, down_other, relay_send.at[3], relay_recv.at[3])
    for relay in first:
        relay.start()
    second.start()
    gains.wait_recv()
    parts = 8
    size = rows // parts
    own = pl.ds(pl.multiple_of(x_at * half, half), half)
    other = pl.ds(pl.multiple_of((1 - x_at) * half, half), half)

    def cut_of(i):
        return pl.ds(pl.multiple_of(i * size, size), size)

    def norm(i, carry):
        cut = cut_of(i)
        left = x_ref[cut, own].astype(F32)
        right = x_ref[cut, other].astype(F32)
        total = jnp.sum(left * left, axis=1, keepdims=True) + jnp.sum(right * right, axis=1, keepdims=True)
        scale = lax.rsqrt(total / width + EPSILON)
        n_ref[cut, :half] = (left * scale * gain_ref[0:1, :]).astype(BF)
        n_ref[cut, half:] = (right * scale * gain_other[0:1, :]).astype(BF)
        return carry

    lax.fori_loop(0, parts, norm, 0)
    for relay in first:
        relay.hop(0)
    second.hop(0)

    def local(i, carry):
        cut = cut_of(i)
        acc_ref[cut, :] = matmul(n_ref[cut, :half], w_ref[...])
        return carry

    lax.fori_loop(0, parts, local, 0)
    for j in range(1, len(high_bits(n_ctx))):
        for relay in first:
            relay.hop(j)
    for relay in first:
        relay.landed()

    def rotated(wide, cut):
        low = lax.rem(lanes(wide.shape), HEAD_DIM) < HEAD_DIM // 2
        turned = jnp.where(low, pltpu.roll(wide, 128 - HEAD_DIM // 2, 1), pltpu.roll(wide, HEAD_DIM // 2, 1))
        return wide * cos_ref[cut, :] + turned * sin_ref[cut, :]

    def pairs(i, carry):
        cut = cut_of(i)
        both = acc_ref[cut, q_width:] + matmul(n_ref[cut, half:], w_other[:, q_width:])
        pair = jnp.where(lanes(both.shape) < HEAD_DIM, rotated(both, cut), both)
        p_ref[pl.ds(pl.multiple_of(block * rows + i * size, size), size), :] = pair.astype(BF)
        return carry

    def queries(i, carry):
        cut = cut_of(i)
        whole = acc_ref[cut, :q_width] + matmul(n_ref[cut, half:], w_other[:, :q_width])
        for j in range(q_width // 128):
            sl = slice(j * 128, (j + 1) * 128)
            q_ref[cut, sl] = (rotated(whole[:, sl], cut) * 0.125).astype(BF)
        return carry

    lax.fori_loop(0, parts, pairs, 0)
    finish = gather_pairs(n_ctx, rows, p_ref, send, recv)
    third.start()
    lax.fori_loop(0, parts, queries, 0)
    finish()
    for j in range(1, len(high_bits(n_ctx))):
        second.hop(j)
    second.landed()
    third.landed(0)
    for relay in first + [second]:
        relay.drain()
    third.drain(slice(0, 1))
    gains.wait_send()


def project(inputs, w_local, gains, cosine, sine, w_out, w_down, q_width, n_ctx, collective_id):
    rows, width = inputs.shape
    vmem = pl.BlockSpec(memory_space=pltpu.VMEM)
    anywhere = pl.BlockSpec(memory_space=pl.ANY)
    return pl.pallas_call(
        functools.partial(project_kernel, n_ctx),
        out_shape=(
            jax.ShapeDtypeStruct((rows, q_width), BF),
            jax.ShapeDtypeStruct((rows * 2 * n_ctx, 2 * HEAD_DIM), BF),
            jax.ShapeDtypeStruct((rows, width), BF),
            jax.ShapeDtypeStruct(w_local.shape, BF),
            jax.ShapeDtypeStruct(gains.shape, F32),
            jax.ShapeDtypeStruct(w_out.shape, BF),
            jax.ShapeDtypeStruct(w_down.shape, BF),
        ),
        in_specs=[vmem] * 5 + [anywhere] * 2,
        out_specs=(vmem,) * 5 + (anywhere,) * 2,
        scratch_shapes=[
            pltpu.VMEM((rows, w_local.shape[1]), F32),
            pltpu.SemaphoreType.DMA((n_ctx,)),
            pltpu.SemaphoreType.DMA((n_ctx,)),
            pltpu.SemaphoreType.DMA((4, n_ctx)),
            pltpu.SemaphoreType.DMA((4, n_ctx)),
            pltpu.SemaphoreType.DMA,
            pltpu.SemaphoreType.DMA,
        ],
        compiler_params=pltpu.CompilerParams(collective_id=collective_id, has_side_effects=True),
        name="project",
    )(inputs, w_local, gains, cosine, sine, w_out, w_down)


def line_sum(n, left, right, work_l, work_r, o_ref, from_lo, from_hi, sems, lag=LAG):
    s_up, r_up, s_dn, r_dn, s_a, r_a, s_b, r_b = sems
    me = lax.axis_index("head")
    rows, cols = left.shape
    size = rows // CHUNKS
    has_lo = me > 0
    has_hi = me < n - 1
    middle = jnp.logical_and(has_lo, has_hi)

    def at(k):
        return pl.ds(pl.multiple_of(k * size, size), size)

    def remote(src, dst, send, recv, target):
        return pltpu.make_async_remote_copy(
            src_ref=src,
            dst_ref=dst,
            send_sem=send,
            recv_sem=recv,
            device_id={"head": target},
            device_id_type=MESH,
        )

    def up(k, src):
        return remote(src.at[at(k)], from_lo.at[at(k)], s_up.at[k], r_up.at[k], me + 1)

    def down(k, src):
        return remote(src.at[at(k)], from_hi.at[at(k)], s_dn.at[k], r_dn.at[k], me - 1)

    def spread_a(k):
        part = o_ref.at[at(k), pl.ds(0, cols)]
        return remote(part, part, s_a.at[k], r_a.at[k], me + 1)

    def spread_b(k):
        part = o_ref.at[at(k), pl.ds(cols, cols)]
        return remote(part, part, s_b.at[k], r_b.at[k], me - 1)

    def valid(k):
        return jnp.logical_and(k >= 0, k < CHUNKS)

    def added(mine, there, k):
        return (mine[at(k), :].astype(F32) + there[at(k), :].astype(F32)).astype(BF)

    def step(s):
        k1 = s - lag * me
        k2 = s - lag * (n - 1 - me)
        k3 = s - lag * (n - 1 + me)
        k4 = s - lag * (2 * (n - 1) - me)

        @pl.when(jnp.logical_and(valid(k1), me == 0))
        def _():
            up(k1, right).start()

        @pl.when(jnp.logical_and(valid(k2), me == n - 1))
        def _():
            down(k2, left).start()

        @pl.when(jnp.logical_and(valid(k1), middle))
        def _():
            up(k1, right).wait_recv()
            work_r[at(k1), :] = added(right, from_lo, k1)
            up(k1, work_r).start()

        @pl.when(jnp.logical_and(valid(k1), me == n - 1))
        def _():
            up(k1, right).wait_recv()
            o_ref[at(k1), cols:] = added(right, from_lo, k1)
            spread_b(k1).start()

        @pl.when(jnp.logical_and(valid(k2), middle))
        def _():
            down(k2, left).wait_recv()
            work_l[at(k2), :] = added(left, from_hi, k2)
            down(k2, work_l).start()

        @pl.when(jnp.logical_and(valid(k2), me == 0))
        def _():
            down(k2, left).wait_recv()
            o_ref[at(k2), :cols] = added(left, from_hi, k2)
            spread_a(k2).start()

        @pl.when(jnp.logical_and(valid(k3), has_lo))
        def _():
            spread_a(k3).wait_recv()

            @pl.when(has_hi)
            def _():
                spread_a(k3).start()

        @pl.when(jnp.logical_and(valid(k4), has_hi))
        def _():
            spread_b(k4).wait_recv()

            @pl.when(has_lo)
            def _():
                spread_b(k4).start()

    def drain():
        def one(k, carry):
            @pl.when(has_hi)
            def _():
                up(k, right).wait_send()
                spread_a(k).wait_send()

            @pl.when(has_lo)
            def _():
                down(k, left).wait_send()
                spread_b(k).wait_send()

            return carry

        lax.fori_loop(0, CHUNKS, one, 0)

    return step, CHUNKS + 2 * lag * (n - 1), drain


def line_greet(n):
    me = lax.axis_index("head")
    barrier = pltpu.get_barrier_semaphore()

    @pl.when(me > 0)
    def _():
        pl.semaphore_signal(barrier, inc=1, device_id={"head": me - 1}, device_id_type=MESH)

    @pl.when(me < n - 1)
    def _():
        pl.semaphore_signal(barrier, inc=1, device_id={"head": me + 1}, device_id_type=MESH)

    return barrier


def line_peers(n):
    me = lax.axis_index("head")
    return jnp.where(me > 0, 1, 0) + jnp.where(me < n - 1, 1, 0)


def line_scratch(rows, width):
    return [pltpu.VMEM((rows, width // 2), BF)] * 4 + [pltpu.SemaphoreType.DMA((CHUNKS,))] * 8


def last_kernel(
    n_ctx,
    n_head,
    dq_ref,
    part_ref,
    cos_ref,
    sin_ref,
    w_l,
    w_r,
    n_ref,
    att_ref,
    low_ref,
    up_ref,
    gate_ref,
    down_ref,
    sum_ref,
    qkv_full,
    out_full,
    gate_full,
    up_full,
    down_full,
    work,
    land,
    raw,
    raw_land,
    n_land,
    low_land,
    att_land,
    up_sum,
    out_sent,
    out_kept,
    out_land,
    qkv_sent,
    qkv_kept,
    qkv_land,
    up_far,
    out_far,
    qkv_far,
    pair_send,
    pair_recv,
    trade_send,
    trade_recv,
    cross_send,
    cross_recv,
    far_send,
    far_recv,
    full_send,
    full_recv,
    full_local,
    left,
    right,
    from_lo,
    from_hi,
    *sems,
):
    rows, q_width = dq_ref.shape
    half = n_ref.shape[1] // 2
    quarter = half // 2
    x_at = lax.axis_index("fsdp")
    ctx = lax.axis_index("ctx")
    core = lax.rem(ctx, 2)
    barrier = line_greet(n_head)
    greet(n_ctx)
    work[...] = part_ref[...].astype(BF)
    up_sum[...] = up_ref[...]
    pl.semaphore_wait(barrier, line_peers(n_head) + len(partners(n_ctx)))

    def relative(side, c):
        return pl.ds(pl.multiple_of(side * half + c * quarter, quarter), quarter)

    def trade(src, dst, at):
        return exchange(src, dst, "ctx", 1, trade_send.at[at], trade_recv.at[at])

    pairs = []
    used = [0]

    def give(start, size, axis, bit):
        e = len(pairs)
        cut = pl.ds(pl.multiple_of(start, rows), size)
        copy = exchange(
            work.at[cut], land.at[pl.ds(used[0], size)], axis, bit, pair_send.at[e], pair_recv.at[e]
        )
        copy.start()
        pairs.append(copy)
        used[0] += size
        return copy, used[0] - size

    def take(start, size, at):
        cut = pl.ds(pl.multiple_of(start, rows), size)
        work[cut, :] = (work[cut, :].astype(F32) + land[at : at + size, :].astype(F32)).astype(BF)

    up_chain = Chain(n_ctx, up_sum, up_far, far_send.at[0], far_recv.at[0])
    out_chain = Chain(n_ctx, out_kept, out_far, far_send.at[1], far_recv.at[1])
    qkv_chain = Chain(n_ctx, qkv_kept, qkv_far, far_send.at[2], far_recv.at[2])

    def turned(wide, cut):
        low = lax.rem(lanes(wide.shape), HEAD_DIM) < HEAD_DIM // 2
        swapped = jnp.where(low, pltpu.roll(wide, 128 - HEAD_DIM // 2, 1), pltpu.roll(wide, HEAD_DIM // 2, 1))
        return wide * cos_ref[cut, :] - swapped * sin_ref[cut, :]

    def rotate_rows(i, carry):
        cut = pl.ds(pl.multiple_of(i * 128, 128), 128)
        for j in range(q_width // 128):
            sl = slice(j * 128, (j + 1) * 128)
            raw[cut, sl] = turned(dq_ref[cut, sl] * 0.125, cut).astype(BF)
        return carry

    trades = [trade(att_ref, att_land, 0)]
    for side in range(2):
        landing = pl.ds(side * quarter, quarter)
        trades.append(trade(low_ref.at[:, relative(side, 1 - core)], low_land.at[:, landing], 1 + side))
    late = []
    for side in range(2):
        landing = pl.ds(side * quarter, quarter)
        late.append(trade(n_ref.at[:, relative(side, 1 - core)], n_land.at[:, landing], 3 + side))

    def out_tiles(dst, side):
        def one(t, carry):
            cut = pl.ds(pl.multiple_of(t * 128, 128), 128)
            dst[cut, :] = (
                trans_mat(att_ref[:, cut], low_ref[:, relative(side, core)])
                + trans_mat(att_land[:, cut], low_land[:, side * quarter : (side + 1) * quarter])
            ).astype(BF)
            return carry

        lax.fori_loop(0, q_width // 128, one, 0)

    bits = high_bits(n_ctx)
    for j in range(len(bits)):
        bit = bits[len(bits) - 1 - j]
        masks = masks_of(bits[: len(bits) - 1 - j])
        now = [give((ctx ^ bit ^ m) * 2 * rows, 2 * rows, "ctx", bit) for m in masks]
        if j == 0:
            for t in trades + late:
                t.start()
            lax.fori_loop(0, rows // 128, rotate_rows, 0)
        if j == 1:
            for t in trades:
                t.wait_recv()
            out_tiles(out_sent, 1)
        for (copy, at), m in zip(now, masks):
            copy.wait_recv()
            take((ctx ^ m) * 2 * rows, 2 * rows, at)
    copy, at = give((ctx * 2 + 1 - x_at) * rows, rows, "fsdp", 1)
    out_cross = exchange(out_sent, out_land, "fsdp", 1, cross_send.at[0], cross_recv.at[0])
    out_cross.start()
    up_chain.start()
    out_tiles(out_kept, 0)
    copy.wait_recv()
    base = pl.multiple_of((ctx * 2 + x_at) * rows, rows)

    def finish_pair(i, carry):
        cut = pl.ds(pl.multiple_of(i * 128, 128), 128)
        mine = work[pl.ds(base + i * 128, 128), :].astype(F32) + land[pl.ds(at + i * 128, 128), :].astype(F32)
        raw[cut, q_width:] = jnp.where(lanes(mine.shape) < HEAD_DIM, turned(mine, cut), mine).astype(BF)
        left[cut, :] = mat_trans(raw[cut, :], w_l[...]).astype(BF)
        right[cut, :] = mat_trans(raw[cut, :], w_r[...]).astype(BF)
        return carry

    lax.fori_loop(0, rows // 128, finish_pair, 0)
    raw_trade = trade(raw, raw_land, 5)
    raw_trade.start()
    late.append(raw_trade)
    step, steps, drain = line_sum(n_head, left, right, left, right, sum_ref, from_lo, from_hi, sems)

    def run(s, carry):
        step(s)
        return carry

    def spread(src, whole, by_rows, e):
        size = src.shape[0 if by_rows else 1]
        cut = pl.ds(pl.multiple_of(core * size, size), size)
        dst = whole.at[cut] if by_rows else whole.at[:, cut]
        return (
            pltpu.make_async_copy(src, dst, full_local.at[e]),
            exchange(src, dst, "ctx", 1, full_send.at[e], full_recv.at[e]),
        )

    spreads = [spread(gate_ref, gate_full, True, 0), spread(down_ref, down_full, False, 1)]
    for pair in spreads:
        for copy in pair:
            copy.start()

    def qkv_tiles(dst, side):
        def one(t, carry):
            cut = pl.ds(pl.multiple_of(t * 128, 128), 128)
            there = pl.ds(pl.multiple_of(side * half + core * quarter + t * 128, 128), 128)
            landing = pl.ds(pl.multiple_of(side * quarter + t * 128, 128), 128)
            dst[cut, :] = (
                trans_mat(n_ref[:, there], raw[...]) + trans_mat(n_land[:, landing], raw_land[...])
            ).astype(BF)
            step(steps_at + t)
            return carry

        lax.fori_loop(0, quarter // 128, one, 0)

    lax.fori_loop(0, 2, run, 0)
    for t in late:
        t.wait_recv()
    steps_at = 2
    qkv_tiles(qkv_sent, 1)
    qkv_cross = exchange(qkv_sent, qkv_land, "fsdp", 1, cross_send.at[1], cross_recv.at[1])
    qkv_cross.start()
    steps_at += quarter // 128
    qkv_tiles(qkv_kept, 0)
    steps_at += quarter // 128
    out_cross.wait_recv()
    add_into(out_kept, out_kept, out_land)
    out_chain.start()
    rest = steps - steps_at
    stops = [steps_at + (rest * i) // 8 for i in range(9)]
    lax.fori_loop(stops[0], stops[2], run, 0)
    qkv_cross.wait_recv()
    add_into(qkv_kept, qkv_kept, qkv_land)
    qkv_chain.start()
    lax.fori_loop(stops[2], stops[4], run, 0)
    up_chain.finish()
    spreads.append(spread(up_sum, up_full, True, 2))
    for copy in spreads[-1]:
        copy.start()
    lax.fori_loop(stops[4], stops[6], run, 0)
    out_chain.finish()
    spreads.append(spread(out_kept, out_full, False, 3))
    for copy in spreads[-1]:
        copy.start()
    lax.fori_loop(stops[6], stops[8], run, 0)
    qkv_chain.finish()
    spreads.append(spread(qkv_kept, qkv_full, True, 4))
    for copy in spreads[-1]:
        copy.start()
    drain()
    for t in pairs + trades + late + [out_cross, qkv_cross]:
        t.wait_send()
    for local, remote in spreads:
        local.wait()
        remote.wait()


def last_sum(
    dq, part, cosine, sine, w_left, w_right, normed, attended, low, up, gate, down, n_ctx, n_head, collective_id
):
    rows, q_width = dq.shape
    width = normed.shape[1]
    half = width // 2
    quarter = half // 2
    narrow = w_left.shape[1]
    units = gate.shape[1]
    n_far = len(high_bits(n_ctx)) - 1
    vmem = pl.BlockSpec(memory_space=pltpu.VMEM)
    anywhere = pl.BlockSpec(memory_space=pl.ANY)
    dma = pltpu.SemaphoreType.DMA
    return pl.pallas_call(
        functools.partial(last_kernel, n_ctx, n_head),
        out_shape=(
            jax.ShapeDtypeStruct((rows, width), BF),
            jax.ShapeDtypeStruct((half, narrow), BF),
            jax.ShapeDtypeStruct((q_width, half), BF),
            jax.ShapeDtypeStruct((half, units), BF),
            jax.ShapeDtypeStruct((half, units), BF),
            jax.ShapeDtypeStruct((units, half), BF),
        ),
        in_specs=[vmem] * 12,
        out_specs=(vmem,) + (anywhere,) * 5,
        scratch_shapes=[
            pltpu.VMEM(part.shape, BF),
            pltpu.VMEM(part.shape, BF),
            pltpu.VMEM((rows, narrow), BF),
            pltpu.VMEM((rows, narrow), BF),
            pltpu.VMEM((rows, half), BF),
            pltpu.VMEM((rows, half), BF),
            pltpu.VMEM((rows, q_width), BF),
            pltpu.VMEM(up.shape, BF),
            pltpu.VMEM((q_width, quarter), BF),
            pltpu.VMEM((q_width, quarter), BF),
            pltpu.VMEM((q_width, quarter), BF),
            pltpu.VMEM((quarter, narrow), BF),
            pltpu.VMEM((quarter, narrow), BF),
            pltpu.VMEM((quarter, narrow), BF),
            pltpu.VMEM((n_far,) + up.shape, BF),
            pltpu.VMEM((n_far, q_width, quarter), BF),
            pltpu.VMEM((n_far, quarter, narrow), BF),
            dma((n_ctx,)),
            dma((n_ctx,)),
            dma((6,)),
            dma((6,)),
            dma((2,)),
            dma((2,)),
            dma((3, n_far)),
            dma((3, n_far)),
            dma((5,)),
            dma((5,)),
            dma((5,)),
        ]
        + line_scratch(rows, width),
        compiler_params=pltpu.CompilerParams(
            collective_id=collective_id, has_side_effects=True, vmem_limit_bytes=66_000_000
        ),
        cost_estimate=pl.CostEstimate(
            flops=50_000_000_000, bytes_accessed=8 * rows * width, transcendentals=0
        ),
        name="last_sum",
    )(dq, part, cosine, sine, w_left, w_right, normed, attended, low, up, gate, down)


def ffn_kernel(
    n_head,
    x_ref,
    mix_ref,
    cot_ref,
    gain_ref,
    gain_other,
    gate_l_hbm,
    gate_r_hbm,
    up_l_hbm,
    up_r_hbm,
    down_l_hbm,
    down_r_hbm,
    sum_ref,
    ffn_left,
    ffn_right,
    down_kept,
    gate_both,
    up_both,
    gate_l,
    gate_r,
    up_l,
    up_r,
    down_l,
    down_r,
    load_sem,
    n_ref,
    act_ref,
    gig_ref,
    uig_ref,
    cot_land,
    n_land,
    act_land,
    gig_land,
    uig_land,
    down_sent,
    down_land,
    out_tile,
    out_sem,
    trade_send,
    trade_recv,
    cross_send,
    cross_recv,
    left,
    right,
    from_lo,
    from_hi,
    *sems,
):
    rows, width = x_ref.shape
    half = width // 2
    quarter = half // 2
    units = act_ref.shape[1]
    x_at = lax.axis_index("fsdp")
    ctx_at = lax.axis_index("ctx")
    core = lax.rem(ctx_at, 2)
    own = pl.ds(pl.multiple_of(x_at * half, half), half)
    other = pl.ds(pl.multiple_of((1 - x_at) * half, half), half)
    barrier = line_greet(n_head)
    pl.semaphore_signal(barrier, inc=1, device_id={"fsdp": 1 - x_at}, device_id_type=MESH)
    pl.semaphore_signal(barrier, inc=1, device_id={"ctx": ctx_at ^ 1}, device_id_type=MESH)
    loads = [
        pltpu.make_async_copy(src, dst, load_sem.at[i])
        for i, (src, dst) in enumerate(
            (
                (gate_l_hbm, gate_l),
                (gate_r_hbm, gate_r),
                (up_l_hbm, up_l),
                (up_r_hbm, up_r),
                (down_l_hbm, down_l),
                (down_r_hbm, down_r),
            )
        )
    ]
    for load in loads:
        load.start()
    pl.semaphore_wait(barrier, line_peers(n_head) + 2)

    def trade(src, dst, at):
        return pltpu.make_async_remote_copy(
            src_ref=src,
            dst_ref=dst,
            send_sem=trade_send.at[at],
            recv_sem=trade_recv.at[at],
            device_id={"ctx": ctx_at ^ 1},
            device_id_type=MESH,
        )

    def absolute(side, c):
        start = (x_at if side == 0 else 1 - x_at) * half + c * quarter
        return pl.ds(pl.multiple_of(start, quarter), quarter)

    def relative(side, c):
        return pl.ds(pl.multiple_of(side * half + c * quarter, quarter), quarter)

    cot_trades = [
        trade(cot_ref.at[:, absolute(j, 1 - core)], cot_land.at[:, pl.ds(j * quarter, quarter)], j)
        for j in range(2)
    ]
    for copy in cot_trades:
        copy.start()

    def row_trades(g):
        mine = pl.ds(pl.multiple_of(g * (rows // FFN_GROUPS), rows // FFN_GROUPS), rows // FFN_GROUPS)
        at = 2 + g * 5
        return [
            trade(act_ref.at[mine], act_land.at[mine], at),
            trade(gig_ref.at[mine], gig_land.at[mine], at + 1),
            trade(uig_ref.at[mine], uig_land.at[mine], at + 2),
            trade(n_ref.at[mine, relative(0, 1 - core)], n_land.at[mine, pl.ds(0, quarter)], at + 3),
            trade(n_ref.at[mine, relative(1, 1 - core)], n_land.at[mine, pl.ds(quarter, quarter)], at + 4),
        ]

    step, steps, drain = line_sum(n_head, left, right, left, right, sum_ref, from_lo, from_hi, sems)

    def run(s, carry):
        step(s)
        return carry

    size = rows // FFN_GROUPS
    per_group = CHUNKS // FFN_GROUPS

    def one_group(g, carry):
        mine = pl.ds(pl.multiple_of(g * size, size), size)
        base = (g - 1) * per_group
        stops = [base + (per_group * i) // 4 for i in range(5)]
        hid_l = x_ref[mine, own].astype(F32) + mix_ref[mine, :half].astype(F32)
        hid_r = x_ref[mine, other].astype(F32) + mix_ref[mine, half:].astype(F32)
        total = jnp.sum(hid_l * hid_l, axis=1, keepdims=True) + jnp.sum(hid_r * hid_r, axis=1, keepdims=True)
        scale = lax.rsqrt(total / width + EPSILON)
        n_ref[mine, :half] = (hid_l * scale * gain_ref[1:2, :]).astype(BF)
        n_ref[mine, half:] = (hid_r * scale * gain_other[1:2, :]).astype(BF)
        lax.fori_loop(stops[0], stops[1], run, 0)

        @pl.when(g == 0)
        def _():
            for load in loads[:4]:
                load.wait()

        gate = matmul(n_ref[mine, :half], gate_l[...]) + matmul(n_ref[mine, half:], gate_r[...])
        up = matmul(n_ref[mine, :half], up_l[...]) + matmul(n_ref[mine, half:], up_r[...])
        lax.fori_loop(stops[1], stops[2], run, 0)
        sigma = jax.nn.sigmoid(gate)
        silu = gate * sigma
        act_ref[mine, :] = (silu * up).astype(BF)

        @pl.when(g == 0)
        def _():
            for load in loads[4:]:
                load.wait()

        grad = mat_trans(cot_ref[mine, own], down_l[...]) + mat_trans(cot_ref[mine, other], down_r[...])
        gig_ref[mine, :] = (grad * up * sigma * (1.0 + gate * (1.0 - sigma))).astype(BF)
        uig_ref[mine, :] = (grad * silu).astype(BF)
        lax.fori_loop(stops[2], stops[3], run, 0)
        gig = gig_ref[mine, :]
        uig = uig_ref[mine, :]
        left[mine, :] = (mat_trans(gig, gate_l[...]) + mat_trans(uig, up_l[...])).astype(BF)
        lax.fori_loop(stops[3], stops[4], run, 0)
        right[mine, :] = (mat_trans(gig, gate_r[...]) + mat_trans(uig, up_r[...])).astype(BF)
        for copy in row_trades(g):
            copy.start()
        return carry

    lax.fori_loop(0, FFN_GROUPS, one_group, 0)
    first = CHUNKS - per_group
    rest = steps - first
    tile = 128
    down_tiles = units // tile
    row_tiles = quarter // tile
    total_work = down_tiles + 4 * row_tiles + 2 * FFN_GROUPS

    def sums(i, weight=1):
        lax.fori_loop(
            first + (rest * i) // total_work, first + (rest * (i + weight)) // total_work, run, 0
        )

    for copy in cot_trades:
        copy.wait_recv()

    def landed(g, carry):
        for copy in row_trades(g):
            copy.wait_recv()
        return carry

    lax.fori_loop(0, FFN_GROUPS, landed, 0)

    def down_tile(t, carry):
        sums(t)
        cut = pl.ds(pl.multiple_of(t * tile, tile), tile)
        mine = act_ref[:, cut]
        theirs = act_land[:, cut]
        for dst, side in ((down_sent, 1), (down_kept, 0)):
            dst[cut, :] = (
                trans_mat(mine, cot_ref[:, absolute(side, core)])
                + trans_mat(theirs, cot_land[:, side * quarter : (side + 1) * quarter])
            ).astype(BF)
        return carry

    lax.fori_loop(0, down_tiles, down_tile, 0)
    cross = pltpu.make_async_remote_copy(
        src_ref=down_sent,
        dst_ref=down_land,
        send_sem=cross_send,
        recv_sem=cross_recv,
        device_id={"fsdp": 1 - x_at},
        device_id_type=MESH,
    )
    cross.start()
    done = down_tiles

    def out_copy(dst, t, slot):
        cut = pl.ds(pl.multiple_of(lax.rem(t, row_tiles) * tile, tile), tile)
        return pltpu.make_async_copy(out_tile.at[slot], dst.at[1 - t // row_tiles, cut], out_sem.at[slot])

    for dst, own_grad, their_grad in ((gate_both, gig_ref, gig_land), (up_both, uig_ref, uig_land)):

        def row_tile(t, carry):
            sums(done + t)
            slot = lax.rem(t, 2)
            side = 1 - t // row_tiles
            row = lax.rem(t, row_tiles) * tile
            there = pl.ds(pl.multiple_of(side * half + core * quarter + row, tile), tile)
            landing = pl.ds(pl.multiple_of(side * quarter + row, tile), tile)
            value = (
                trans_mat(n_ref[:, there], own_grad[...]) + trans_mat(n_land[:, landing], their_grad[...])
            ).astype(BF)

            @pl.when(t >= 2)
            def _():
                out_copy(dst, t - 2, slot).wait()

            out_tile[slot] = value
            out_copy(dst, t, slot).start()
            return carry

        lax.fori_loop(0, 2 * row_tiles, row_tile, 0)
        for t in range(2 * row_tiles - 2, 2 * row_tiles):
            out_copy(dst, t, t % 2).wait()
        done += 2 * row_tiles

    def project_down(g, carry):
        mine = pl.ds(pl.multiple_of(g * size, size), size)
        sums(done + 2 * g, 2)
        ffn_left[mine, :] = matmul(act_ref[mine, :], down_l[...]).astype(BF)
        ffn_right[mine, :] = matmul(act_ref[mine, :], down_r[...]).astype(BF)
        return carry

    lax.fori_loop(0, FFN_GROUPS, project_down, 0)
    cross.wait_recv()

    def finish(t, carry):
        cut = pl.ds(pl.multiple_of(t * tile, tile), tile)
        down_kept[cut, :] = (down_kept[cut, :].astype(F32) + down_land[cut, :].astype(F32)).astype(BF)
        return carry

    lax.fori_loop(0, down_tiles, finish, 0)
    cross.wait_send()
    for copy in cot_trades:
        copy.wait_send()

    def sent(g, carry):
        for copy in row_trades(g):
            copy.wait_send()
        return carry

    lax.fori_loop(0, FFN_GROUPS, sent, 0)
    drain()


def ffn_sum(inputs, mixed, cot, gains, gains_other, gate, gate_o, up, up_o, down, down_o, n_head, collective_id):
    rows, width = inputs.shape
    units = gate.shape[1]
    vmem = pl.BlockSpec(memory_space=pltpu.VMEM)
    wide = jax.ShapeDtypeStruct((rows, width), BF)
    narrow = jax.ShapeDtypeStruct((rows, width // 2), BF)
    quarter = width // 4
    flat = jax.ShapeDtypeStruct((2, quarter, units), BF)
    anywhere = pl.BlockSpec(memory_space=pl.ANY)
    trades = 2 + 5 * FFN_GROUPS
    return pl.pallas_call(
        functools.partial(ffn_kernel, n_head),
        out_shape=(wide, narrow, narrow, jax.ShapeDtypeStruct((units, quarter), BF), flat, flat),
        in_specs=[vmem] * 5 + [anywhere] * 6,
        out_specs=(vmem,) * 4 + (anywhere,) * 2,
        scratch_shapes=[pltpu.VMEM(w.shape, BF) for w in (gate, gate, up, up, down, down)]
        + [pltpu.SemaphoreType.DMA((6,)), pltpu.VMEM((rows, width), BF)]
        + [pltpu.VMEM((rows, units), BF)] * 3
        + [pltpu.VMEM((rows, width // 2), BF)] * 2
        + [pltpu.VMEM((rows, units), BF)] * 3
        + [pltpu.VMEM((units, quarter), BF)] * 2
        + [
            pltpu.VMEM((2, 128, units), BF),
            pltpu.SemaphoreType.DMA((2,)),
            pltpu.SemaphoreType.DMA((trades,)),
            pltpu.SemaphoreType.DMA((trades,)),
            pltpu.SemaphoreType.DMA,
            pltpu.SemaphoreType.DMA,
        ]
        + line_scratch(rows, width),
        compiler_params=pltpu.CompilerParams(
            collective_id=collective_id, has_side_effects=True, vmem_limit_bytes=66_000_000
        ),
        cost_estimate=pl.CostEstimate(
            flops=50_000_000_000, bytes_accessed=8 * rows * width, transcendentals=0
        ),
        name="ffn_sum",
    )(inputs, mixed, cot, gains, gains_other, gate, gate_o, up, up_o, down, down_o)


def halves(ref, x_at):
    half = ref.shape[1] // 2
    own = pl.ds(pl.multiple_of(x_at * half, half), half)
    other = pl.ds(pl.multiple_of((1 - x_at) * half, half), half)
    return ref[:, own].astype(F32), ref[:, other].astype(F32)


def norm_back(values, grads, gains, width):
    scale = lax.rsqrt(sum(jnp.sum(v * v, axis=1, keepdims=True) for v in values) / width + EPSILON)
    units = [v * scale for v in values]
    scaled = [g * gain for g, gain in zip(grads, gains)]
    mean = sum(jnp.sum(s * u, axis=1, keepdims=True) for s, u in zip(scaled, units)) / width
    return [scale * (s - u * mean) for s, u in zip(scaled, units)], [g * u for g, u in zip(grads, units)]


def add_gain(gain_ref, products):
    @pl.when(pl.program_id(0) == 0)
    def _():
        gain_ref[...] = jnp.zeros_like(gain_ref)

    half = products[0].shape[1]
    gain_ref[0:1, :half] += jnp.sum(products[0], axis=0, keepdims=True)
    gain_ref[0:1, half:] += jnp.sum(products[1], axis=0, keepdims=True)


def middle_kernel(at_ref, x_ref, mix_ref, grad_ref, cot_ref, gain_ref, other_ref, wl_ref, wr_ref, hid_ref, low_ref, att_ref, part_ref):
    width = x_ref.shape[1]
    half = width // 2
    x_at = at_ref[0]
    x_l, x_r = halves(x_ref, x_at)
    cot_l, cot_r = halves(cot_ref, x_at)
    values = (x_l + mix_ref[:, :half].astype(F32), x_r + mix_ref[:, half:].astype(F32))
    grads = (grad_ref[:, :half].astype(F32), grad_ref[:, half:].astype(F32))
    (d_l, d_r), products = norm_back(values, grads, (gain_ref[1:2, :], other_ref[1:2, :]), width)
    add_gain(part_ref, products)
    hid_l = cot_l + d_l
    hid_r = cot_r + d_r
    hid_ref[:, :half] = hid_l
    hid_ref[:, half:] = hid_r
    low_l = hid_l.astype(BF)
    low_r = hid_r.astype(BF)
    low_ref[:, :half] = low_l
    low_ref[:, half:] = low_r
    att_ref[...] = (mat_trans(low_l, wl_ref[...]) + mat_trans(low_r, wr_ref[...])).astype(BF)


def end_kernel(at_ref, x_ref, mix_ref, ffn_ref, grad_ref, hid_ref, gain_ref, other_ref, out_ref, in_grad_ref, part_ref):
    width = x_ref.shape[1]
    half = width // 2
    x_at = at_ref[0]
    own = pl.ds(pl.multiple_of(x_at * half, half), half)
    other = pl.ds(pl.multiple_of((1 - x_at) * half, half), half)
    x_l, x_r = halves(x_ref, x_at)
    out_ref[:, own] = (x_l + mix_ref[:, :half].astype(F32) + ffn_ref[:, :half].astype(F32)).astype(BF)
    out_ref[:, other] = (x_r + mix_ref[:, half:].astype(F32) + ffn_ref[:, half:].astype(F32)).astype(BF)
    grads = (grad_ref[:, :half].astype(F32), grad_ref[:, half:].astype(F32))
    (d_l, d_r), products = norm_back((x_l, x_r), grads, (gain_ref[0:1, :], other_ref[0:1, :]), width)
    add_gain(part_ref, products)
    in_grad_ref[:, own] = hid_ref[:, :half] + d_l
    in_grad_ref[:, other] = hid_ref[:, half:] + d_r


def by_rows(kernel, x_at, arrays, whole, outs):
    rows, width = arrays[0].shape
    size = min(128, rows)

    def block(shape):
        return pl.BlockSpec((size, shape[1]), lambda i, *_: (i, 0))

    def all_of(shape):
        return pl.BlockSpec(shape, lambda i, *_: (0, 0))

    gain = jax.ShapeDtypeStruct((8, width), F32)
    return pl.pallas_call(
        kernel,
        out_shape=tuple(outs) + (gain,),
        grid_spec=pltpu.PrefetchScalarGridSpec(
            num_scalar_prefetch=1,
            grid=(rows // size,),
            in_specs=[block(a.shape) for a in arrays] + [all_of(a.shape) for a in whole],
            out_specs=[block(o.shape) for o in outs] + [all_of(gain.shape)],
        ),
        cost_estimate=pl.CostEstimate(flops=4_000_000_000, bytes_accessed=24 * rows * width, transcendentals=0),
    )(x_at, *arrays, *whole)


def flip(array, axis, bit, size):
    return lax.ppermute(array, axis, [(i, i ^ bit) for i in range(size)])


def shards(
    n_ctx,
    n_head,
    inputs,
    query_weight,
    key_weight,
    value_weight,
    output_weight,
    gate_weight,
    up_weight,
    down_weight,
    attn_gain,
    ffn_gain,
    cotangent,
):
    rows, width = inputs.shape
    half = width // 2
    x_at = lax.axis_index("fsdp")
    ctx_at = lax.axis_index("ctx")
    core = lax.rem(ctx_at, 2)
    block = ctx_at * 2 + x_at
    block_arr = jnp.reshape(block, (1,)).astype(jnp.int32)

    every = high_bits(n_ctx)

    q_width = query_weight.shape[1]
    half_dim = HEAD_DIM // 2
    positions = block * rows + jnp.arange(rows, dtype=jnp.int32)
    lane = lax.broadcasted_iota(jnp.int32, (rows, 2 * HEAD_DIM), 1)
    freqs = 10000.0 ** (-2.0 * (lane % half_dim).astype(F32) / HEAD_DIM)
    angles = positions.astype(F32)[:, None] * freqs
    cosine = jnp.cos(angles)
    sine = jnp.sin(angles)
    signed = jnp.where(lane % HEAD_DIM < half_dim, -sine, sine)
    qkv_local = jnp.concatenate([query_weight, key_weight, value_weight], axis=1)
    gains_local = jnp.stack([attn_gain.astype(F32), ffn_gain.astype(F32)])
    queries, pair, normed_one, qkv_other, gains_other, out_other, down_begun = project(
        inputs, qkv_local, gains_local, cosine, signed, output_weight, down_weight, q_width, n_ctx, 4
    )
    attended, lse, mixed, gate_other, up_other, down_other = attend_sum(
        queries, pair, output_weight, out_other, gate_weight, up_weight, down_begun, n_ctx, n_head, 1
    )
    low_sum, down_left, down_right, down_kept, gate_both, up_both = ffn_sum(
        inputs,
        mixed,
        cotangent,
        gains_local,
        gains_other,
        gate_weight,
        gate_other,
        up_weight,
        up_other,
        down_weight,
        down_other,
        n_head,
        2,
    )
    x_arr = jnp.reshape(x_at, (1,)).astype(jnp.int32)
    wide = jax.ShapeDtypeStruct((rows, width), F32)
    flat = jax.ShapeDtypeStruct((rows, width), BF)
    hidden_grad, hidden_low, attended_grad, gain_two_part = by_rows(
        middle_kernel,
        x_arr,
        (inputs, mixed, low_sum, cotangent),
        (gains_local, gains_other, output_weight, out_other),
        (wide, flat, jax.ShapeDtypeStruct(attended.shape, BF)),
    )
    down_far = down_kept
    for bit in every[:-1]:
        down_far = (down_far.astype(F32) + flip(down_far, "ctx", bit, n_ctx).astype(F32)).astype(BF)
    query_acc, pair_acc, ffn_out, gate_far, up_crossed = attend_back(
        queries,
        attended_grad,
        attended,
        lse,
        pair,
        down_left,
        down_right,
        (gate_both, up_both),
        n_ctx,
        n_head,
        6,
    )
    last, qkv_full, out_full, gate_full, up_full, down_full = last_sum(
        query_acc,
        pair_acc,
        cosine,
        signed,
        qkv_local,
        qkv_other,
        normed_one,
        attended,
        hidden_low,
        up_crossed,
        gate_far,
        down_far,
        n_ctx,
        n_head,
        3,
    )
    outputs, input_grad, gain_one_part = by_rows(
        end_kernel, x_arr, (inputs, mixed, ffn_out, last, hidden_grad), (gains_local, gains_other), (flat, wide)
    )
    query_grad = qkv_full[:, :q_width].astype(F32)
    key_grad = qkv_full[:, q_width : q_width + HEAD_DIM].astype(F32)
    value_grad = qkv_full[:, q_width + HEAD_DIM :].astype(F32)

    gain_parts = jnp.stack([gain_one_part[0], gain_two_part[0]])
    gain_kept = gain_parts[:, :half] + flip(gain_parts[:, half:], "fsdp", 1, 2)
    for bit in every:
        gain_kept = gain_kept + flip(gain_kept, "ctx", bit, n_ctx)

    return (
        outputs,
        input_grad,
        query_grad,
        key_grad,
        value_grad,
        out_full.astype(F32),
        gate_full.astype(F32),
        up_full.astype(F32),
        down_full.astype(F32),
        gain_kept[0],
        gain_kept[1],
    )


def solution(mesh):
    n_ctx = mesh.shape["ctx"]

    def body(*args):
        return shards(n_ctx, mesh.shape["head"], *args)

    return jax.shard_map(
        body,
        mesh=mesh,
        in_specs=(
            P(("ctx", "fsdp"), None),
            P("fsdp", "head"),
            P("fsdp", "head"),
            P("fsdp", "head"),
            P("head", "fsdp"),
            P("fsdp", "head"),
            P("fsdp", "head"),
            P("head", "fsdp"),
            P("fsdp"),
            P("fsdp"),
            P(("ctx", "fsdp"), None),
        ),
        out_specs=(
            P(("ctx", "fsdp"), None),
            P(("ctx", "fsdp"), None),
            P("fsdp", "head"),
            P("fsdp", "head"),
            P("fsdp", "head"),
            P("head", "fsdp"),
            P("fsdp", "head"),
            P("fsdp", "head"),
            P("head", "fsdp"),
            P("fsdp"),
            P("fsdp"),
        ),
        check_vma=False,
    )
```

```python
import functools

import jax
import jax.numpy as jnp
from jax import lax
from jax.experimental import pallas as pl
from jax.experimental.pallas import tpu as pltpu
from jax.sharding import PartitionSpec as P


HEAD_DIM = 64
EPSILON = 1e-05
NEG = -1e30
BF = jnp.bfloat16
F32 = jnp.float32
MESH = pl.DeviceIdType.MESH
CHUNKS = 16
LAG = 3
GROUPS = 4
FFN_GROUPS = 2


def matmul(left, right):
    return jnp.dot(left, right, preferred_element_type=F32)


def mat_trans(left, right):
    return lax.dot_general(left, right, (((1,), (1,)), ((), ())), preferred_element_type=F32)


def trans_mat(left, right):
    return lax.dot_general(left, right, (((0,), (0,)), ((), ())), preferred_element_type=F32)


def exchange(src, dst, axis, bit, send, recv):
    return pltpu.make_async_remote_copy(
        src_ref=src,
        dst_ref=dst,
        send_sem=send,
        recv_sem=recv,
        device_id={axis: lax.axis_index(axis) ^ bit},
        device_id_type=MESH,
    )


def add_into(dst, left, right):
    size = 64

    def one(i, carry):
        cut = pl.ds(pl.multiple_of(i * size, size), size)
        dst[cut, :] = (left[cut, :].astype(F32) + right[cut, :].astype(F32)).astype(BF)
        return carry

    lax.fori_loop(0, dst.shape[0] // size, one, 0)


class Chain:
    def __init__(self, n_ctx, ref, land, send, recv):
        self.ref, self.land, self.send, self.recv = ref, land, send, recv
        self.bits = high_bits(n_ctx)[:-1]

    def _copy(self, j):
        return exchange(self.ref, self.land.at[j], "ctx", self.bits[j], self.send.at[j], self.recv.at[j])

    def start(self):
        self._copy(0).start()

    def finish(self):
        for j in range(len(self.bits)):
            if j > 0:
                self._copy(j).start()
            self._copy(j).wait()
            add_into(self.ref, self.ref, self.land.at[j])


def high_bits(size):
    bits = []
    bit = size // 2
    while bit >= 1:
        bits.append(bit)
        bit //= 2
    return bits


def lanes(shape):
    return lax.broadcasted_iota(jnp.int32, shape, 1)


def head_lanes(ref, h, upper):
    wide = ref[:, (h // 2) * 128 : (h // 2) * 128 + 128]
    if (h % 2 == 1) != upper:
        wide = pltpu.roll(wide.astype(F32), HEAD_DIM, 1).astype(BF)
    keep = (lanes(wide.shape) >= HEAD_DIM) if upper else (lanes(wide.shape) < HEAD_DIM)
    return jnp.where(keep, wide, jnp.zeros_like(wide))


class Relay:
    def __init__(self, n_ctx, src, dst, send, recv):
        piece = src.shape[0] // n_ctx
        ctx = lax.axis_index("ctx")
        bits = high_bits(n_ctx)

        def cut(which):
            return pl.ds(pl.multiple_of(which * piece, piece), piece)

        self.levels = [[exchange(src.at[cut(ctx)], dst.at[cut(ctx)], "fsdp", 1, send.at[0], recv.at[0])]]
        e = 1
        for j, bit in enumerate(bits):
            level = []
            for m in masks_of(bits[:j]):
                part = dst.at[cut(ctx ^ m)]
                level.append(exchange(part, part, "ctx", bit, send.at[e], recv.at[e]))
                e += 1
            self.levels.append(level)

    def start(self):
        self.levels[0][0].start()

    def hop(self, j, landed=True):
        if landed:
            for copy in self.levels[j]:
                copy.wait_recv()
        for copy in self.levels[j + 1]:
            copy.start()

    def landed(self, j=-1):
        for copy in self.levels[j]:
            copy.wait_recv()

    def drain(self, levels=slice(None)):
        for level in self.levels[levels]:
            for copy in level:
                copy.wait_send()


def forward_kernel(
    n_ctx,
    n_head,
    span,
    q_ref,
    p_ref,
    wl_ref,
    wr_ref,
    gate_ref,
    up_ref,
    down_ref,
    o_ref,
    lse_ref,
    sum_ref,
    gate_other,
    up_other,
    down_other,
    q_pad,
    ext,
    max_ref,
    acc_ref,
    relay_send,
    relay_recv,
    left,
    right,
    from_lo,
    from_hi,
    *sems,
):
    rows, width = q_ref.shape
    heads = width // HEAD_DIM
    block = lax.axis_index("ctx") * 2 + lax.axis_index("fsdp")
    barrier = line_greet(n_head)
    greet(n_ctx)
    ext[...] = jnp.where(lanes(p_ref.shape) < HEAD_DIM, jnp.ones_like(p_ref[...]), p_ref[...])
    pl.semaphore_wait(barrier, line_peers(n_head) + len(partners(n_ctx)))
    gate = Relay(n_ctx, gate_ref, gate_other, relay_send.at[0], relay_recv.at[0])
    up = Relay(n_ctx, up_ref, up_other, relay_send.at[1], relay_recv.at[1])
    down = Relay(n_ctx, down_ref, down_other, relay_send.at[2], relay_recv.at[2])
    gate.start()
    up.start()
    down.hop(0, landed=False)
    step, steps, drain = line_sum(n_head, left, right, left, right, sum_ref, from_lo, from_hi, sems, 2)
    size = rows // GROUPS
    stack = heads * size
    sub = min(512, stack)
    per_group = CHUNKS // GROUPS

    def tile(start, first_row, masked):
        cut = pl.ds(start, span)
        for j in range(stack // sub):
            part = pl.ds(j * sub, sub)
            scores = mat_trans(q_pad[part, :], p_ref[cut, :])
            if masked:
                row = first_row + lax.rem(lax.broadcasted_iota(jnp.int32, (sub, span), 0), size)
                col = start + lax.broadcasted_iota(jnp.int32, (sub, span), 1)
                scores = jnp.where(col <= row, scores, NEG)
            old = max_ref[part, :]
            new = jnp.maximum(old, jnp.max(scores, axis=1, keepdims=True))
            weights = jnp.exp(scores - jnp.tile(new, (1, span // 128))).astype(BF)
            acc_ref[part, :] = acc_ref[part, :] * jnp.exp(old - new) + matmul(weights, ext[cut, :])
            max_ref[part, :] = new

    def run(s, carry):
        step(s)
        return carry

    def one_group(g, carry):
        @pl.when(jnp.logical_and(g == GROUPS - 1, block >= n_ctx))
        def _():
            gate.hop(0)
            down.hop(1)

        mine = pl.ds(pl.multiple_of(g * size, size), size)
        first_row = block * rows + g * size
        for h in range(heads):
            q_pad[h * size : (h + 1) * size, :] = head_lanes(q_ref.at[mine], h, False)
        max_ref[...] = jnp.full_like(max_ref, NEG)
        acc_ref[...] = jnp.zeros_like(acc_ref)

        tiles = (block + 1) * (rows // span)
        base = (g - 1) * per_group

        def sums(i):
            lax.fori_loop((i * per_group) // tiles, ((i + 1) * per_group) // tiles, lambda j, c: run(base + j, c), 0)

        def full(i, c):
            sums(i)
            tile(pl.multiple_of(i * span, span), first_row, False)
            return c

        lax.fori_loop(0, block * (rows // span), full, 0)
        for j in range(rows // span):
            sums(block * (rows // span) + j)
            tile(pl.multiple_of(block * rows + j * span, span), first_row, True)
        for h in range(heads):
            acc = acc_ref[h * size : (h + 1) * size, :]
            total = acc[:, :HEAD_DIM]
            o_ref[mine, h * HEAD_DIM : (h + 1) * HEAD_DIM] = (acc[:, HEAD_DIM:] / total).astype(BF)
            lse = max_ref[h * size : (h + 1) * size, :] + jnp.log(jnp.concatenate([total, total], axis=1))
            lse_ref[h, :, mine] = lse.T[0:1, :]
        att = o_ref[mine, :]
        left[mine, :] = matmul(att, wl_ref[...]).astype(BF)
        right[mine, :] = matmul(att, wr_ref[...]).astype(BF)
        return carry

    lax.fori_loop(0, GROUPS, one_group, 0)
    lax.fori_loop(CHUNKS - per_group, CHUNKS, run, 0)

    @pl.when(block < n_ctx)
    def _():
        gate.hop(0)
        down.hop(1)

    hops = len(high_bits(n_ctx))
    later = [(down, j) for j in range(2, hops)] + [(gate, 1), (up, 0)]
    for j in range(1, hops):
        later += [(up, j)] + ([(gate, j + 1)] if j + 1 < hops else [])
    at = CHUNKS
    rest = steps - at
    for i, (relay, j) in enumerate(later):
        to = CHUNKS + (rest * (2 * i + 1)) // (2 * len(later))
        lax.fori_loop(at, to, run, 0)
        at = to
        relay.hop(j)
    lax.fori_loop(at, steps, run, 0)
    for relay in (gate, up, down):
        relay.landed()
    gate.drain()
    up.drain()
    down.drain(slice(1, None))
    drain()


def attend_sum(queries, pair, out_left, out_right, gate, up, down, n_ctx, n_head, collective_id):
    rows, width = queries.shape
    heads = width // HEAD_DIM
    seq = pair.shape[0]
    span = min(512, rows)
    wide = 2 * out_left.shape[1]
    vmem = pl.BlockSpec(memory_space=pltpu.VMEM)
    anywhere = pl.BlockSpec(memory_space=pl.ANY)
    stack = heads * rows // GROUPS
    cost = pl.CostEstimate(flops=50_000_000_000, bytes_accessed=8 * rows * wide, transcendentals=0)
    return pl.pallas_call(
        functools.partial(forward_kernel, n_ctx, n_head, span),
        out_shape=(
            jax.ShapeDtypeStruct((rows, width), BF),
            jax.ShapeDtypeStruct((heads, 1, rows), F32),
            jax.ShapeDtypeStruct((rows, wide), BF),
            jax.ShapeDtypeStruct(gate.shape, BF),
            jax.ShapeDtypeStruct(up.shape, BF),
            jax.ShapeDtypeStruct(down.shape, BF),
        ),
        input_output_aliases={6: 5},
        in_specs=[vmem] * 4 + [anywhere] * 3,
        out_specs=(vmem, vmem, vmem, anywhere, anywhere, anywhere),
        scratch_shapes=[
            pltpu.VMEM((stack, 128), BF),
            pltpu.VMEM((seq, 128), BF),
            pltpu.VMEM((stack, 128), F32),
            pltpu.VMEM((stack, 128), F32),
            pltpu.SemaphoreType.DMA((3, n_ctx)),
            pltpu.SemaphoreType.DMA((3, n_ctx)),
        ]
        + line_scratch(rows, wide),
        compiler_params=pltpu.CompilerParams(collective_id=collective_id, has_side_effects=True),
        cost_estimate=cost,
        name="attend_sum",
    )(queries, pair, out_left, out_right, gate, up, down)


def backward_kernel(
    n_ctx,
    n_head,
    group,
    span,
    q_ref,
    g_ref,
    o_ref,
    lse_ref,
    p_ref,
    left_ref,
    right_ref,
    gate_both,
    up_both,
    dq_ref,
    dp_ref,
    sum_ref,
    gate_out,
    up_out,
    q_pad,
    g_pad,
    acc_ref,
    dl_ref,
    gate_land,
    up_land,
    far_land,
    cross_send,
    cross_recv,
    far_send,
    far_recv,
    work_l,
    work_r,
    from_lo,
    from_hi,
    *sems,
):
    rows, width = q_ref.shape
    heads = width // HEAD_DIM
    tiles = rows // span
    block = lax.axis_index("ctx") * 2 + lax.axis_index("fsdp")
    barrier = line_greet(n_head)
    greet(n_ctx)
    pl.semaphore_wait(barrier, line_peers(n_head) + len(partners(n_ctx)))
    part = gate_out.shape[0] // 2
    tops = [pl.ds(i * part, part) for i in range(2)]
    crosses = [
        exchange(gate_both.at[1, top], gate_land.at[top], "fsdp", 1, cross_send.at[i], cross_recv.at[i])
        for i, top in enumerate(tops)
    ] + [exchange(up_both.at[1], up_land, "fsdp", 1, cross_send.at[2], cross_recv.at[2])]
    for cross in crosses:
        cross.start()
    fars = [
        Chain(n_ctx, gate_out.at[top], far_land.at[i], far_send.at[i], far_recv.at[i])
        for i, top in enumerate(tops)
    ]
    hops = (11, 19)
    step, steps, drain = line_sum(
        n_head, left_ref, right_ref, work_l, work_r, sum_ref, from_lo, from_hi, sems
    )

    def hop(i):
        crosses[i].wait_recv()
        add_into(gate_out.at[tops[i]], gate_both.at[0, tops[i]], gate_land.at[tops[i]])
        fars[i].start()

    ahead = 3
    for s in range(ahead):
        step(s)
    dp_ref[...] = jnp.zeros_like(dp_ref)
    acc_ref[...] = jnp.zeros_like(acc_ref)
    for h in range(heads):
        cut = slice(h * HEAD_DIM, (h + 1) * HEAD_DIM)
        q_pad[h] = head_lanes(q_ref, h, False)
        g_pad[h] = head_lanes(g_ref, h, True)
        product = g_ref[:, cut].astype(F32) * o_ref[:, cut].astype(F32)
        dl_ref[h] = jnp.sum(product.T, axis=0, keepdims=True)

    def head_tile(h, pairs, start, masked):
        probs = jnp.exp(mat_trans(pairs, q_pad[h]) - lse_ref[h])
        if masked:
            row = block * rows + lax.broadcasted_iota(jnp.int32, (span, rows), 1)
            col = start + lax.broadcasted_iota(jnp.int32, (span, rows), 0)
            probs = jnp.where(col <= row, probs, 0.0)
        grads = (probs * (mat_trans(pairs, g_pad[h]) - dl_ref[h])).astype(BF)
        acc_ref[h] += trans_mat(grads, pairs)
        return matmul(probs.astype(BF), g_pad[h]) + matmul(grads, q_pad[h])

    groups = heads // group

    def two_steps(t):
        for j in range(2):

            @pl.when(ahead + 2 * t + j < steps)
            def _():
                step(ahead + 2 * t + j)

        for i in range(2):

            @pl.when(ahead + 2 * t == hops[i])
            def _():
                hop(i)

    def full(t, carry):
        two_steps(t)
        first = lax.rem(t, groups) * group
        start = pl.multiple_of((t // groups) * span, span)
        cut = pl.ds(start, span)
        total = head_tile(first, p_ref[cut, :], start, False)
        for h in range(1, group):
            total = total + head_tile(first + h, p_ref[cut, :], start, False)
        dp_ref[cut, :] += total
        return carry

    count = block * tiles * groups
    lax.fori_loop(0, count, full, 0)

    def last(t, carry):
        h = lax.rem(2 * t, heads)

        @pl.when(lax.rem(2 * t, group) == 0)
        def _():
            two_steps(count + 2 * t // group)

        start = pl.multiple_of(block * rows + (2 * t // heads) * span, span)
        cut = pl.ds(start, span)
        dp_ref[cut, :] += head_tile(h, p_ref[cut, :], start, True) + head_tile(h + 1, p_ref[cut, :], start, True)
        return carry

    lax.fori_loop(0, heads * tiles // 2, last, 0)
    for h in range(heads):
        dq_ref[:, h * HEAD_DIM : (h + 1) * HEAD_DIM] = acc_ref[h][:, :HEAD_DIM]

    begun = ahead + 2 * (count + groups * tiles)

    def rest(s, carry):
        step(s)

        for i in range(2):

            @pl.when(s == hops[i])
            def _():
                hop(i)

        return carry

    lax.fori_loop(jnp.minimum(begun, steps), steps, rest, 0)
    drain()
    crosses[2].wait_recv()
    add_into(up_out, up_both.at[0], up_land)
    for cross in crosses:
        cross.wait_send()
    for far in fars:
        far.finish()


def attend_back(queries, grads, attended, lse, pair, left, right, parts, n_ctx, n_head, collective_id):
    rows, width = queries.shape
    heads = width // HEAD_DIM
    seq = pair.shape[0]
    group = 4 if heads % 4 == 0 else 2
    span = min(512, rows)
    vmem = pl.BlockSpec(memory_space=pltpu.VMEM)
    flat = jax.ShapeDtypeStruct(parts[0].shape[1:], BF)
    n_far = len(high_bits(n_ctx)) - 1
    cost = pl.CostEstimate(
        flops=32 * rows * seq * width, bytes_accessed=8 * rows * width, transcendentals=0
    )
    return pl.pallas_call(
        functools.partial(backward_kernel, n_ctx, n_head, group, span),
        out_shape=(
            jax.ShapeDtypeStruct((rows, width), F32),
            jax.ShapeDtypeStruct((seq, 2 * HEAD_DIM), F32),
            jax.ShapeDtypeStruct((rows, 2 * left.shape[1]), BF),
            flat,
            flat,
        ),
        in_specs=[vmem] * 9,
        out_specs=(vmem,) * 5,
        scratch_shapes=[
            pltpu.VMEM((heads, rows, 128), BF),
            pltpu.VMEM((heads, rows, 128), BF),
            pltpu.VMEM((heads, rows, 128), F32),
            pltpu.VMEM((heads, 1, rows), F32),
            pltpu.VMEM(flat.shape, BF),
            pltpu.VMEM(flat.shape, BF),
            pltpu.VMEM((2, n_far, flat.shape[0] // 2, flat.shape[1]), BF),
            pltpu.SemaphoreType.DMA((3,)),
            pltpu.SemaphoreType.DMA((3,)),
            pltpu.SemaphoreType.DMA((2, n_far)),
            pltpu.SemaphoreType.DMA((2, n_far)),
        ]
        + line_scratch(rows, 2 * left.shape[1]),
        compiler_params=pltpu.CompilerParams(collective_id=collective_id, has_side_effects=True),
        cost_estimate=cost,
        name="attend_backward",
    )(queries, grads, attended, lse, pair, left, right, *parts)


def partners(n_ctx):
    return [("fsdp", 1)] + [("ctx", bit) for bit in high_bits(n_ctx)]


def greet(n_ctx):
    barrier = pltpu.get_barrier_semaphore()
    for axis, bit in partners(n_ctx):
        pl.semaphore_signal(
            barrier, inc=1, device_id={axis: lax.axis_index(axis) ^ bit}, device_id_type=MESH
        )
    return barrier


def masks_of(bits):
    masks = [0]
    for bit in bits:
        masks = masks + [m | bit for m in masks]
    return masks


def gather_pairs(n_ctx, rows, all_ref, send, recv):
    x = lax.axis_index("fsdp")
    ctx = lax.axis_index("ctx")
    copies = []

    def part(start, size, axis, bit):
        e = len(copies)
        cut = all_ref.at[pl.ds(pl.multiple_of(start, rows), size)]
        copy = pltpu.make_async_remote_copy(
            src_ref=cut,
            dst_ref=cut,
            send_sem=send.at[e],
            recv_sem=recv.at[e],
            device_id={axis: lax.axis_index(axis) ^ bit},
            device_id_type=MESH,
        )
        copy.start()
        copies.append(copy)
        return copy

    opening = part((ctx * 2 + x) * rows, rows, "fsdp", 1)

    def finish():
        opening.wait_recv()
        done = []
        for bit in high_bits(n_ctx):
            now = [part((ctx ^ m) * 2 * rows, 2 * rows, "ctx", bit) for m in masks_of(done)]
            for copy in now:
                copy.wait_recv()
            done.append(bit)
        for copy in copies:
            copy.wait_send()

    return finish


def project_kernel(
    n_ctx,
    x_ref,
    w_ref,
    gain_ref,
    cos_ref,
    sin_ref,
    wo_ref,
    down_ref,
    q_ref,
    p_ref,
    n_ref,
    w_other,
    gain_other,
    wo_other,
    down_other,
    acc_ref,
    send,
    recv,
    relay_send,
    relay_recv,
    gain_send,
    gain_recv,
):
    rows, width = x_ref.shape
    half = width // 2
    q_width = q_ref.shape[1]
    x_at = lax.axis_index("fsdp")
    block = lax.axis_index("ctx") * 2 + x_at
    barrier = greet(n_ctx)
    pl.semaphore_wait(barrier, len(partners(n_ctx)))
    gains = pltpu.make_async_remote_copy(
        src_ref=gain_ref,
        dst_ref=gain_other,
        send_sem=gain_send,
        recv_sem=gain_recv,
        device_id={"fsdp": 1 - x_at},
        device_id_type=MESH,
    )
    gains.start()
    part = half // 2
    first = [
        Relay(
            n_ctx,
            w_ref.at[pl.ds(i * part, part)],
            w_other.at[pl.ds(i * part, part)],
            relay_send.at[i],
            relay_recv.at[i],
        )
        for i in range(2)
    ]
    second = Relay(n_ctx, wo_ref, wo_other, relay_send.at[2], relay_recv.at[2])
    third = Relay(n_ctx, down_ref, down_other, relay_send.at[3], relay_recv.at[3])
    for relay in first:
        relay.start()
    second.start()
    gains.wait_recv()
    parts = 8
    size = rows // parts
    own = pl.ds(pl.multiple_of(x_at * half, half), half)
    other = pl.ds(pl.multiple_of((1 - x_at) * half, half), half)

    def cut_of(i):
        return pl.ds(pl.multiple_of(i * size, size), size)

    def norm(i, carry):
        cut = cut_of(i)
        left = x_ref[cut, own].astype(F32)
        right = x_ref[cut, other].astype(F32)
        total = jnp.sum(left * left, axis=1, keepdims=True) + jnp.sum(right * right, axis=1, keepdims=True)
        scale = lax.rsqrt(total / width + EPSILON)
        n_ref[cut, :half] = (left * scale * gain_ref[0:1, :]).astype(BF)
        n_ref[cut, half:] = (right * scale * gain_other[0:1, :]).astype(BF)
        return carry

    lax.fori_loop(0, parts, norm, 0)
    for relay in first:
        relay.hop(0)
    second.hop(0)

    def local(i, carry):
        cut = cut_of(i)
        acc_ref[cut, :] = matmul(n_ref[cut, :half], w_ref[...])
        return carry

    lax.fori_loop(0, parts, local, 0)
    for j in range(1, len(high_bits(n_ctx))):
        for relay in first:
            relay.hop(j)
    for relay in first:
        relay.landed()

    def rotated(wide, cut):
        low = lax.rem(lanes(wide.shape), HEAD_DIM) < HEAD_DIM // 2
        turned = jnp.where(low, pltpu.roll(wide, 128 - HEAD_DIM // 2, 1), pltpu.roll(wide, HEAD_DIM // 2, 1))
        return wide * cos_ref[cut, :] + turned * sin_ref[cut, :]

    def pairs(i, carry):
        cut = cut_of(i)
        both = acc_ref[cut, q_width:] + matmul(n_ref[cut, half:], w_other[:, q_width:])
        pair = jnp.where(lanes(both.shape) < HEAD_DIM, rotated(both, cut), both)
        p_ref[pl.ds(pl.multiple_of(block * rows + i * size, size), size), :] = pair.astype(BF)
        return carry

    def queries(i, carry):
        cut = cut_of(i)
        whole = acc_ref[cut, :q_width] + matmul(n_ref[cut, half:], w_other[:, :q_width])
        for j in range(q_width // 128):
            sl = slice(j * 128, (j + 1) * 128)
            q_ref[cut, sl] = (rotated(whole[:, sl], cut) * 0.125).astype(BF)
        return carry

    lax.fori_loop(0, parts, pairs, 0)
    finish = gather_pairs(n_ctx, rows, p_ref, send, recv)
    third.start()
    lax.fori_loop(0, parts, queries, 0)
    finish()
    for j in range(1, len(high_bits(n_ctx))):
        second.hop(j)
    second.landed()
    third.landed(0)
    for relay in first + [second]:
        relay.drain()
    third.drain(slice(0, 1))
    gains.wait_send()


def project(inputs, w_local, gains, cosine, sine, w_out, w_down, q_width, n_ctx, collective_id):
    rows, width = inputs.shape
    vmem = pl.BlockSpec(memory_space=pltpu.VMEM)
    anywhere = pl.BlockSpec(memory_space=pl.ANY)
    return pl.pallas_call(
        functools.partial(project_kernel, n_ctx),
        out_shape=(
            jax.ShapeDtypeStruct((rows, q_width), BF),
            jax.ShapeDtypeStruct((rows * 2 * n_ctx, 2 * HEAD_DIM), BF),
            jax.ShapeDtypeStruct((rows, width), BF),
            jax.ShapeDtypeStruct(w_local.shape, BF),
            jax.ShapeDtypeStruct(gains.shape, F32),
            jax.ShapeDtypeStruct(w_out.shape, BF),
            jax.ShapeDtypeStruct(w_down.shape, BF),
        ),
        in_specs=[vmem] * 5 + [anywhere] * 2,
        out_specs=(vmem,) * 5 + (anywhere,) * 2,
        scratch_shapes=[
            pltpu.VMEM((rows, w_local.shape[1]), F32),
            pltpu.SemaphoreType.DMA((n_ctx,)),
            pltpu.SemaphoreType.DMA((n_ctx,)),
            pltpu.SemaphoreType.DMA((4, n_ctx)),
            pltpu.SemaphoreType.DMA((4, n_ctx)),
            pltpu.SemaphoreType.DMA,
            pltpu.SemaphoreType.DMA,
        ],
        compiler_params=pltpu.CompilerParams(collective_id=collective_id, has_side_effects=True),
        name="project",
    )(inputs, w_local, gains, cosine, sine, w_out, w_down)


def line_sum(n, left, right, work_l, work_r, o_ref, from_lo, from_hi, sems, lag=LAG):
    s_up, r_up, s_dn, r_dn, s_a, r_a, s_b, r_b = sems
    me = lax.axis_index("head")
    rows, cols = left.shape
    size = rows // CHUNKS
    has_lo = me > 0
    has_hi = me < n - 1
    middle = jnp.logical_and(has_lo, has_hi)

    def at(k):
        return pl.ds(pl.multiple_of(k * size, size), size)

    def remote(src, dst, send, recv, target):
        return pltpu.make_async_remote_copy(
            src_ref=src,
            dst_ref=dst,
            send_sem=send,
            recv_sem=recv,
            device_id={"head": target},
            device_id_type=MESH,
        )

    def up(k, src):
        return remote(src.at[at(k)], from_lo.at[at(k)], s_up.at[k], r_up.at[k], me + 1)

    def down(k, src):
        return remote(src.at[at(k)], from_hi.at[at(k)], s_dn.at[k], r_dn.at[k], me - 1)

    def spread_a(k):
        part = o_ref.at[at(k), pl.ds(0, cols)]
        return remote(part, part, s_a.at[k], r_a.at[k], me + 1)

    def spread_b(k):
        part = o_ref.at[at(k), pl.ds(cols, cols)]
        return remote(part, part, s_b.at[k], r_b.at[k], me - 1)

    def valid(k):
        return jnp.logical_and(k >= 0, k < CHUNKS)

    def added(mine, there, k):
        return (mine[at(k), :].astype(F32) + there[at(k), :].astype(F32)).astype(BF)

    def step(s):
        k1 = s - lag * me
        k2 = s - lag * (n - 1 - me)
        k3 = s - lag * (n - 1 + me)
        k4 = s - lag * (2 * (n - 1) - me)

        @pl.when(jnp.logical_and(valid(k1), me == 0))
        def _():
            up(k1, right).start()

        @pl.when(jnp.logical_and(valid(k2), me == n - 1))
        def _():
            down(k2, left).start()

        @pl.when(jnp.logical_and(valid(k1), middle))
        def _():
            up(k1, right).wait_recv()
            work_r[at(k1), :] = added(right, from_lo, k1)
            up(k1, work_r).start()

        @pl.when(jnp.logical_and(valid(k1), me == n - 1))
        def _():
            up(k1, right).wait_recv()
            o_ref[at(k1), cols:] = added(right, from_lo, k1)
            spread_b(k1).start()

        @pl.when(jnp.logical_and(valid(k2), middle))
        def _():
            down(k2, left).wait_recv()
            work_l[at(k2), :] = added(left, from_hi, k2)
            down(k2, work_l).start()

        @pl.when(jnp.logical_and(valid(k2), me == 0))
        def _():
            down(k2, left).wait_recv()
            o_ref[at(k2), :cols] = added(left, from_hi, k2)
            spread_a(k2).start()

        @pl.when(jnp.logical_and(valid(k3), has_lo))
        def _():
            spread_a(k3).wait_recv()

            @pl.when(has_hi)
            def _():
                spread_a(k3).start()

        @pl.when(jnp.logical_and(valid(k4), has_hi))
        def _():
            spread_b(k4).wait_recv()

            @pl.when(has_lo)
            def _():
                spread_b(k4).start()

    def drain():
        def one(k, carry):
            @pl.when(has_hi)
            def _():
                up(k, right).wait_send()
                spread_a(k).wait_send()

            @pl.when(has_lo)
            def _():
                down(k, left).wait_send()
                spread_b(k).wait_send()

            return carry

        lax.fori_loop(0, CHUNKS, one, 0)

    return step, CHUNKS + 2 * lag * (n - 1), drain


def line_greet(n):
    me = lax.axis_index("head")
    barrier = pltpu.get_barrier_semaphore()

    @pl.when(me > 0)
    def _():
        pl.semaphore_signal(barrier, inc=1, device_id={"head": me - 1}, device_id_type=MESH)

    @pl.when(me < n - 1)
    def _():
        pl.semaphore_signal(barrier, inc=1, device_id={"head": me + 1}, device_id_type=MESH)

    return barrier


def line_peers(n):
    me = lax.axis_index("head")
    return jnp.where(me > 0, 1, 0) + jnp.where(me < n - 1, 1, 0)


def line_scratch(rows, width):
    return [pltpu.VMEM((rows, width // 2), BF)] * 4 + [pltpu.SemaphoreType.DMA((CHUNKS,))] * 8


def last_kernel(
    n_ctx,
    n_head,
    dq_ref,
    part_ref,
    cos_ref,
    sin_ref,
    w_l,
    w_r,
    n_ref,
    att_ref,
    low_ref,
    up_ref,
    gate_ref,
    down_ref,
    sum_ref,
    qkv_full,
    out_full,
    gate_full,
    up_full,
    down_full,
    work,
    land,
    raw,
    raw_land,
    n_land,
    low_land,
    att_land,
    up_sum,
    out_sent,
    out_kept,
    out_land,
    qkv_sent,
    qkv_kept,
    qkv_land,
    up_far,
    out_far,
    qkv_far,
    pair_send,
    pair_recv,
    trade_send,
    trade_recv,
    cross_send,
    cross_recv,
    far_send,
    far_recv,
    full_send,
    full_recv,
    full_local,
    left,
    right,
    from_lo,
    from_hi,
    *sems,
):
    rows, q_width = dq_ref.shape
    half = n_ref.shape[1] // 2
    quarter = half // 2
    x_at = lax.axis_index("fsdp")
    ctx = lax.axis_index("ctx")
    core = lax.rem(ctx, 2)
    barrier = line_greet(n_head)
    greet(n_ctx)
    work[...] = part_ref[...].astype(BF)
    up_sum[...] = up_ref[...]
    pl.semaphore_wait(barrier, line_peers(n_head) + len(partners(n_ctx)))

    def relative(side, c):
        return pl.ds(pl.multiple_of(side * half + c * quarter, quarter), quarter)

    def trade(src, dst, at):
        return exchange(src, dst, "ctx", 1, trade_send.at[at], trade_recv.at[at])

    pairs = []
    used = [0]

    def give(start, size, axis, bit):
        e = len(pairs)
        cut = pl.ds(pl.multiple_of(start, rows), size)
        copy = exchange(
            work.at[cut], land.at[pl.ds(used[0], size)], axis, bit, pair_send.at[e], pair_recv.at[e]
        )
        copy.start()
        pairs.append(copy)
        used[0] += size
        return copy, used[0] - size

    def take(start, size, at):
        cut = pl.ds(pl.multiple_of(start, rows), size)
        work[cut, :] = (work[cut, :].astype(F32) + land[at : at + size, :].astype(F32)).astype(BF)

    up_chain = Chain(n_ctx, up_sum, up_far, far_send.at[0], far_recv.at[0])
    out_chain = Chain(n_ctx, out_kept, out_far, far_send.at[1], far_recv.at[1])
    qkv_chain = Chain(n_ctx, qkv_kept, qkv_far, far_send.at[2], far_recv.at[2])

    def turned(wide, cut):
        low = lax.rem(lanes(wide.shape), HEAD_DIM) < HEAD_DIM // 2
        swapped = jnp.where(low, pltpu.roll(wide, 128 - HEAD_DIM // 2, 1), pltpu.roll(wide, HEAD_DIM // 2, 1))
        return wide * cos_ref[cut, :] - swapped * sin_ref[cut, :]

    def rotate_rows(i, carry):
        cut = pl.ds(pl.multiple_of(i * 128, 128), 128)
        for j in range(q_width // 128):
            sl = slice(j * 128, (j + 1) * 128)
            raw[cut, sl] = turned(dq_ref[cut, sl] * 0.125, cut).astype(BF)
        return carry

    trades = [trade(att_ref, att_land, 0)]
    for side in range(2):
        landing = pl.ds(side * quarter, quarter)
        trades.append(trade(low_ref.at[:, relative(side, 1 - core)], low_land.at[:, landing], 1 + side))
    late = []
    for side in range(2):
        landing = pl.ds(side * quarter, quarter)
        late.append(trade(n_ref.at[:, relative(side, 1 - core)], n_land.at[:, landing], 3 + side))

    def out_tiles(dst, side):
        def one(t, carry):
            cut = pl.ds(pl.multiple_of(t * 128, 128), 128)
            dst[cut, :] = (
                trans_mat(att_ref[:, cut], low_ref[:, relative(side, core)])
                + trans_mat(att_land[:, cut], low_land[:, side * quarter : (side + 1) * quarter])
            ).astype(BF)
            return carry

        lax.fori_loop(0, q_width // 128, one, 0)

    bits = high_bits(n_ctx)
    for j in range(len(bits)):
        bit = bits[len(bits) - 1 - j]
        masks = masks_of(bits[: len(bits) - 1 - j])
        now = [give((ctx ^ bit ^ m) * 2 * rows, 2 * rows, "ctx", bit) for m in masks]
        if j == 0:
            for t in trades + late:
                t.start()
            lax.fori_loop(0, rows // 128, rotate_rows, 0)
        if j == 1:
            for t in trades:
                t.wait_recv()
            out_tiles(out_sent, 1)
        for (copy, at), m in zip(now, masks):
            copy.wait_recv()
            take((ctx ^ m) * 2 * rows, 2 * rows, at)
    copy, at = give((ctx * 2 + 1 - x_at) * rows, rows, "fsdp", 1)
    out_cross = exchange(out_sent, out_land, "fsdp", 1, cross_send.at[0], cross_recv.at[0])
    out_cross.start()
    up_chain.start()
    out_tiles(out_kept, 0)
    copy.wait_recv()
    base = pl.multiple_of((ctx * 2 + x_at) * rows, rows)

    def finish_pair(i, carry):
        cut = pl.ds(pl.multiple_of(i * 128, 128), 128)
        mine = work[pl.ds(base + i * 128, 128), :].astype(F32) + land[pl.ds(at + i * 128, 128), :].astype(F32)
        raw[cut, q_width:] = jnp.where(lanes(mine.shape) < HEAD_DIM, turned(mine, cut), mine).astype(BF)
        left[cut, :] = mat_trans(raw[cut, :], w_l[...]).astype(BF)
        right[cut, :] = mat_trans(raw[cut, :], w_r[...]).astype(BF)
        return carry

    lax.fori_loop(0, rows // 128, finish_pair, 0)
    raw_trade = trade(raw, raw_land, 5)
    raw_trade.start()
    late.append(raw_trade)
    step, steps, drain = line_sum(n_head, left, right, left, right, sum_ref, from_lo, from_hi, sems)

    def run(s, carry):
        step(s)
        return carry

    def spread(src, whole, by_rows, e):
        size = src.shape[0 if by_rows else 1]
        cut = pl.ds(pl.multiple_of(core * size, size), size)
        dst = whole.at[cut] if by_rows else whole.at[:, cut]
        return (
            pltpu.make_async_copy(src, dst, full_local.at[e]),
            exchange(src, dst, "ctx", 1, full_send.at[e], full_recv.at[e]),
        )

    spreads = [spread(gate_ref, gate_full, True, 0), spread(down_ref, down_full, False, 1)]
    for pair in spreads:
        for copy in pair:
            copy.start()

    def qkv_tiles(dst, side):
        def one(t, carry):
            cut = pl.ds(pl.multiple_of(t * 128, 128), 128)
            there = pl.ds(pl.multiple_of(side * half + core * quarter + t * 128, 128), 128)
            landing = pl.ds(pl.multiple_of(side * quarter + t * 128, 128), 128)
            dst[cut, :] = (
                trans_mat(n_ref[:, there], raw[...]) + trans_mat(n_land[:, landing], raw_land[...])
            ).astype(BF)
            step(steps_at + t)
            return carry

        lax.fori_loop(0, quarter // 128, one, 0)

    lax.fori_loop(0, 2, run, 0)
    for t in late:
        t.wait_recv()
    steps_at = 2
    qkv_tiles(qkv_sent, 1)
    qkv_cross = exchange(qkv_sent, qkv_land, "fsdp", 1, cross_send.at[1], cross_recv.at[1])
    qkv_cross.start()
    steps_at += quarter // 128
    qkv_tiles(qkv_kept, 0)
    steps_at += quarter // 128
    out_cross.wait_recv()
    add_into(out_kept, out_kept, out_land)
    out_chain.start()
    rest = steps - steps_at
    stops = [steps_at + (rest * i) // 8 for i in range(9)]
    lax.fori_loop(stops[0], stops[2], run, 0)
    qkv_cross.wait_recv()
    add_into(qkv_kept, qkv_kept, qkv_land)
    qkv_chain.start()
    lax.fori_loop(stops[2], stops[4], run, 0)
    up_chain.finish()
    spreads.append(spread(up_sum, up_full, True, 2))
    for copy in spreads[-1]:
        copy.start()
    lax.fori_loop(stops[4], stops[6], run, 0)
    out_chain.finish()
    spreads.append(spread(out_kept, out_full, False, 3))
    for copy in spreads[-1]:
        copy.start()
    lax.fori_loop(stops[6], stops[8], run, 0)
    qkv_chain.finish()
    spreads.append(spread(qkv_kept, qkv_full, True, 4))
    for copy in spreads[-1]:
        copy.start()
    drain()
    for t in pairs + trades + late + [out_cross, qkv_cross]:
        t.wait_send()
    for local, remote in spreads:
        local.wait()
        remote.wait()


def last_sum(
    dq, part, cosine, sine, w_left, w_right, normed, attended, low, up, gate, down, n_ctx, n_head, collective_id
):
    rows, q_width = dq.shape
    width = normed.shape[1]
    half = width // 2
    quarter = half // 2
    narrow = w_left.shape[1]
    units = gate.shape[1]
    n_far = len(high_bits(n_ctx)) - 1
    vmem = pl.BlockSpec(memory_space=pltpu.VMEM)
    anywhere = pl.BlockSpec(memory_space=pl.ANY)
    dma = pltpu.SemaphoreType.DMA
    return pl.pallas_call(
        functools.partial(last_kernel, n_ctx, n_head),
        out_shape=(
            jax.ShapeDtypeStruct((rows, width), BF),
            jax.ShapeDtypeStruct((half, narrow), BF),
            jax.ShapeDtypeStruct((q_width, half), BF),
            jax.ShapeDtypeStruct((half, units), BF),
            jax.ShapeDtypeStruct((half, units), BF),
            jax.ShapeDtypeStruct((units, half), BF),
        ),
        in_specs=[vmem] * 12,
        out_specs=(vmem,) + (anywhere,) * 5,
        scratch_shapes=[
            pltpu.VMEM(part.shape, BF),
            pltpu.VMEM(part.shape, BF),
            pltpu.VMEM((rows, narrow), BF),
            pltpu.VMEM((rows, narrow), BF),
            pltpu.VMEM((rows, half), BF),
            pltpu.VMEM((rows, half), BF),
            pltpu.VMEM((rows, q_width), BF),
            pltpu.VMEM(up.shape, BF),
            pltpu.VMEM((q_width, quarter), BF),
            pltpu.VMEM((q_width, quarter), BF),
            pltpu.VMEM((q_width, quarter), BF),
            pltpu.VMEM((quarter, narrow), BF),
            pltpu.VMEM((quarter, narrow), BF),
            pltpu.VMEM((quarter, narrow), BF),
            pltpu.VMEM((n_far,) + up.shape, BF),
            pltpu.VMEM((n_far, q_width, quarter), BF),
            pltpu.VMEM((n_far, quarter, narrow), BF),
            dma((n_ctx,)),
            dma((n_ctx,)),
            dma((6,)),
            dma((6,)),
            dma((2,)),
            dma((2,)),
            dma((3, n_far)),
            dma((3, n_far)),
            dma((5,)),
            dma((5,)),
            dma((5,)),
        ]
        + line_scratch(rows, width),
        compiler_params=pltpu.CompilerParams(
            collective_id=collective_id, has_side_effects=True, vmem_limit_bytes=66_000_000
        ),
        cost_estimate=pl.CostEstimate(
            flops=50_000_000_000, bytes_accessed=8 * rows * width, transcendentals=0
        ),
        name="last_sum",
    )(dq, part, cosine, sine, w_left, w_right, normed, attended, low, up, gate, down)


def ffn_kernel(
    n_head,
    x_ref,
    mix_ref,
    cot_ref,
    gain_ref,
    gain_other,
    gate_l_hbm,
    gate_r_hbm,
    up_l_hbm,
    up_r_hbm,
    down_l_hbm,
    down_r_hbm,
    sum_ref,
    ffn_left,
    ffn_right,
    down_kept,
    gate_both,
    up_both,
    gate_l,
    gate_r,
    up_l,
    up_r,
    down_l,
    down_r,
    load_sem,
    n_ref,
    act_ref,
    gig_ref,
    uig_ref,
    cot_land,
    n_land,
    act_land,
    gig_land,
    uig_land,
    down_sent,
    down_land,
    out_tile,
    out_sem,
    trade_send,
    trade_recv,
    cross_send,
    cross_recv,
    left,
    right,
    from_lo,
    from_hi,
    *sems,
):
    rows, width = x_ref.shape
    half = width // 2
    quarter = half // 2
    units = act_ref.shape[1]
    x_at = lax.axis_index("fsdp")
    ctx_at = lax.axis_index("ctx")
    core = lax.rem(ctx_at, 2)
    own = pl.ds(pl.multiple_of(x_at * half, half), half)
    other = pl.ds(pl.multiple_of((1 - x_at) * half, half), half)
    barrier = line_greet(n_head)
    pl.semaphore_signal(barrier, inc=1, device_id={"fsdp": 1 - x_at}, device_id_type=MESH)
    pl.semaphore_signal(barrier, inc=1, device_id={"ctx": ctx_at ^ 1}, device_id_type=MESH)
    loads = [
        pltpu.make_async_copy(src, dst, load_sem.at[i])
        for i, (src, dst) in enumerate(
            (
                (gate_l_hbm, gate_l),
                (gate_r_hbm, gate_r),
                (up_l_hbm, up_l),
                (up_r_hbm, up_r),
                (down_l_hbm, down_l),
                (down_r_hbm, down_r),
            )
        )
    ]
    for load in loads:
        load.start()
    pl.semaphore_wait(barrier, line_peers(n_head) + 2)

    def trade(src, dst, at):
        return pltpu.make_async_remote_copy(
            src_ref=src,
            dst_ref=dst,
            send_sem=trade_send.at[at],
            recv_sem=trade_recv.at[at],
            device_id={"ctx": ctx_at ^ 1},
            device_id_type=MESH,
        )

    def absolute(side, c):
        start = (x_at if side == 0 else 1 - x_at) * half + c * quarter
        return pl.ds(pl.multiple_of(start, quarter), quarter)

    def relative(side, c):
        return pl.ds(pl.multiple_of(side * half + c * quarter, quarter), quarter)

    cot_trades = [
        trade(cot_ref.at[:, absolute(j, 1 - core)], cot_land.at[:, pl.ds(j * quarter, quarter)], j)
        for j in range(2)
    ]
    for copy in cot_trades:
        copy.start()

    def row_trades(g):
        mine = pl.ds(pl.multiple_of(g * (rows // FFN_GROUPS), rows // FFN_GROUPS), rows // FFN_GROUPS)
        at = 2 + g * 5
        return [
            trade(act_ref.at[mine], act_land.at[mine], at),
            trade(gig_ref.at[mine], gig_land.at[mine], at + 1),
            trade(uig_ref.at[mine], uig_land.at[mine], at + 2),
            trade(n_ref.at[mine, relative(0, 1 - core)], n_land.at[mine, pl.ds(0, quarter)], at + 3),
            trade(n_ref.at[mine, relative(1, 1 - core)], n_land.at[mine, pl.ds(quarter, quarter)], at + 4),
        ]

    step, steps, drain = line_sum(n_head, left, right, left, right, sum_ref, from_lo, from_hi, sems)

    def run(s, carry):
        step(s)
        return carry

    size = rows // FFN_GROUPS
    per_group = CHUNKS // FFN_GROUPS

    def one_group(g, carry):
        mine = pl.ds(pl.multiple_of(g * size, size), size)
        base = (g - 1) * per_group
        stops = [base + (per_group * i) // 4 for i in range(5)]
        hid_l = x_ref[mine, own].astype(F32) + mix_ref[mine, :half].astype(F32)
        hid_r = x_ref[mine, other].astype(F32) + mix_ref[mine, half:].astype(F32)
        total = jnp.sum(hid_l * hid_l, axis=1, keepdims=True) + jnp.sum(hid_r * hid_r, axis=1, keepdims=True)
        scale = lax.rsqrt(total / width + EPSILON)
        n_ref[mine, :half] = (hid_l * scale * gain_ref[1:2, :]).astype(BF)
        n_ref[mine, half:] = (hid_r * scale * gain_other[1:2, :]).astype(BF)
        lax.fori_loop(stops[0], stops[1], run, 0)

        @pl.when(g == 0)
        def _():
            for load in loads[:4]:
                load.wait()

        gate = matmul(n_ref[mine, :half], gate_l[...]) + matmul(n_ref[mine, half:], gate_r[...])
        up = matmul(n_ref[mine, :half], up_l[...]) + matmul(n_ref[mine, half:], up_r[...])
        lax.fori_loop(stops[1], stops[2], run, 0)
        sigma = jax.nn.sigmoid(gate)
        silu = gate * sigma
        act_ref[mine, :] = (silu * up).astype(BF)

        @pl.when(g == 0)
        def _():
            for load in loads[4:]:
                load.wait()

        grad = mat_trans(cot_ref[mine, own], down_l[...]) + mat_trans(cot_ref[mine, other], down_r[...])
        gig_ref[mine, :] = (grad * up * sigma * (1.0 + gate * (1.0 - sigma))).astype(BF)
        uig_ref[mine, :] = (grad * silu).astype(BF)
        lax.fori_loop(stops[2], stops[3], run, 0)
        gig = gig_ref[mine, :]
        uig = uig_ref[mine, :]
        left[mine, :] = (mat_trans(gig, gate_l[...]) + mat_trans(uig, up_l[...])).astype(BF)
        lax.fori_loop(stops[3], stops[4], run, 0)
        right[mine, :] = (mat_trans(gig, gate_r[...]) + mat_trans(uig, up_r[...])).astype(BF)
        for copy in row_trades(g):
            copy.start()
        return carry

    lax.fori_loop(0, FFN_GROUPS, one_group, 0)
    first = CHUNKS - per_group
    rest = steps - first
    tile = 128
    down_tiles = units // tile
    row_tiles = quarter // tile
    total_work = down_tiles + 4 * row_tiles + 2 * FFN_GROUPS

    def sums(i, weight=1):
        lax.fori_loop(
            first + (rest * i) // total_work, first + (rest * (i + weight)) // total_work, run, 0
        )

    for copy in cot_trades:
        copy.wait_recv()

    def landed(g, carry):
        for copy in row_trades(g):
            copy.wait_recv()
        return carry

    lax.fori_loop(0, FFN_GROUPS, landed, 0)

    def down_tile(t, carry):
        sums(t)
        cut = pl.ds(pl.multiple_of(t * tile, tile), tile)
        mine = act_ref[:, cut]
        theirs = act_land[:, cut]
        for dst, side in ((down_sent, 1), (down_kept, 0)):
            dst[cut, :] = (
                trans_mat(mine, cot_ref[:, absolute(side, core)])
                + trans_mat(theirs, cot_land[:, side * quarter : (side + 1) * quarter])
            ).astype(BF)
        return carry

    lax.fori_loop(0, down_tiles, down_tile, 0)
    cross = pltpu.make_async_remote_copy(
        src_ref=down_sent,
        dst_ref=down_land,
        send_sem=cross_send,
        recv_sem=cross_recv,
        device_id={"fsdp": 1 - x_at},
        device_id_type=MESH,
    )
    cross.start()
    done = down_tiles

    def out_copy(dst, t, slot):
        cut = pl.ds(pl.multiple_of(lax.rem(t, row_tiles) * tile, tile), tile)
        return pltpu.make_async_copy(out_tile.at[slot], dst.at[1 - t // row_tiles, cut], out_sem.at[slot])

    for dst, own_grad, their_grad in ((gate_both, gig_ref, gig_land), (up_both, uig_ref, uig_land)):

        def row_tile(t, carry):
            sums(done + t)
            slot = lax.rem(t, 2)
            side = 1 - t // row_tiles
            row = lax.rem(t, row_tiles) * tile
            there = pl.ds(pl.multiple_of(side * half + core * quarter + row, tile), tile)
            landing = pl.ds(pl.multiple_of(side * quarter + row, tile), tile)
            value = (
                trans_mat(n_ref[:, there], own_grad[...]) + trans_mat(n_land[:, landing], their_grad[...])
            ).astype(BF)

            @pl.when(t >= 2)
            def _():
                out_copy(dst, t - 2, slot).wait()

            out_tile[slot] = value
            out_copy(dst, t, slot).start()
            return carry

        lax.fori_loop(0, 2 * row_tiles, row_tile, 0)
        for t in range(2 * row_tiles - 2, 2 * row_tiles):
            out_copy(dst, t, t % 2).wait()
        done += 2 * row_tiles

    def project_down(g, carry):
        mine = pl.ds(pl.multiple_of(g * size, size), size)
        sums(done + 2 * g, 2)
        ffn_left[mine, :] = matmul(act_ref[mine, :], down_l[...]).astype(BF)
        ffn_right[mine, :] = matmul(act_ref[mine, :], down_r[...]).astype(BF)
        return carry

    lax.fori_loop(0, FFN_GROUPS, project_down, 0)
    cross.wait_recv()

    def finish(t, carry):
        cut = pl.ds(pl.multiple_of(t * tile, tile), tile)
        down_kept[cut, :] = (down_kept[cut, :].astype(F32) + down_land[cut, :].astype(F32)).astype(BF)
        return carry

    lax.fori_loop(0, down_tiles, finish, 0)
    cross.wait_send()
    for copy in cot_trades:
        copy.wait_send()

    def sent(g, carry):
        for copy in row_trades(g):
            copy.wait_send()
        return carry

    lax.fori_loop(0, FFN_GROUPS, sent, 0)
    drain()


def ffn_sum(inputs, mixed, cot, gains, gains_other, gate, gate_o, up, up_o, down, down_o, n_head, collective_id):
    rows, width = inputs.shape
    units = gate.shape[1]
    vmem = pl.BlockSpec(memory_space=pltpu.VMEM)
    wide = jax.ShapeDtypeStruct((rows, width), BF)
    narrow = jax.ShapeDtypeStruct((rows, width // 2), BF)
    quarter = width // 4
    flat = jax.ShapeDtypeStruct((2, quarter, units), BF)
    anywhere = pl.BlockSpec(memory_space=pl.ANY)
    trades = 2 + 5 * FFN_GROUPS
    return pl.pallas_call(
        functools.partial(ffn_kernel, n_head),
        out_shape=(wide, narrow, narrow, jax.ShapeDtypeStruct((units, quarter), BF), flat, flat),
        in_specs=[vmem] * 5 + [anywhere] * 6,
        out_specs=(vmem,) * 4 + (anywhere,) * 2,
        scratch_shapes=[pltpu.VMEM(w.shape, BF) for w in (gate, gate, up, up, down, down)]
        + [pltpu.SemaphoreType.DMA((6,)), pltpu.VMEM((rows, width), BF)]
        + [pltpu.VMEM((rows, units), BF)] * 3
        + [pltpu.VMEM((rows, width // 2), BF)] * 2
        + [pltpu.VMEM((rows, units), BF)] * 3
        + [pltpu.VMEM((units, quarter), BF)] * 2
        + [
            pltpu.VMEM((2, 128, units), BF),
            pltpu.SemaphoreType.DMA((2,)),
            pltpu.SemaphoreType.DMA((trades,)),
            pltpu.SemaphoreType.DMA((trades,)),
            pltpu.SemaphoreType.DMA,
            pltpu.SemaphoreType.DMA,
        ]
        + line_scratch(rows, width),
        compiler_params=pltpu.CompilerParams(
            collective_id=collective_id, has_side_effects=True, vmem_limit_bytes=66_000_000
        ),
        cost_estimate=pl.CostEstimate(
            flops=50_000_000_000, bytes_accessed=8 * rows * width, transcendentals=0
        ),
        name="ffn_sum",
    )(inputs, mixed, cot, gains, gains_other, gate, gate_o, up, up_o, down, down_o)


def halves(ref, x_at):
    half = ref.shape[1] // 2
    own = pl.ds(pl.multiple_of(x_at * half, half), half)
    other = pl.ds(pl.multiple_of((1 - x_at) * half, half), half)
    return ref[:, own].astype(F32), ref[:, other].astype(F32)


def norm_back(values, grads, gains, width):
    scale = lax.rsqrt(sum(jnp.sum(v * v, axis=1, keepdims=True) for v in values) / width + EPSILON)
    units = [v * scale for v in values]
    scaled = [g * gain for g, gain in zip(grads, gains)]
    mean = sum(jnp.sum(s * u, axis=1, keepdims=True) for s, u in zip(scaled, units)) / width
    return [scale * (s - u * mean) for s, u in zip(scaled, units)], [g * u for g, u in zip(grads, units)]


def add_gain(gain_ref, products):
    @pl.when(pl.program_id(0) == 0)
    def _():
        gain_ref[...] = jnp.zeros_like(gain_ref)

    half = products[0].shape[1]
    gain_ref[0:1, :half] += jnp.sum(products[0], axis=0, keepdims=True)
    gain_ref[0:1, half:] += jnp.sum(products[1], axis=0, keepdims=True)


def middle_kernel(at_ref, x_ref, mix_ref, grad_ref, cot_ref, gain_ref, other_ref, wl_ref, wr_ref, hid_ref, low_ref, att_ref, part_ref):
    width = x_ref.shape[1]
    half = width // 2
    x_at = at_ref[0]
    x_l, x_r = halves(x_ref, x_at)
    cot_l, cot_r = halves(cot_ref, x_at)
    values = (x_l + mix_ref[:, :half].astype(F32), x_r + mix_ref[:, half:].astype(F32))
    grads = (grad_ref[:, :half].astype(F32), grad_ref[:, half:].astype(F32))
    (d_l, d_r), products = norm_back(values, grads, (gain_ref[1:2, :], other_ref[1:2, :]), width)
    add_gain(part_ref, products)
    hid_l = cot_l + d_l
    hid_r = cot_r + d_r
    hid_ref[:, :half] = hid_l
    hid_ref[:, half:] = hid_r
    low_l = hid_l.astype(BF)
    low_r = hid_r.astype(BF)
    low_ref[:, :half] = low_l
    low_ref[:, half:] = low_r
    att_ref[...] = (mat_trans(low_l, wl_ref[...]) + mat_trans(low_r, wr_ref[...])).astype(BF)


def end_kernel(at_ref, x_ref, mix_ref, ffn_ref, grad_ref, hid_ref, gain_ref, other_ref, out_ref, in_grad_ref, part_ref):
    width = x_ref.shape[1]
    half = width // 2
    x_at = at_ref[0]
    own = pl.ds(pl.multiple_of(x_at * half, half), half)
    other = pl.ds(pl.multiple_of((1 - x_at) * half, half), half)
    x_l, x_r = halves(x_ref, x_at)
    out_ref[:, own] = (x_l + mix_ref[:, :half].astype(F32) + ffn_ref[:, :half].astype(F32)).astype(BF)
    out_ref[:, other] = (x_r + mix_ref[:, half:].astype(F32) + ffn_ref[:, half:].astype(F32)).astype(BF)
    grads = (grad_ref[:, :half].astype(F32), grad_ref[:, half:].astype(F32))
    (d_l, d_r), products = norm_back((x_l, x_r), grads, (gain_ref[0:1, :], other_ref[0:1, :]), width)
    add_gain(part_ref, products)
    in_grad_ref[:, own] = hid_ref[:, :half] + d_l
    in_grad_ref[:, other] = hid_ref[:, half:] + d_r


def by_rows(kernel, x_at, arrays, whole, outs):
    rows, width = arrays[0].shape
    size = min(128, rows)

    def block(shape):
        return pl.BlockSpec((size, shape[1]), lambda i, *_: (i, 0))

    def all_of(shape):
        return pl.BlockSpec(shape, lambda i, *_: (0, 0))

    gain = jax.ShapeDtypeStruct((8, width), F32)
    return pl.pallas_call(
        kernel,
        out_shape=tuple(outs) + (gain,),
        grid_spec=pltpu.PrefetchScalarGridSpec(
            num_scalar_prefetch=1,
            grid=(rows // size,),
            in_specs=[block(a.shape) for a in arrays] + [all_of(a.shape) for a in whole],
            out_specs=[block(o.shape) for o in outs] + [all_of(gain.shape)],
        ),
        cost_estimate=pl.CostEstimate(flops=4_000_000_000, bytes_accessed=24 * rows * width, transcendentals=0),
    )(x_at, *arrays, *whole)


def flip(array, axis, bit, size):
    return lax.ppermute(array, axis, [(i, i ^ bit) for i in range(size)])


def shards(
    n_ctx,
    n_head,
    inputs,
    query_weight,
    key_weight,
    value_weight,
    output_weight,
    gate_weight,
    up_weight,
    down_weight,
    attn_gain,
    ffn_gain,
    cotangent,
):
    rows, width = inputs.shape
    half = width // 2
    x_at = lax.axis_index("fsdp")
    ctx_at = lax.axis_index("ctx")
    core = lax.rem(ctx_at, 2)
    block = ctx_at * 2 + x_at
    block_arr = jnp.reshape(block, (1,)).astype(jnp.int32)

    every = high_bits(n_ctx)

    q_width = query_weight.shape[1]
    half_dim = HEAD_DIM // 2
    positions = block * rows + jnp.arange(rows, dtype=jnp.int32)
    lane = lax.broadcasted_iota(jnp.int32, (rows, 2 * HEAD_DIM), 1)
    freqs = 10000.0 ** (-2.0 * (lane % half_dim).astype(F32) / HEAD_DIM)
    angles = positions.astype(F32)[:, None] * freqs
    cosine = jnp.cos(angles)
    sine = jnp.sin(angles)
    signed = jnp.where(lane % HEAD_DIM < half_dim, -sine, sine)
    qkv_local = jnp.concatenate([query_weight, key_weight, value_weight], axis=1)
    gains_local = jnp.stack([attn_gain.astype(F32), ffn_gain.astype(F32)])
    queries, pair, normed_one, qkv_other, gains_other, out_other, down_begun = project(
        inputs, qkv_local, gains_local, cosine, signed, output_weight, down_weight, q_width, n_ctx, 4
    )
    attended, lse, mixed, gate_other, up_other, down_other = attend_sum(
        queries, pair, output_weight, out_other, gate_weight, up_weight, down_begun, n_ctx, n_head, 1
    )
    low_sum, down_left, down_right, down_kept, gate_both, up_both = ffn_sum(
        inputs,
        mixed,
        cotangent,
        gains_local,
        gains_other,
        gate_weight,
        gate_other,
        up_weight,
        up_other,
        down_weight,
        down_other,
        n_head,
        2,
    )
    x_arr = jnp.reshape(x_at, (1,)).astype(jnp.int32)
    wide = jax.ShapeDtypeStruct((rows, width), F32)
    flat = jax.ShapeDtypeStruct((rows, width), BF)
    hidden_grad, hidden_low, attended_grad, gain_two_part = by_rows(
        middle_kernel,
        x_arr,
        (inputs, mixed, low_sum, cotangent),
        (gains_local, gains_other, output_weight, out_other),
        (wide, flat, jax.ShapeDtypeStruct(attended.shape, BF)),
    )
    down_far = down_kept
    for bit in every[:-1]:
        down_far = (down_far.astype(F32) + flip(down_far, "ctx", bit, n_ctx).astype(F32)).astype(BF)
    query_acc, pair_acc, ffn_out, gate_far, up_crossed = attend_back(
        queries,
        attended_grad,
        attended,
        lse,
        pair,
        down_left,
        down_right,
        (gate_both, up_both),
        n_ctx,
        n_head,
        6,
    )
    last, qkv_full, out_full, gate_full, up_full, down_full = last_sum(
        query_acc,
        pair_acc,
        cosine,
        signed,
        qkv_local,
        qkv_other,
        normed_one,
        attended,
        hidden_low,
        up_crossed,
        gate_far,
        down_far,
        n_ctx,
        n_head,
        3,
    )
    outputs, input_grad, gain_one_part = by_rows(
        end_kernel, x_arr, (inputs, mixed, ffn_out, last, hidden_grad), (gains_local, gains_other), (flat, wide)
    )
    query_grad = qkv_full[:, :q_width].astype(F32)
    key_grad = qkv_full[:, q_width : q_width + HEAD_DIM].astype(F32)
    value_grad = qkv_full[:, q_width + HEAD_DIM :].astype(F32)

    gain_parts = jnp.stack([gain_one_part[0], gain_two_part[0]])
    gain_kept = gain_parts[:, :half] + flip(gain_parts[:, half:], "fsdp", 1, 2)
    for bit in every:
        gain_kept = gain_kept + flip(gain_kept, "ctx", bit, n_ctx)

    return (
        outputs,
        input_grad,
        query_grad,
        key_grad,
        value_grad,
        out_full.astype(F32),
        gate_full.astype(F32),
        up_full.astype(F32),
        down_full.astype(F32),
        gain_kept[0],
        gain_kept[1],
    )


def solution(mesh):
    n_ctx = mesh.shape["ctx"]

    def body(*args):
        return shards(n_ctx, mesh.shape["head"], *args)

    return jax.shard_map(
        body,
        mesh=mesh,
        in_specs=(
            P(("ctx", "fsdp"), None),
            P("fsdp", "head"),
            P("fsdp", "head"),
            P("fsdp", "head"),
            P("head", "fsdp"),
            P("fsdp", "head"),
            P("fsdp", "head"),
            P("head", "fsdp"),
            P("fsdp"),
            P("fsdp"),
            P(("ctx", "fsdp"), None),
        ),
        out_specs=(
            P(("ctx", "fsdp"), None),
            P(("ctx", "fsdp"), None),
            P("fsdp", "head"),
            P("fsdp", "head"),
            P("fsdp", "head"),
            P("head", "fsdp"),
            P("fsdp", "head"),
            P("fsdp", "head"),
            P("head", "fsdp"),
            P("fsdp"),
            P("fsdp"),
        ),
        check_vma=False,
    )
```
